32 devices in a mesh: dp: 4 (over z), expert: 8 (over y, x, core).
Axes of the slice: x: 2, y: 2, z: 4, core: 2. Of those that a mesh axis runs over, the one named last changes fastest.
Arguments:
- tokens: bfloat16 [2, 12288, 768], P(None, ('dp', 'expert')), may hold values from -6 to 6
- cotangent: bfloat16 [2, 12288, 768], P(None, ('dp', 'expert')), may hold values from -6 to 6
- token_ids: int32 [2, 12288], P(None, ('dp', 'expert')), may hold values from 0 to 8007, as said below
- hash_table: int32 [8008], replicated, may hold values from 0 to 7, as said below
- segment_ids: int32 [2, 12288], P(None, ('dp', 'expert')), may hold values from 0 to 1, as said below
- query_weight: bfloat16 [768, 768], replicated, may hold values from -0.21875 to 0.21875
- key_weight: bfloat16 [768, 768], replicated, may hold values from -0.21875 to 0.21875
- value_weight: bfloat16 [768, 768], replicated, may hold values from -0.21875 to 0.21875
- output_weight: bfloat16 [768, 768], replicated, may hold values from -2.5 to 2.5
- gain_attn: float32 [768], replicated, may hold values from 0.5 to 1.5
- gain_ffn: float32 [768], replicated, may hold values from 0.5 to 1.5
- expert_in: bfloat16 [8, 768, 3072], P('expert'), may hold values from -0.21875 to 0.21875
- expert_out: bfloat16 [8, 3072, 768], P('expert'), may hold values from -0.109375 to 0.109375
Outputs:
- block_out: bfloat16 [2, 12288, 768], P(None, ('dp', 'expert'))
- grad_tokens: bfloat16 [2, 12288, 768], P(None, ('dp', 'expert'))
- grad_query: float32 [768, 768], replicated
- grad_key: float32 [768, 768], replicated
- grad_value: float32 [768, 768], replicated
- grad_output: float32 [768, 768], replicated
- grad_gain_attn: float32 [768], replicated
- grad_gain_ffn: float32 [768], replicated
- grad_expert_in: float32 [8, 768, 3072], P('expert')
- grad_expert_out: float32 [8, 3072, 768], P('expert')
The draws below stay inside these ranges and needn't reach their ends.
Inputs may be any that keep to these rules, and one draw needn't show every extreme that they name: hash_table sends 8008 // 8 or more ids to every expert. `token_ids`: in every micro-batch the 384 tokens of one device name any expert, through hash_table, at most 96 times; in every micro-batch one expert is named exactly 96 times by the tokens of every device. `segment_ids`: in each micro-batch a device's block holds either one sequence (all 0) or a sequence of 256 tokens (0) followed by one of the rest (1).
All inputs are finite; a program needn't handle non-finite values.
Results may differ from the reference program's by a relative error of at most 0.012.
Values may be sent and summed in bfloat16 or wider, within the bound.
No kernel may reach another device: no remote copies, remote signals or barrier semaphores. Data moves between devices by JAX's collectives and lax.ppermute only.
A program may use at most 192 MiB of HBM per device.

```python
import jax
import jax.numpy as jnp
from jax import lax

D = 768
HEADS = 12
HEAD_DIM = 64
FF = 3072
VOCAB = 8008
TOK_DEV = 384
MICRO = 2
EXPERTS = 8
BLOCKS = 32
TOKENS = 12288
CAP = 96


def vocab_order(key):
    return jax.random.permutation(jax.random.fold_in(key, 11), VOCAB)


def draw_hash_table(key, part):
    return (vocab_order(key) % EXPERTS).astype(jnp.int32)


def device_experts(key, favored):
    slot_order = jax.random.permutation(key, EXPERTS * CAP)
    is_favored = (slot_order // CAP == favored).astype(jnp.int32)
    arranged = slot_order[jnp.argsort(1 - is_favored, stable=True)]
    chosen = arranged[:TOK_DEV] // CAP
    return chosen[jax.random.permutation(jax.random.fold_in(key, 5), TOK_DEV)]


def draw_token_ids(key, part):
    order = vocab_order(key)
    inverse = jnp.argsort(order).astype(jnp.int32)
    base = jax.random.fold_in(key, 23)
    batches = []
    for batch in range(MICRO):
        favored = jax.random.randint(jax.random.fold_in(base, 1000 + batch), (), 0, EXPERTS)
        device_keys = jax.random.split(jax.random.fold_in(base, batch), BLOCKS)

        def one_device(device_key):
            return device_experts(device_key, favored)
        batches.append(jax.vmap(one_device)(device_keys).reshape(TOKENS))
    assigned = jnp.stack(batches).astype(jnp.int32)
    choose = jax.random.randint(jax.random.fold_in(key, 31), assigned.shape, 0, VOCAB // EXPERTS)
    return inverse[assigned + EXPERTS * choose].astype(jnp.int32)


def draw_segment_ids(key, part):
    split_rows = jax.random.randint(key, (MICRO, BLOCKS, 1), 0, 2)
    split_rows = split_rows.at[0, 0, 0].set(1).at[0, 1, 0].set(0)
    position = jnp.arange(TOK_DEV)[None, None, :]
    later = (position >= 2 * TOK_DEV // 3).astype(jnp.int32)
    return (split_rows * later).reshape(MICRO, TOKENS).astype(jnp.int32)


def level_of(stream_key, shape, pieces, smallest, top_value):
    def one(dim, parts):
        draws = jax.random.uniform(jax.random.fold_in(jax.random.fold_in(stream_key, 6), dim), (parts,), jnp.float32, smallest / len(pieces), top_value / len(pieces))
        return jnp.repeat(jnp.exp(draws), shape[dim] // parts).reshape((-1,) + (1,) * (len(shape) - dim - 1))

    factor_of = one(*pieces[0])
    for cut in pieces[1:]:
        factor_of = factor_of * one(*cut)
    return factor_of


def noise(key, shape, spread, limit, pieces=(), kind=jnp.bfloat16):
    array = spread * jax.random.normal(key, shape, jnp.float32)
    if pieces:
        array = array * level_of(key, shape, pieces, -0.22, 0.18)
    return jnp.clip(array, -limit, limit).astype(kind)


def setup_inputs(seed: int = 0) -> dict:
    keys = jax.random.split(jax.random.key(seed), 14)
    return {
        "tokens": noise(keys[0], (MICRO, TOKENS, D), 1.0, 6.0, ((1, 32),)),
        "cotangent": noise(keys[1], (MICRO, TOKENS, D), 1.0, 6.0, ((1, 32),)),
        "token_ids": draw_token_ids(jax.random.fold_in(keys[13], 71), 0),
        "hash_table": draw_hash_table(jax.random.fold_in(keys[13], 71), 0),
        "segment_ids": draw_segment_ids(jax.random.fold_in(keys[13], 71), 0),
        "query_weight": noise(keys[5], (D, D), D ** -0.5, 0.21875),
        "key_weight": noise(keys[6], (D, D), D ** -0.5, 0.21875),
        "value_weight": noise(keys[7], (D, D), D ** -0.5, 0.21875),
        "output_weight": noise(keys[8], (D, D), (max(2, D // 128)) ** -0.5, 2.5),
        "gain_attn": jnp.clip(1.0 + 0.1 * jax.random.normal(keys[9], (D,), jnp.float32), 0.5, 1.5),
        "gain_ffn": jnp.clip(1.0 + 0.1 * jax.random.normal(keys[10], (D,), jnp.float32), 0.5, 1.5),
        "expert_in": noise(keys[11], (EXPERTS, D, FF), D ** -0.5, 0.21875, ((0, 8),)),
        "expert_out": noise(keys[12], (EXPERTS, FF, D), FF ** -0.5, 0.109375, ((0, 8),)),
    }


@jax.custom_vjp
def low(v):
    return lax.optimization_barrier(v.astype(jnp.bfloat16)).astype(jnp.float32)

@jax.custom_vjp
def low_back(v):
    return v

def low_keep(v):
    return (low(v), None)

def low_pass(kept, grad):
    return (grad,)

def back_keep(v):
    return (v, None)

def back_low(kept, grad):
    return (low(grad),)
low.defvjp(low_keep, low_pass)
low_back.defvjp(back_keep, back_low)
highest = lax.Precision.HIGHEST
epsilon = 1e-05

def matmul(left, right):
    return jnp.matmul(left, right, precision=highest)

def normalize(values, gain):
    return values * lax.rsqrt(lax.optimization_barrier(jnp.mean(values * values, axis=-1, keepdims=True)) + epsilon) * gain

def attend(normed, segments, query_weight, key_weight, value_weight, output_weight):
    length = normed.shape[0]

    def heads_of(weight):
        return low_back(low(matmul(normed, weight))).reshape(length, HEADS, HEAD_DIM).transpose(1, 0, 2)
    queries = heads_of(query_weight)
    keys_all = heads_of(key_weight)
    values_all = heads_of(value_weight)
    scores = low_back(jnp.einsum('hqd,hkd->hqk', queries, keys_all, precision=highest) * HEAD_DIM ** (-0.5))
    position = jnp.arange(length, dtype=jnp.int32)
    segments = segments.astype(jnp.int32)
    allowed = (position[:, None] >= position[None, :]) & (segments[:, None] == segments[None, :])
    scores = jnp.where(allowed[None], scores, jnp.asarray(-1e+30, normed.dtype))
    weights_soft = jax.nn.softmax(scores, axis=-1)
    mixed = jnp.einsum('hqk,hkd->hqd', low(weights_soft), values_all, precision=highest)
    mixed = low_back(low(mixed)).transpose(1, 0, 2).reshape(length, HEADS * HEAD_DIM)
    return low_back(matmul(mixed, output_weight))

def expert_apply(pack):
    rows, weight_in, weight_out = pack
    pre_active = low_back(matmul(rows, weight_in))
    active = low(jax.nn.silu(pre_active))
    return low_back(low(matmul(active, weight_out)))

def place_slots(ids_row, hash_table):
    experts = jnp.take(hash_table, ids_row.astype(jnp.int32)).reshape(BLOCKS, TOK_DEV).astype(jnp.int32)
    onehot = (experts[..., None] == jnp.arange(EXPERTS, dtype=jnp.int32)).astype(jnp.int32)
    rank = lax.optimization_barrier(jnp.sum((jnp.cumsum(onehot, axis=1, dtype=jnp.int32) - onehot) * onehot, axis=-1, dtype=jnp.int32))
    source = jnp.arange(BLOCKS, dtype=jnp.int32)[:, None]
    return (experts * (BLOCKS * CAP) + source * CAP + rank).reshape(TOKENS).astype(jnp.int32)

def forward(inputs_f, segments, slot_index, query_weight, key_weight, value_weight, output_weight, gain_attn, gain_ffn, expert_in, expert_out):
    normed = low(normalize(inputs_f, gain_attn))

    def one_block(pair):
        return attend(pair[0], pair[1], query_weight, key_weight, value_weight, output_weight)
    attended = lax.map(jax.checkpoint(one_block), (normed.reshape(BLOCKS, TOK_DEV, D), segments.reshape(BLOCKS, TOK_DEV).astype(jnp.int32)))
    hidden = inputs_f + attended.reshape(TOKENS, D)
    routed = low_back(low(normalize(hidden, gain_ffn)))
    packed = jnp.zeros((EXPERTS * BLOCKS * CAP, D), inputs_f.dtype).at[slot_index].set(routed)
    produced = lax.map(jax.checkpoint(expert_apply), (packed.reshape(EXPERTS, BLOCKS * CAP, D), expert_in, expert_out))
    return hidden + produced.reshape(EXPERTS * BLOCKS * CAP, D)[slot_index]

def reference(tokens, cotangent, token_ids, hash_table, segment_ids, query_weight, key_weight, value_weight, output_weight, gain_attn, gain_ffn, expert_in, expert_out):
    weights = tuple((weight.astype(jnp.float32) for weight in (query_weight, key_weight, value_weight, output_weight, gain_attn, gain_ffn, expert_in, expert_out)))
    totals = tuple((jnp.zeros_like(weight) for weight in weights))
    outputs = []
    grads_in = []
    for batch in range(MICRO):
        slot_index = place_slots(token_ids[batch], hash_table)
        segments = segment_ids[batch].astype(jnp.int32)

        def bound(inputs_f, *params):
            return forward(inputs_f, segments, slot_index, *params)
        result, pull = jax.vjp(bound, tokens[batch].astype(jnp.float32), *weights)
        grads = pull(cotangent[batch].astype(jnp.float32).astype(result.dtype))
        outputs.append(result.astype(jnp.bfloat16))
        grads_in.append(grads[0].astype(jnp.bfloat16))
        totals = tuple((total + grad for total, grad in zip(totals, grads[1:])))
    return (jnp.stack(outputs), jnp.stack(grads_in), totals[0], totals[1], totals[2], totals[3], totals[4], totals[5], totals[6], totals[7])
```

```python
import functools

import jax
import jax.numpy as jnp
from jax import lax
from jax.experimental import pallas as pl
from jax.experimental.pallas import tpu as pltpu
from jax.sharding import PartitionSpec as P

HEADS = 12
HEAD_DIM = 64
EPS = 1e-05
SCALE = HEAD_DIM ** (-0.5)
PAIR = 2 * HEAD_DIM
F32 = jnp.float32
BF16 = jnp.bfloat16
VMEM_LIMIT = 56 * 1024 * 1024


def dot(a, b, ca=1, cb=0):
    return lax.dot_general(a, b, (((ca,), (cb,)), ((), ())), preferred_element_type=F32)


def params(n):
    return pltpu.CompilerParams(
        dimension_semantics=("arbitrary",) * n, vmem_limit_bytes=VMEM_LIMIT
    )


def full(*shape):
    return pl.BlockSpec(shape, lambda *_: (0,) * len(shape))


ANY = pl.BlockSpec(memory_space=pl.ANY)


def iota(shape, axis):
    return lax.broadcasted_iota(jnp.int32, shape, axis)


def to_column(row):
    n = row.shape[1]
    eye = iota((n, n), 0) == iota((n, n), 1)
    return jnp.sum(jnp.where(eye, row, 0), axis=1, keepdims=True)


def route_kernel(m, owners, cap, ids_ref, table_ref, cot_ref, slot_ref, pack_ref):
    n = ids_ref.shape[1]
    ids = ids_ref[pl.ds(m, 1), :]
    rows = table_ref.shape[0]
    pick = (iota((rows, n), 0) == (ids >> 7)).astype(BF16)
    values = dot(table_ref[...].astype(BF16), pick, 0, 0)
    lane = ids & 127
    expert = jnp.sum(jnp.where(iota((128, n), 0) == lane, values, 0.0), axis=0, keepdims=True)
    kinds = -(-owners // 16) * 16
    named = iota((kinds, n), 0).astype(F32) == expert
    before = (iota((n, n), 0) < iota((n, n), 1)).astype(BF16)
    counts = dot(named.astype(BF16), before)
    rank = jnp.sum(jnp.where(named, counts, 0.0), axis=0, keepdims=True)
    slot = (expert * cap + rank).astype(jnp.int32)
    slot_ref[...] = slot
    places = (iota((owners * cap, n), 0) == slot).astype(BF16)
    pack_ref[...] = dot(places, cot_ref[0]).astype(BF16)


def route(m, ids, table, cot, owners, cap):
    micro, n = ids.shape
    width = cot.shape[2]
    rows = table.shape[0]
    return pl.pallas_call(
        functools.partial(route_kernel, m, owners, cap),
        grid=(1,),
        in_specs=[
            full(micro, n), full(rows, 128), pl.BlockSpec((1, n, width), lambda i: (m, 0, 0)),
        ],
        out_specs=[full(1, n), full(owners * cap, width)],
        out_shape=[
            jax.ShapeDtypeStruct((1, n), jnp.int32),
            jax.ShapeDtypeStruct((owners * cap, width), BF16),
        ],
        compiler_params=params(1),
    )(ids, table, cot)


def bias_of(seg):
    n = seg.shape[1]
    key, query = iota((n, n), 0), iota((n, n), 1)
    seen = (key <= query) & (to_column(seg) == seg)
    return jnp.where(seen, 0.0, -1e30)


def forward_kernel(
    m, slot_ref, seg_ref, tok_ref, wq_ref, wk_ref, wv_ref, wo_ref, ga_ref, gf_ref, dep_ref,
    normed_ref, q_ref, k_ref, v_ref, lse_ref, mixed_ref, hidden_ref, pack_ref, bias_ref,
):
    x = tok_ref[0].astype(F32)
    n = x.shape[0]
    r = lax.rsqrt(jnp.mean(x * x, axis=1, keepdims=True) + EPS)
    normed = (x * r * ga_ref[...]).astype(BF16)
    normed_ref[...] = normed
    q_ref[...] = (dot(normed, wq_ref[...]).astype(BF16) * SCALE).astype(BF16)
    k_ref[...] = dot(normed, wk_ref[...]).astype(BF16)
    v_ref[...] = dot(normed, wv_ref[...]).astype(BF16)
    bias_ref[...] = bias_of(seg_ref[pl.ds(m, 1), :])
    low = iota((n, PAIR), 1) < HEAD_DIM

    def pair(p, carry):
        cols = pl.ds(pl.multiple_of(p * PAIR, PAIR), PAIR)
        q, k, v = q_ref[:, cols], k_ref[:, cols], v_ref[:, cols]
        parts = []
        for h in range(2):
            mine = low if h == 0 else ~low
            s = dot(k, jnp.where(mine, q, 0), 1, 1) + bias_ref[...]
            top = jnp.max(s, axis=0, keepdims=True)
            e = jnp.exp(s - top)
            total = jnp.sum(e, axis=0, keepdims=True)
            lse_ref[pl.ds(2 * p + h, 1), :] = top + jnp.log(total)
            probs = (e * (1.0 / total)).astype(BF16)
            parts.append(dot(probs, v, 0, 0))
        mixed_ref[:, cols] = jnp.where(low, parts[0], parts[1]).astype(BF16)
        return carry

    lax.fori_loop(0, HEADS // 2, pair, 0)
    hidden = x + dot(mixed_ref[...], wo_ref[...])
    hidden_ref[...] = hidden
    r = lax.rsqrt(jnp.mean(hidden * hidden, axis=1, keepdims=True) + EPS)
    routed = (hidden * r * gf_ref[...]).astype(BF16)
    places = (iota((pack_ref.shape[0], n), 0) == slot_ref[...]).astype(BF16)
    pack_ref[...] = dot(places, routed).astype(BF16)


def forward(m, slot, seg, tokens, wq, wk, wv, wo, ga, gf, slots, dep):
    _, n, d = tokens.shape
    shapes = [
        ((n, d), BF16), ((n, d), BF16), ((n, d), BF16), ((n, d), BF16), ((16, n), F32),
        ((n, d), BF16), ((n, d), F32), ((slots, d), BF16),
    ]
    return pl.pallas_call(
        functools.partial(forward_kernel, m),
        grid=(1,),
        in_specs=[
            full(1, n), full(*seg.shape), pl.BlockSpec((1, n, d), lambda i: (m, 0, 0)),
            full(d, d), full(d, d), full(d, d), full(d, d), full(1, d), full(1, d), ANY,
        ],
        out_specs=[full(*s) for s, _ in shapes],
        out_shape=[jax.ShapeDtypeStruct(s, t) for s, t in shapes],
        scratch_shapes=[pltpu.VMEM((n, n), F32)],
        compiler_params=params(1),
    )(slot, seg, tokens, wq, wk, wv, wo, ga, gf, dep)


BLOCK = 256


def expert_kernel(rx0_ref, rx1_ref, g0_ref, g1_ref, win_ref, wout_ref, *rest):
    chunk_ref, act_ref, gpre_ref = rest[-3:]
    win, wout = win_ref[0], wout_ref[0]
    f = win.shape[1]
    rows = rx0_ref.shape[0]
    gout, gin = None, None
    for m, (x_ref, g_ref) in enumerate(((rx0_ref, g0_ref), (rx1_ref, g1_ref))):
        x, g = x_ref[...], g_ref[...]
        pre = dot(x, win)
        sig = jax.nn.sigmoid(pre)
        act = (pre * sig).astype(BF16)
        slope = sig * (1.0 + pre * (1.0 - sig))
        gpre = (dot(g, wout, 1, 1) * slope).astype(BF16)
        act_ref[pl.ds(m * rows, rows), :] = act
        gpre_ref[pl.ds(m * rows, rows), :] = gpre
        a, b = dot(act, g, 0, 0), dot(gpre, x, 0, 0)
        gout, gin = (a, b) if m == 0 else (gout + a, gin + b)
    chunk_ref[pl.ds(0, f), :] = gout.astype(BF16)
    chunk_ref[pl.ds(f, f), :] = gin.astype(BF16)


def expert(c, units, rx, g, win, wout, held, dep):
    rows, d = rx[0].shape
    ff = win.shape[2]
    f = BLOCK
    extra = ([] if held is None else list(held)) + [dep]
    alias = {} if held is None else {6: 1, 7: 2}
    return pl.pallas_call(
        expert_kernel,
        grid=(units,),
        in_specs=[full(rows, d)] * 4
        + [
            pl.BlockSpec((1, d, f), lambda i: (0, 0, c + i)),
            pl.BlockSpec((1, f, d), lambda i: (0, c + i, 0)),
        ]
        + [ANY] * len(extra),
        out_specs=[
            pl.BlockSpec((2 * f, d), lambda i: (i, 0)),
            pl.BlockSpec((2 * rows, f), lambda i: (0, c + i)),
            pl.BlockSpec((2 * rows, f), lambda i: (0, c + i)),
        ],
        out_shape=[
            jax.ShapeDtypeStruct((units * 2 * f, d), BF16),
            jax.ShapeDtypeStruct((2 * rows, ff), BF16),
            jax.ShapeDtypeStruct((2 * rows, ff), BF16),
        ],
        input_output_aliases=alias,
        compiler_params=params(1),
    )(*rx, *g, win, wout, *extra)


def rows_kernel(side, a_ref, w_ref, dep_ref, o_ref):
    o_ref[...] = dot(a_ref[...], w_ref[0], 1, side).astype(BF16)


def back_rows(m, a, w, side, dep, blk=384):
    ff = a.shape[1]
    rows = a.shape[0] // 2
    d = w.shape[1 + (1 - side)]
    steps = rows // blk
    return pl.pallas_call(
        functools.partial(rows_kernel, side),
        grid=(steps,),
        in_specs=[pl.BlockSpec((blk, ff), lambda i: (m * steps + i, 0)), full(*w.shape), ANY],
        out_specs=pl.BlockSpec((blk, d), lambda i: (i, 0)),
        out_shape=jax.ShapeDtypeStruct((rows, d), BF16),
        compiler_params=params(1),
    )(a, w, dep)


def backward_kernel(
    m, slot_ref, seg_ref, tok_ref, cot_ref, back_ref, normed_ref, q_ref, k_ref, v_ref, lse_ref,
    hidden_ref, wq_ref, wk_ref, wv_ref, wo_ref, ga_ref, gf_ref, *rest,
):
    gtok_ref, gattn_ref, gq_ref, gk_ref, gv_ref, gain_ref, bias_ref, gm_ref, gh_ref = rest[-9:]
    n, d = normed_ref.shape
    slots = back_ref.shape[0]
    places = (iota((n, slots), 1) == to_column(slot_ref[...])).astype(BF16)
    grad_routed = dot(places, back_ref[...])
    hidden = hidden_ref[...]
    r = lax.rsqrt(jnp.mean(hidden * hidden, axis=1, keepdims=True) + EPS)
    unit = hidden * r
    g = grad_routed * gf_ref[...]
    grad_hidden = cot_ref[0].astype(F32) + r * (
        g - unit * jnp.mean(g * unit, axis=1, keepdims=True)
    )
    gh_ref[...] = grad_hidden
    gain_ref[pl.ds(1, 1), :] = jnp.sum(grad_routed * unit, axis=0, keepdims=True)
    grad_attn = grad_hidden.astype(BF16)
    gattn_ref[...] = grad_attn
    gm_ref[...] = dot(grad_attn, wo_ref[...], 1, 1).astype(BF16)
    bias_ref[...] = bias_of(seg_ref[pl.ds(m, 1), :])
    low = iota((n, PAIR), 1) < HEAD_DIM

    def pair(p, carry):
        cols = pl.ds(pl.multiple_of(p * PAIR, PAIR), PAIR)
        q, k, v, gm = q_ref[:, cols], k_ref[:, cols], v_ref[:, cols], gm_ref[:, cols]
        gqs, gks, gvs = [], [], []
        for h in range(2):
            mine = low if h == 0 else ~low
            s = dot(k, jnp.where(mine, q, 0), 1, 1) + bias_ref[...]
            probs = jnp.exp(s - lse_ref[pl.ds(2 * p + h, 1), :])
            gvs.append(dot(probs.astype(BF16), gm))
            gp = dot(v, jnp.where(mine, gm, 0), 1, 1)
            shared = jnp.sum(probs * gp, axis=0, keepdims=True)
            gs = (probs * (gp - shared)).astype(BF16)
            gks.append(dot(gs, q))
            gqs.append(dot(gs, k, 0, 0))
        gq_ref[:, cols] = (jnp.where(low, gqs[0], gqs[1]) * SCALE).astype(BF16)
        gk_ref[:, cols] = jnp.where(low, gks[0], gks[1]).astype(BF16)
        gv_ref[:, cols] = jnp.where(low, gvs[0], gvs[1]).astype(BF16)
        return carry

    lax.fori_loop(0, HEADS // 2, pair, 0)
    grad_normed = (
        dot(gq_ref[...], wq_ref[...], 1, 1)
        + dot(gk_ref[...], wk_ref[...], 1, 1)
        + dot(gv_ref[...], wv_ref[...], 1, 1)
    )
    x = tok_ref[0].astype(F32)
    r = lax.rsqrt(jnp.mean(x * x, axis=1, keepdims=True) + EPS)
    unit = x * r
    gain_ref[pl.ds(0, 1), :] = jnp.sum(grad_normed * unit, axis=0, keepdims=True)
    g = grad_normed * ga_ref[...]
    gtok_ref[0] = (
        gh_ref[...] + r * (g - unit * jnp.mean(g * unit, axis=1, keepdims=True))
    ).astype(BF16)


def backward(m, slot, seg, tokens, cot, back, saved, wq, wk, wv, wo, ga, gf, held, dep):
    micro, n, d = tokens.shape
    normed, q, k, v, lse, _, hidden = saved
    mat = pl.BlockSpec((1, n, d), lambda i: (m, 0, 0))
    extra = [dep] if held is None else [dep, held]
    return pl.pallas_call(
        functools.partial(backward_kernel, m),
        grid=(1,),
        in_specs=[full(1, n), full(*seg.shape), mat, mat, full(*back.shape)]
        + [full(*a.shape) for a in (normed, q, k, v, lse, hidden)]
        + [full(d, d)] * 4 + [full(1, d)] * 2 + [ANY] * len(extra),
        out_specs=[mat] + [full(n, d)] * 4 + [full(8, d)],
        out_shape=[jax.ShapeDtypeStruct((micro, n, d), BF16)]
        + [jax.ShapeDtypeStruct((n, d), BF16)] * 4
        + [jax.ShapeDtypeStruct((8, d), F32)],
        scratch_shapes=[
            pltpu.VMEM((n, n), F32), pltpu.VMEM((n, d), BF16), pltpu.VMEM((n, d), F32)
        ],
        compiler_params=params(1),
        input_output_aliases={} if held is None else {18: 0},
    )(slot, seg, tokens, cot, back, normed, q, k, v, lse, hidden, wq, wk, wv, wo, ga, gf, *extra)


def weights_kernel(n0, n1, x0, x1, q0, q1, k0, k1, v0, v1, a0, a1, gain0, gain1, dep_ref, o_ref):
    d = n0.shape[1]
    for i, (l0, l1, r0, r1) in enumerate(
        ((n0, n1, q0, q1), (n0, n1, k0, k1), (n0, n1, v0, v1), (x0, x1, a0, a1))
    ):
        both = dot(l0[...], r0[...], 0, 0) + dot(l1[...], r1[...], 0, 0)
        o_ref[pl.ds(i * d, d), :] = both.astype(BF16)
    rest = o_ref.shape[0] - 4 * d
    line = iota((rest, d), 0)
    gain = gain0[...] + gain1[...]
    o_ref[pl.ds(4 * d, rest), :] = jnp.where(
        line == 0, gain[0:1, :], jnp.where(line == 1, gain[1:2, :], 0.0)
    ).astype(BF16)


def dense_grads(saved, grads, rest, dep):
    n, d = saved[0][0].shape
    pairs = [(saved[0][0], saved[1][0]), (saved[0][5], saved[1][5])]
    pairs += [(grads[0][i], grads[1][i]) for i in (1, 2, 3, 0, 4)]
    flat = [a for both in pairs for a in both]
    return pl.pallas_call(
        weights_kernel,
        grid=(1,),
        in_specs=[full(*a.shape) for a in flat] + [ANY],
        out_specs=full(4 * d + rest, d),
        out_shape=jax.ShapeDtypeStruct((4 * d + rest, d), BF16),
        compiler_params=params(1),
    )(*flat, dep)


def output_kernel(s0_ref, s1_ref, b0_ref, b1_ref, h0_ref, h1_ref, dep_ref, o_ref):
    n = o_ref.shape[1]
    for m, (s_ref, b_ref, h_ref) in enumerate(((s0_ref, b0_ref, h0_ref), (s1_ref, b1_ref, h1_ref))):
        places = (iota((n, b_ref.shape[0]), 1) == to_column(s_ref[...])).astype(BF16)
        o_ref[m] = (h_ref[...] + dot(places, b_ref[...])).astype(BF16)


def block_output(slots, backs, hiddens, dep):
    micro = len(slots)
    n, d = hiddens[0].shape
    flat = [*slots, *backs, *hiddens]
    return pl.pallas_call(
        output_kernel,
        grid=(1,),
        in_specs=[full(*a.shape) for a in flat] + [ANY],
        out_specs=full(micro, n, d),
        out_shape=jax.ShapeDtypeStruct((micro, n, d), BF16),
        compiler_params=params(1),
    )(*flat, dep)


def add_kernel(a_ref, b_ref, dep_ref, o_ref):
    o_ref[...] = (a_ref[...].astype(F32) + b_ref[...].astype(F32)).astype(BF16)


def add(a, b, dep):
    rows, d = a.shape
    blk = 2 * BLOCK if rows % (2 * BLOCK) == 0 else rows
    spec = pl.BlockSpec((blk, d), lambda i: (i, 0))
    return pl.pallas_call(
        add_kernel,
        grid=(rows // blk,),
        in_specs=[spec, spec, ANY],
        out_specs=spec,
        out_shape=jax.ShapeDtypeStruct((rows, d), BF16),
        compiler_params=params(1),
    )(a, b, dep)


def pick_kernel(flag_ref, a_ref, b_ref, dep_ref, o_ref):
    o_ref[...] = jnp.where(flag_ref[0] == 1, b_ref[...], a_ref[...])


def pick(flag, a, b, dep):
    return pl.pallas_call(
        pick_kernel,
        in_specs=[pl.BlockSpec(memory_space=pltpu.SMEM)]
        + [pl.BlockSpec(memory_space=pltpu.VMEM)] * 2 + [ANY],
        out_specs=pl.BlockSpec(memory_space=pltpu.VMEM),
        out_shape=jax.ShapeDtypeStruct(a.shape, BF16),
        compiler_params=params(0),
    )(flag, a, b, dep)


def store_kernel(flag_ref, a_ref, b_ref, *rest):
    gin_ref, gout_ref = rest[-2:]
    f = gout_ref.shape[1]

    def put(ref):
        gout_ref[0] = ref[pl.ds(0, f), :].astype(F32)
        gin_ref[0] = ref[pl.ds(f, f), :].astype(F32).T

    @pl.when(flag_ref[0] == 1)
    def _():
        put(b_ref)

    @pl.when(flag_ref[0] != 1)
    def _():
        put(a_ref)


def store(c, flag, a, b, ff, held, dep):
    rows, d = a.shape
    f = BLOCK
    spec = pl.BlockSpec((2 * f, d), lambda i: (i, 0))
    extra = ([] if held is None else list(held)) + [dep]
    return pl.pallas_call(
        store_kernel,
        grid=(rows // (2 * f),),
        in_specs=[pl.BlockSpec(memory_space=pltpu.SMEM), spec, spec] + [ANY] * len(extra),
        out_specs=[
            pl.BlockSpec((1, d, f), lambda i: (0, 0, c + i)),
            pl.BlockSpec((1, f, d), lambda i: (0, c + i, 0)),
        ],
        out_shape=[
            jax.ShapeDtypeStruct((1, d, ff), F32),
            jax.ShapeDtypeStruct((1, ff, d), F32),
        ],
        input_output_aliases={} if held is None else {3: 0, 4: 1},
        compiler_params=params(1),
    )(flag, a, b, *extra)


SIZES = (1, 1, 2, 2, 2, 2, 1, 1)


PLAN = (
    ("E", 0), ("S1", 0), ("E", 1), ("S1", 1), ("E", 2), ("E", 3), ("S1", 2), ("G1", 0), ("E", 4),
    ("S1", 3), ("G1", 1), ("E", 5), ("G2", 0), ("E", 6), ("E", 7), ("G2", 1), ("Q1", 0), ("G3", 0),
    ("Q1", 1), ("G3", 1), ("S1", 4), ("G1", 2), ("B", 0), ("S1", 5), ("G1", 3), ("B", 1), ("W", 0),
    ("G2", 2), ("Q2", 0), ("S1", 6), ("G1", 4), ("Q2", 1), ("G2", 3), ("S1", 7), ("G1", 5), ("O",
    0), ("G3", 2), ("G1", 6), ("S1", "A"), ("G1", 7), ("G1", "A"), ("G3", 3), ("G2", 4), ("G2", 6),
    ("G3", 4), ("G2", "A"), ("G2", 7), ("G2", 5), ("G3", 6), ("G3", "A"), ("G3", 7), ("G3", 5),
)


def per_device(
    tokens, cotangent, token_ids, hash_table, segment_ids, query_weight, key_weight,
    value_weight, output_weight, gain_attn, gain_ffn, expert_in, expert_out,
):
    micro, n, d = tokens.shape
    ff = expert_in.shape[2]
    owners = lax.axis_size("expert")
    depth = lax.axis_size("dp")
    cap = 2 * n // owners
    weights = (query_weight, key_weight, value_weight, output_weight)
    gains = (gain_attn.reshape(1, d), gain_ffn.reshape(1, d))
    place = lax.axis_index("dp")
    outer = ((place == 0) | (place == depth - 1)).astype(jnp.int32).reshape(1)
    size = hash_table.shape[0]
    table_rows = -(-size // 1024) * 8
    table = jnp.pad(hash_table, (0, table_rows * 128 - size)).reshape(table_rows, 128)

    def swap(x):
        return lax.all_to_all(x, "expert", split_axis=0, concat_axis=0, tiled=True)

    def after(x, dep):
        return lax.optimization_barrier((x, dep))[0]

    slots, saved, rx, gx = [], [], [], []
    dep = None
    for m in range(micro):
        slot, packed = route(m, token_ids, table, cotangent, owners, cap)
        gx.append(swap(packed))
        dep = packed if dep is None else dep
        *kept, packed = forward(
            m, slot, segment_ids, tokens, *weights, *gains, owners * cap, dep
        )
        rx.append(swap(packed))
        dep = packed
        slots.append(slot)
        saved.append(tuple(kept))

    starts = [sum(SIZES[:i]) for i in range(len(SIZES))]
    chunk, hop1, hop2, hop3, sum1, total = {}, {}, {}, {}, {}, {}
    held = stored = gtok = None
    backs, results, grads = {}, {}, {}
    dense = block_out = None
    for op, c in PLAN:
        if op == "E":
            chunk[c], *held = expert(
                starts[c], SIZES[c], rx, gx, expert_in, expert_out, held, dep
            )
            dep = chunk[c]
        elif op == "S1":
            x = after(chunk[c], dep)
            if depth == 4:
                hop1[c] = lax.ppermute(x, "dp", [(0, 1), (3, 2)])
            else:
                hop1[c] = x
        elif op == "G1":
            if depth == 4:
                sum1[c] = add(chunk[c], hop1[c], dep)
                hop2[c] = lax.ppermute(sum1[c], "dp", [(1, 2), (2, 1)])
                dep = sum1[c]
        elif op == "G2":
            if depth == 4:
                total[c] = add(sum1[c], hop2[c], dep)
                hop3[c] = lax.ppermute(total[c], "dp", [(1, 0), (2, 3)])
                dep = total[c]
            else:
                total[c] = hop3[c] = lax.psum(hop1[c], "dp")
        elif op == "G3":
            if c == "A":
                dense = pick(outer, total[c], hop3[c], dep)
                dep = dense
                dense = lax.all_gather(dense, "expert", axis=0, tiled=True)
            else:
                stored = store(starts[c], outer, total[c], hop3[c], ff, stored, dep)
                dep = stored[0]
        elif op == "Q1":
            dep = back_rows(c, held[1], expert_in, 1, dep)
            backs[c] = swap(dep)
        elif op == "Q2":
            dep = back_rows(c, held[0], expert_out, 0, dep)
            results[c] = swap(dep)
        elif op == "B":
            gtok, *grads[c] = backward(
                c, slots[c], segment_ids, tokens, cotangent, backs[c], saved[c], *weights,
                *gains, gtok, dep,
            )
            dep = grads[c][0]
        elif op == "W":
            dep = dense_grads(saved, grads, 16 * owners, dep)
            chunk["A"] = lax.psum_scatter(dep, "expert", scatter_dimension=0, tiled=True)
        elif op == "O":
            block_out = block_output(
                slots, [results[m] for m in range(micro)], [s[6] for s in saved], dep
            )
            dep = block_out
    wide = dense.astype(F32)
    return (
        block_out,
        gtok,
        *(wide[i * d : (i + 1) * d] for i in range(4)),
        wide[4 * d],
        wide[4 * d + 1],
        *stored,
    )


def solution(mesh):
    blocks, ids = P(None, ("dp", "expert"), None), P(None, ("dp", "expert"))
    owned = P("expert", None, None)
    return jax.shard_map(
        per_device,
        mesh=mesh,
        in_specs=(blocks, blocks, ids, P(), ids, P(), P(), P(), P(), P(), P(), owned, owned),
        out_specs=(blocks, blocks, P(), P(), P(), P(), P(), P(), owned, owned),
        check_vma=False,
    )
```

```python
import functools

import jax
import jax.numpy as jnp
from jax import lax
from jax.experimental import pallas as pl
from jax.experimental.pallas import tpu as pltpu
from jax.sharding import PartitionSpec as P

HEADS = 12
HEAD_DIM = 64
EPS = 1e-05
SCALE = HEAD_DIM ** (-0.5)
PAIR = 2 * HEAD_DIM
F32 = jnp.float32
BF16 = jnp.bfloat16


def dot(a, b, ca=1, cb=0):
    return lax.dot_general(a, b, (((ca,), (cb,)), ((), ())), preferred_element_type=F32)


def params(mib):
    return pltpu.CompilerParams(
        dimension_semantics=("arbitrary",), vmem_limit_bytes=mib * 1024 * 1024
    )


PACE = 100.0


def cost(us):
    return pl.CostEstimate(flops=int(us * PACE * 1.15e9), bytes_accessed=int(us * 3.0e6), transcendentals=0)


def full(*shape):
    return pl.BlockSpec(shape, lambda *_: (0,) * len(shape))


ANY = pl.BlockSpec(memory_space=pl.ANY)


def iota(shape, axis):
    return lax.broadcasted_iota(jnp.int32, shape, axis)


def to_column(row):
    n = row.shape[1]
    eye = iota((n, n), 0) == iota((n, n), 1)
    return jnp.sum(jnp.where(eye, row, 0), axis=1, keepdims=True)


def spread(slots, values, count):
    total = None
    for slot, value in zip(slots, values):
        places = (iota((count, slot.shape[1]), 0) == slot).astype(BF16)
        part = dot(places, value)
        total = part if total is None else total + part
    return total.astype(BF16)


def route_kernel(owners, cap, ids_ref, table_ref, cot_ref, slot0_ref, slot1_ref, pack_ref):
    micro, n = ids_ref.shape
    rows = table_ref.shape[0]
    table = table_ref[...].astype(BF16)
    kinds = -(-owners // 16) * 16
    before = (iota((n, n), 0) < iota((n, n), 1)).astype(BF16)
    slots = []
    for m, slot_ref in enumerate((slot0_ref, slot1_ref)):
        ids = ids_ref[pl.ds(m, 1), :]
        pick = (iota((rows, n), 0) == (ids >> 7)).astype(BF16)
        values = dot(table, pick, 0, 0)
        lane = ids & 127
        expert = jnp.sum(
            jnp.where(iota((128, n), 0) == lane, values, 0.0), axis=0, keepdims=True
        )
        named = iota((kinds, n), 0).astype(F32) == expert
        counts = dot(named.astype(BF16), before)
        rank = jnp.sum(jnp.where(named, counts, 0.0), axis=0, keepdims=True)
        slot = (expert * cap + rank).astype(jnp.int32)
        slot_ref[...] = slot
        slots.append(slot)
    pack_ref[...] = spread(slots[:1], (cot_ref[0],), pack_ref.shape[0])


def route(ids, table, cot, owners, cap):
    micro, n = ids.shape
    width = cot.shape[2]
    rows = table.shape[0]
    return pl.pallas_call(
        functools.partial(route_kernel, owners, cap),
        grid=(1,),
        in_specs=[full(micro, n), full(rows, 128), full(1, n, width)],
        out_specs=[full(1, n), full(1, n), full(owners * cap, width)],
        out_shape=[
            jax.ShapeDtypeStruct((1, n), jnp.int32),
            jax.ShapeDtypeStruct((1, n), jnp.int32),
            jax.ShapeDtypeStruct((owners * cap, width), BF16),
        ],
        cost_estimate=cost(5.0),
        compiler_params=params(12),
    )(ids, table, cot)


def bias_of(seg):
    n = seg.shape[1]
    key, query = iota((n, n), 0), iota((n, n), 1)
    seen = (key <= query) & (to_column(seg) == seg)
    return jnp.where(seen, 0.0, -1e30)


def forward_kernel(
    m, cap, slot_ref, seg_ref, tok_ref, cot_ref, wq_ref, wk_ref, wv_ref, wo_ref, ga_ref, gf_ref,
    dep_ref, normed_ref, q_ref, k_ref, v_ref, lse_ref, mixed_ref, hidden_ref, last_ref, bias_ref,
):
    x = tok_ref[0].astype(F32)
    n = x.shape[0]
    r = lax.rsqrt(jnp.mean(x * x, axis=1, keepdims=True) + EPS)
    normed = (x * r * ga_ref[...]).astype(BF16)
    normed_ref[...] = normed
    q_ref[...] = (dot(normed, wq_ref[...]).astype(BF16) * SCALE).astype(BF16)
    k_ref[...] = dot(normed, wk_ref[...]).astype(BF16)
    v_ref[...] = dot(normed, wv_ref[...]).astype(BF16)
    bias_ref[...] = bias_of(seg_ref[pl.ds(m, 1), :])
    low = iota((n, PAIR), 1) < HEAD_DIM

    def pair(p, carry):
        cols = pl.ds(pl.multiple_of(p * PAIR, PAIR), PAIR)
        q, k, v = q_ref[:, cols], k_ref[:, cols], v_ref[:, cols]
        parts = []
        for h in range(2):
            mine = low if h == 0 else ~low
            s = dot(k, jnp.where(mine, q, 0), 1, 1) + bias_ref[...]
            top = jnp.max(s, axis=0, keepdims=True)
            e = jnp.exp(s - top)
            total = jnp.sum(e, axis=0, keepdims=True)
            lse_ref[pl.ds(2 * p + h, 1), :] = top + jnp.log(total)
            probs = (e * (1.0 / total)).astype(BF16)
            parts.append(dot(probs, v, 0, 0))
        mixed_ref[:, cols] = jnp.where(low, parts[0], parts[1]).astype(BF16)
        return carry

    lax.fori_loop(0, HEADS // 2, pair, 0)
    hidden = x + dot(mixed_ref[...], wo_ref[...])
    hidden_ref[...] = hidden
    r = lax.rsqrt(jnp.mean(hidden * hidden, axis=1, keepdims=True) + EPS)
    routed = (hidden * r * gf_ref[...]).astype(BF16)
    slot = slot_ref[...]
    if m == 0:
        last_ref[...] = spread((slot,), (routed,), last_ref.shape[0])
    else:
        slot = slot + slot // cap * cap
        last_ref[...] = spread((slot, slot + cap), (cot_ref[0], routed), last_ref.shape[0])


def forward(m, slot, seg, tokens, cot, wq, wk, wv, wo, ga, gf, slots, cap, dep):
    _, n, d = tokens.shape
    shapes = [
        ((n, d), BF16), ((n, d), BF16), ((n, d), BF16), ((n, d), BF16), ((16, n), F32),
        ((n, d), BF16), ((n, d), F32), ((slots * (m + 1), d), BF16),
    ]
    mat = pl.BlockSpec((1, n, d), lambda i: (m, 0, 0))
    return pl.pallas_call(
        functools.partial(forward_kernel, m, cap),
        grid=(1,),
        in_specs=[
            full(1, n), full(*seg.shape), mat, mat,
            full(d, d), full(d, d), full(d, d), full(d, d), full(1, d), full(1, d), ANY,
        ],
        out_specs=[full(*s) for s, _ in shapes],
        out_shape=[jax.ShapeDtypeStruct(s, t) for s, t in shapes],
        scratch_shapes=[pltpu.VMEM((n, n), F32)],
        cost_estimate=cost(13.4),
        compiler_params=params(26),
    )(slot, seg, tokens, cot, wq, wk, wv, wo, ga, gf, dep)


BLOCK = 256
HALF = 128


def hidden_units(x, g, win, wout):
    pre = dot(x, win)
    sig = jax.nn.sigmoid(pre)
    soft = pre * sig
    slope = sig + soft * (1.0 - sig)
    return soft.astype(BF16), (dot(g, wout, 1, 1) * slope).astype(BF16)


def put_chunk(chunk_ref, gout, gin):
    for i in range(BLOCK // HALF):
        part = slice(i * HALF, (i + 1) * HALF)
        chunk_ref[pl.ds(2 * i * HALF, HALF), :] = gout[part].astype(BF16)
        chunk_ref[pl.ds((2 * i + 1) * HALF, HALF), :] = gin[part].astype(BF16)


def units_kernel(rx_ref, gx_ref, win_ref, wout_ref, *rest):
    act_ref, gpre_ref = rest[-2:]
    act_ref[...], gpre_ref[...] = hidden_units(
        rx_ref[...], gx_ref[...], win_ref[0], wout_ref[0]
    )


def split_units_kernel(cap, both_ref, win_ref, wout_ref, *rest):
    act_ref, gpre_ref, rx_ref, gx_ref = rest[-4:]

    @pl.when(pl.program_id(0) == 0)
    def _():
        for e in range(rx_ref.shape[0] // cap):
            mine = pl.ds(e * cap, cap)
            gx_ref[mine, :] = both_ref[pl.ds(2 * e * cap, cap), :]
            rx_ref[mine, :] = both_ref[pl.ds((2 * e + 1) * cap, cap), :]

    act_ref[...], gpre_ref[...] = hidden_units(
        rx_ref[...], gx_ref[...], win_ref[0], wout_ref[0]
    )


def expert_units(c, units, given, win, wout, dep, cap=None):
    d = win.shape[1]
    rows = given[0].shape[0] // (1 if cap is None else 2)
    f = BLOCK
    columns = pl.BlockSpec((rows, f), lambda i: (0, i))
    kernel = units_kernel if cap is None else functools.partial(split_units_kernel, cap)
    return pl.pallas_call(
        kernel,
        grid=(units,),
        in_specs=[full(*x.shape) for x in given]
        + [
            pl.BlockSpec((1, d, f), lambda i: (0, 0, c + i)),
            pl.BlockSpec((1, f, d), lambda i: (0, c + i, 0)),
            ANY,
        ],
        out_specs=[columns] * 2 + ([full(rows, d)] * 2 if cap else []),
        out_shape=[jax.ShapeDtypeStruct((rows, units * f), BF16)] * 2
        + ([jax.ShapeDtypeStruct((rows, d), BF16)] * 2 if cap else []),
        cost_estimate=cost(3 + units),
        compiler_params=params(20),
    )(*given, win, wout, dep)


def chunk_kernel(
    rx0_ref, rx1_ref, gx0_ref, gx1_ref, act0_ref, act1_ref, gpre0_ref, gpre1_ref, dep_ref,
    chunk_ref,
):
    put_chunk(
        chunk_ref,
        dot(act0_ref[...], gx0_ref[...], 0, 0) + dot(act1_ref[...], gx1_ref[...], 0, 0),
        dot(gpre0_ref[...], rx0_ref[...], 0, 0) + dot(gpre1_ref[...], rx1_ref[...], 0, 0),
    )


def expert_grads(units, rx, gx, acts, gpres, at, dep):
    rows, d = rx[0].shape
    f = BLOCK
    columns = [pl.BlockSpec((rows, f), lambda i, k=k: (0, k + i)) for k in at]
    return pl.pallas_call(
        chunk_kernel,
        grid=(units,),
        in_specs=[full(rows, d)] * 4 + columns * 2 + [ANY],
        out_specs=pl.BlockSpec((2 * f, d), lambda i: (i, 0)),
        out_shape=jax.ShapeDtypeStruct((units * 2 * f, d), BF16),
        cost_estimate=cost(0.5 + 1.5 * units),
        compiler_params=params(20),
    )(*rx, *gx, *acts, *gpres, dep)


def rows_kernel(side, *refs):
    *parts, w_ref, _, o_ref = refs
    total, start = None, 0
    for a_ref in parts:
        count = a_ref.shape[1]
        units = pl.ds(start, count)
        w = w_ref[0, :, units] if side == 1 else w_ref[0, units, :]
        term = dot(a_ref[...], w, 1, side)
        total = term if total is None else total + term
        start += count
    o_ref[...] = total.astype(BF16)


def back_rows(parts, w, side, dep, blk=256):
    rows = parts[0].shape[0]
    d = w.shape[1 + (1 - side)]
    return pl.pallas_call(
        functools.partial(rows_kernel, side),
        grid=(rows // blk,),
        in_specs=[pl.BlockSpec((blk, a.shape[1]), lambda i: (i, 0)) for a in parts]
        + [full(*w.shape), ANY],
        out_specs=pl.BlockSpec((blk, d), lambda i: (i, 0)),
        out_shape=jax.ShapeDtypeStruct((rows, d), BF16),
        cost_estimate=cost(4.5),
        compiler_params=params(16),
    )(*parts, w, dep)


def backward_kernel(
    m, slot_ref, seg_ref, tok_ref, cot_ref, back_ref, normed_ref, q_ref, k_ref, v_ref, lse_ref,
    hidden_ref, wq_ref, wk_ref, wv_ref, wo_ref, ga_ref, gf_ref, *rest,
):
    gtok_ref, gattn_ref, gq_ref, gk_ref, gv_ref, gain_ref, bias_ref, gm_ref, gh_ref = rest[-9:]
    n, d = normed_ref.shape
    slots = back_ref.shape[0]
    places = (iota((n, slots), 1) == to_column(slot_ref[...])).astype(BF16)
    grad_routed = dot(places, back_ref[...])
    hidden = hidden_ref[...]
    r = lax.rsqrt(jnp.mean(hidden * hidden, axis=1, keepdims=True) + EPS)
    unit = hidden * r
    g = grad_routed * gf_ref[...]
    grad_hidden = cot_ref[0].astype(F32) + r * (
        g - unit * jnp.mean(g * unit, axis=1, keepdims=True)
    )
    gh_ref[...] = grad_hidden
    gain_ref[pl.ds(1, 1), :] = jnp.sum(grad_routed * unit, axis=0, keepdims=True)
    grad_attn = grad_hidden.astype(BF16)
    gattn_ref[...] = grad_attn
    gm_ref[...] = dot(grad_attn, wo_ref[...], 1, 1).astype(BF16)
    bias_ref[...] = bias_of(seg_ref[pl.ds(m, 1), :])
    low = iota((n, PAIR), 1) < HEAD_DIM

    def pair(p, carry):
        cols = pl.ds(pl.multiple_of(p * PAIR, PAIR), PAIR)
        q, k, v, gm = q_ref[:, cols], k_ref[:, cols], v_ref[:, cols], gm_ref[:, cols]
        gqs, gks, gvs = [], [], []
        for h in range(2):
            mine = low if h == 0 else ~low
            s = dot(k, jnp.where(mine, q, 0), 1, 1) + bias_ref[...]
            probs = jnp.exp(s - lse_ref[pl.ds(2 * p + h, 1), :])
            gvs.append(dot(probs.astype(BF16), gm))
            gp = dot(v, jnp.where(mine, gm, 0), 1, 1)
            shared = jnp.sum(probs * gp, axis=0, keepdims=True)
            gs = (probs * (gp - shared)).astype(BF16)
            gks.append(dot(gs, q))
            gqs.append(dot(gs, k, 0, 0))
        gq_ref[:, cols] = (jnp.where(low, gqs[0], gqs[1]) * SCALE).astype(BF16)
        gk_ref[:, cols] = jnp.where(low, gks[0], gks[1]).astype(BF16)
        gv_ref[:, cols] = jnp.where(low, gvs[0], gvs[1]).astype(BF16)
        return carry

    lax.fori_loop(0, HEADS // 2, pair, 0)
    grad_normed = (
        dot(gq_ref[...], wq_ref[...], 1, 1)
        + dot(gk_ref[...], wk_ref[...], 1, 1)
        + dot(gv_ref[...], wv_ref[...], 1, 1)
    )
    x = tok_ref[0].astype(F32)
    r = lax.rsqrt(jnp.mean(x * x, axis=1, keepdims=True) + EPS)
    unit = x * r
    gain_ref[pl.ds(0, 1), :] = jnp.sum(grad_normed * unit, axis=0, keepdims=True)
    g = grad_normed * ga_ref[...]
    gtok_ref[0] = (
        gh_ref[...] + r * (g - unit * jnp.mean(g * unit, axis=1, keepdims=True))
    ).astype(BF16)


def backward(m, slot, seg, tokens, cot, back, saved, wq, wk, wv, wo, ga, gf, held, dep):
    micro, n, d = tokens.shape
    normed, q, k, v, lse, _, hidden = saved
    mat = pl.BlockSpec((1, n, d), lambda i: (m, 0, 0))
    extra = [dep] if held is None else [dep, held]
    return pl.pallas_call(
        functools.partial(backward_kernel, m),
        grid=(1,),
        in_specs=[full(1, n), full(*seg.shape), mat, mat, full(*back.shape)]
        + [full(*a.shape) for a in (normed, q, k, v, lse, hidden)]
        + [full(d, d)] * 4 + [full(1, d)] * 2 + [ANY] * len(extra),
        out_specs=[mat] + [full(n, d)] * 4 + [full(8, d)],
        out_shape=[jax.ShapeDtypeStruct((micro, n, d), BF16)]
        + [jax.ShapeDtypeStruct((n, d), BF16)] * 4
        + [jax.ShapeDtypeStruct((8, d), F32)],
        scratch_shapes=[
            pltpu.VMEM((n, n), F32), pltpu.VMEM((n, d), BF16), pltpu.VMEM((n, d), F32)
        ],
        cost_estimate=cost(17.5),
        compiler_params=params(36),
        input_output_aliases={} if held is None else {18: 0},
    )(slot, seg, tokens, cot, back, normed, q, k, v, lse, hidden, wq, wk, wv, wo, ga, gf, *extra)


def weights_kernel(n0, n1, x0, x1, q0, q1, k0, k1, v0, v1, a0, a1, gain0, gain1, dep_ref, o_ref):
    d = n0.shape[1]
    for i, (l0, l1, r0, r1) in enumerate(
        ((n0, n1, q0, q1), (n0, n1, k0, k1), (n0, n1, v0, v1), (x0, x1, a0, a1))
    ):
        both = dot(l0[...], r0[...], 0, 0) + dot(l1[...], r1[...], 0, 0)
        o_ref[pl.ds(i * d, d), :] = both.astype(BF16)
    rest = o_ref.shape[0] - 4 * d
    line = iota((rest, d), 0)
    gain = gain0[...] + gain1[...]
    o_ref[pl.ds(4 * d, rest), :] = jnp.where(
        line == 0, gain[0:1, :], jnp.where(line == 1, gain[1:2, :], 0.0)
    ).astype(BF16)


def dense_grads(saved, grads, rest, dep):
    n, d = saved[0][0].shape
    pairs = [(saved[0][0], saved[1][0]), (saved[0][5], saved[1][5])]
    pairs += [(grads[0][i], grads[1][i]) for i in (1, 2, 3, 0, 4)]
    flat = [a for both in pairs for a in both]
    return pl.pallas_call(
        weights_kernel,
        grid=(1,),
        in_specs=[full(*a.shape) for a in flat] + [ANY],
        out_specs=full(4 * d + rest, d),
        out_shape=jax.ShapeDtypeStruct((4 * d + rest, d), BF16),
        cost_estimate=cost(10.3),
        compiler_params=params(36),
    )(*flat, dep)


def output_kernel(s0_ref, s1_ref, b0_ref, b1_ref, h0_ref, h1_ref, dep_ref, o_ref):
    n = o_ref.shape[1]
    for m, (s_ref, b_ref, h_ref) in enumerate(((s0_ref, b0_ref, h0_ref), (s1_ref, b1_ref, h1_ref))):
        places = (iota((n, b_ref.shape[0]), 1) == to_column(s_ref[...])).astype(BF16)
        o_ref[m] = (h_ref[...] + dot(places, b_ref[...])).astype(BF16)


def block_output(slots, backs, hiddens, dep):
    micro = len(slots)
    n, d = hiddens[0].shape
    flat = [*slots, *backs, *hiddens]
    return pl.pallas_call(
        output_kernel,
        grid=(1,),
        in_specs=[full(*a.shape) for a in flat] + [ANY],
        out_specs=full(micro, n, d),
        out_shape=jax.ShapeDtypeStruct((micro, n, d), BF16),
        cost_estimate=cost(4.4),
        compiler_params=params(16),
    )(*flat, dep)


def after(x, dep):
    return lax.optimization_barrier((x, dep))[0]


def add(a, b, dep):
    return (after(a, dep).astype(F32) + b.astype(F32)).astype(BF16)


def store_kernel(flag_ref, a_ref, b_ref, *rest):
    gin_ref, gout_ref, token_ref = rest[-3:]
    token_ref[...] = jnp.zeros_like(token_ref)

    def put(ref):
        gout_ref[0] = ref[pl.ds(0, HALF), :].astype(F32)
        gin_ref[0] = ref[pl.ds(HALF, HALF), :].astype(F32).T

    @pl.when(flag_ref[0] == 1)
    def _():
        put(b_ref)

    @pl.when(flag_ref[0] != 1)
    def _():
        put(a_ref)


def store(c, flag, a, b, ff, held, dep):
    rows, d = a.shape
    spec = pl.BlockSpec((2 * HALF, d), lambda i: (i, 0))
    base = c * (BLOCK // HALF)
    extra = ([] if held is None else list(held)) + [dep]
    return pl.pallas_call(
        store_kernel,
        grid=(rows // (2 * HALF),),
        in_specs=[pl.BlockSpec(memory_space=pltpu.SMEM), spec, spec] + [ANY] * len(extra),
        out_specs=[
            pl.BlockSpec((1, d, HALF), lambda i: (0, 0, base + i)),
            pl.BlockSpec((1, HALF, d), lambda i: (0, base + i, 0)),
            full(8, 128),
        ],
        out_shape=[
            jax.ShapeDtypeStruct((1, d, ff), F32),
            jax.ShapeDtypeStruct((1, ff, d), F32),
            jax.ShapeDtypeStruct((8, 128), F32),
        ],
        input_output_aliases={} if held is None else {3: 0, 4: 1},
        cost_estimate=cost(0.8 + rows / 480),
        compiler_params=params(6),
    )(flag, a, b, *extra)


SIZES = (1, 1, 1, 1, 1, 1, 1, 1, 1, 1, 1, 1)


PLAN = (
    ("F", 0), ("Q1", 0), ("Fa", 1), ("D", 0), ("S1", 0), ("Fb", 1), ("D", 1), ("S1", 1), ("D", 2),
    ("D", 3), ("G1", 0), ("Q1", 1), ("S1", 2), ("D", 4), ("G1", 1), ("D", 5), ("S1", 3), ("G2", 0),
    ("B", 0), ("G1", 2), ("G2", 1), ("S1", 4), ("G1", 3), ("B", 1), ("S1", 5), ("G2", 2), ("G1", 4),
    ("W", 0), ("D", 6), ("G2", 3), ("S1", 6), ("G1", 5), ("G2", 4), ("D", 7), ("S1", 7), ("D", 8),
    ("G3", 0), ("G1", 6), ("G2", 5), ("G1", 7), ("S1", 8), ("G2", 6), ("D", 9), ("S1", 9), ("D",
    10), ("A2", 0), ("G3", 1), ("G2", 7), ("G1", 8), ("Q2", 1), ("S1", 10), ("G3", 2), ("G1", 9),
    ("G2", 8), ("D", 11), ("G3", 3), ("G3", 4), ("G1", 10), ("S1", 11), ("G3", 5), ("G2", 9), ("G3",
    6), ("G3", 7), ("A3", 0), ("G1", 11), ("G2", 10), ("Q2", 0), ("G2", 11), ("O", 0), ("G3", 8),
    ("G3", 9), ("G3", 10), ("G3", 11),
)


def per_device(
    tokens, cotangent, token_ids, hash_table, segment_ids, query_weight, key_weight,
    value_weight, output_weight, gain_attn, gain_ffn, expert_in, expert_out,
):
    micro, n, d = tokens.shape
    ff = expert_in.shape[2]
    owners = lax.axis_size("expert")
    depth = lax.axis_size("dp")
    cap = 2 * n // owners
    weights = (query_weight, key_weight, value_weight, output_weight)
    gains = (gain_attn.reshape(1, d), gain_ffn.reshape(1, d))
    place = lax.axis_index("dp")
    outer = ((place == 0) | (place == depth - 1)).astype(jnp.int32).reshape(1)
    size = hash_table.shape[0]
    table_rows = -(-size // 1024) * 8
    table = jnp.pad(hash_table, (0, table_rows * 128 - size)).reshape(table_rows, 128)

    def swap(x):
        return lax.all_to_all(x, "expert", split_axis=0, concat_axis=0, tiled=True)

    slot0, slot1, packed = route(token_ids, table, cotangent, owners, cap)
    slots = (slot0, slot1)
    gx = {0: swap(packed)}
    *kept0, packed0 = forward(
        0, slot0, segment_ids, tokens, cotangent, *weights, *gains, owners * cap, cap, packed
    )
    rx = {0: swap(after(packed0, gx[0]))}
    *kept1, packed1 = forward(
        1, slot1, segment_ids, tokens, cotangent, *weights, *gains, owners * cap, cap, packed0
    )
    both = swap(after(packed1, rx[0]))
    saved = (tuple(kept0), tuple(kept1))
    dep = packed1

    starts = [sum(SIZES[:i]) for i in range(len(SIZES))]
    chunk, hop1, hop2, hop3, sum1, total = {}, {}, {}, {}, {}, {}
    stored = gtok = dense = block_out = None
    backs, results, grads = {}, {}, {}
    for op, c in PLAN:
        if op == "F":
            act0, gpre0 = expert_units(0, ff // BLOCK, (rx[0], gx[0]), expert_in, expert_out, dep)
            dep = act0
        elif op == "Fa":
            acta, gprea, rx[1], gx[1] = expert_units(
                0, SIZES[0], (both,), expert_in, expert_out, dep, cap
            )
            dep = rx[1]
        elif op == "Fb":
            actb, gpreb = expert_units(
                SIZES[0], ff // BLOCK - SIZES[0], (rx[1], gx[1]), expert_in, expert_out, dep
            )
            dep = actb
        elif op == "D":
            mine = (acta, gprea) if c == 0 else (actb, gpreb)
            at = (starts[c], 0 if c == 0 else starts[c] - SIZES[0])
            dep = chunk[c] = expert_grads(
                SIZES[c], (rx[0], rx[1]), (gx[0], gx[1]), (act0, mine[0]), (gpre0, mine[1]), at,
                dep,
            )
        elif op == "S1":
            x = after(chunk[c], dep)
            hop1[c] = lax.ppermute(x, "dp", [(0, 1), (3, 2)]) if depth == 4 else x
        elif op == "G1":
            if depth == 4:
                sum1[c] = add(chunk[c], hop1[c], dep)
                hop2[c] = lax.ppermute(sum1[c], "dp", [(1, 2), (2, 1)])
                dep = sum1[c]
        elif op == "G2":
            if depth == 4:
                total[c] = add(sum1[c], hop2[c], dep)
                hop3[c] = lax.ppermute(total[c], "dp", [(1, 0), (2, 3)])
                dep = total[c]
            else:
                total[c] = hop3[c] = lax.psum(hop1[c], "dp")
        elif op == "G3":
            *stored, dep = store(starts[c], outer, total[c], hop3[c], ff, stored, dep)
        elif op == "Q1":
            dep = back_rows((gpre0,) if c == 0 else (gprea, gpreb), expert_in, 1, dep)
            backs[c] = swap(dep)
        elif op == "Q2":
            dep = back_rows((act0,) if c == 0 else (acta, actb), expert_out, 0, dep)
            results[c] = swap(dep)
        elif op == "B":
            gtok, *grads[c] = backward(
                c, slots[c], segment_ids, tokens, cotangent, backs[c], saved[c], *weights,
                *gains, gtok, dep,
            )
            dep = grads[c][0]
        elif op == "W":
            dep = dense_grads(saved, grads, 16 * owners, dep)
            dense = lax.psum_scatter(dep, "expert", scatter_dimension=0, tiled=True)
        elif op == "A2":
            dense = lax.psum(after(dense, dep), "dp")
        elif op == "A3":
            dense = lax.all_gather(after(dense, dep), "expert", axis=0, tiled=True)
        elif op == "O":
            block_out = block_output(
                slots, [results[m] for m in range(micro)], [s[6] for s in saved], dep
            )
            dep = block_out
    wide = dense.astype(F32)
    return (
        block_out,
        gtok,
        *(wide[i * d : (i + 1) * d] for i in range(4)),
        wide[4 * d],
        wide[4 * d + 1],
        *stored,
    )


def solution(mesh):
    blocks, ids = P(None, ("dp", "expert"), None), P(None, ("dp", "expert"))
    owned = P("expert", None, None)
    return jax.shard_map(
        per_device,
        mesh=mesh,
        in_specs=(blocks, blocks, ids, P(), ids, P(), P(), P(), P(), P(), P(), owned, owned),
        out_specs=(blocks, blocks, P(), P(), P(), P(), P(), P(), owned, owned),
        check_vma=False,
    )
```

```python
import functools

import jax
import jax.numpy as jnp
from jax import lax
from jax.experimental import pallas as pl
from jax.experimental.pallas import tpu as pltpu
from jax.sharding import PartitionSpec as P

HEADS = 12
HEAD_DIM = 64
EPS = 1e-05
SCALE = HEAD_DIM ** (-0.5)
PAIR = 2 * HEAD_DIM
F32 = jnp.float32
BF16 = jnp.bfloat16


def dot(a, b, ca=1, cb=0):
    return lax.dot_general(a, b, (((ca,), (cb,)), ((), ())), preferred_element_type=F32)


def params():
    return pltpu.CompilerParams(
        dimension_semantics=("arbitrary",), vmem_limit_bytes=60 * 1024 * 1024
    )


PACE = [100.0, 8.0]


def cost(us):
    return pl.CostEstimate(
        flops=int(us * PACE[0] * 1.15e9), bytes_accessed=int(us * 3.0e6), transcendentals=0
    )


def full(*shape):
    return pl.BlockSpec(shape, lambda *_: (0,) * len(shape))


ANY = pl.BlockSpec(memory_space=pl.ANY)


def iota(shape, axis):
    return lax.broadcasted_iota(jnp.int32, shape, axis)


def to_column(row):
    n = row.shape[1]
    eye = iota((n, n), 0) == iota((n, n), 1)
    return jnp.sum(jnp.where(eye, row, 0), axis=1, keepdims=True)


def spread(slots, values, count):
    total = None
    for slot, value in zip(slots, values):
        places = (iota((count, slot.shape[1]), 0) == slot).astype(BF16)
        part = dot(places, value)
        total = part if total is None else total + part
    return total.astype(BF16)


def route_kernel(owners, cap, ids_ref, table_ref, cot_ref, slot0_ref, slot1_ref, pack_ref):
    micro, n = ids_ref.shape
    rows = table_ref.shape[0]
    table = table_ref[...].astype(BF16)
    kinds = -(-owners // 16) * 16
    before = (iota((n, n), 0) < iota((n, n), 1)).astype(BF16)
    slots = []
    for m, slot_ref in enumerate((slot0_ref, slot1_ref)):
        ids = ids_ref[pl.ds(m, 1), :]
        pick = (iota((rows, n), 0) == (ids >> 7)).astype(BF16)
        values = dot(table, pick, 0, 0)
        lane = ids & 127
        expert = jnp.sum(
            jnp.where(iota((128, n), 0) == lane, values, 0.0), axis=0, keepdims=True
        )
        named = iota((kinds, n), 0).astype(F32) == expert
        counts = dot(named.astype(BF16), before)
        rank = jnp.sum(jnp.where(named, counts, 0.0), axis=0, keepdims=True)
        slot = (expert * cap + rank).astype(jnp.int32)
        slot_ref[...] = slot
        slots.append(slot)
    pack_ref[...] = spread(slots[:1], (cot_ref[0],), pack_ref.shape[0])


def route(ids, table, cot, owners, cap):
    micro, n = ids.shape
    width = cot.shape[2]
    rows = table.shape[0]
    return pl.pallas_call(
        functools.partial(route_kernel, owners, cap),
        grid=(1,),
        in_specs=[full(micro, n), full(rows, 128), full(1, n, width)],
        out_specs=[full(1, n), full(1, n), full(owners * cap, width)],
        out_shape=[
            jax.ShapeDtypeStruct((1, n), jnp.int32),
            jax.ShapeDtypeStruct((1, n), jnp.int32),
            jax.ShapeDtypeStruct((owners * cap, width), BF16),
        ],
        cost_estimate=cost(5.0),
        compiler_params=params(),
    )(ids, table, cot)


def bias_of(seg):
    n = seg.shape[1]
    key, query = iota((n, n), 0), iota((n, n), 1)
    seen = (key <= query) & (to_column(seg) == seg)
    return jnp.where(seen, 0.0, -1e30)


def forward_kernel(
    m, cap, slot_ref, seg_ref, tok_ref, cot_ref, wq_ref, wk_ref, wv_ref, wo_ref, ga_ref, gf_ref,
    dep_ref, normed_ref, q_ref, k_ref, v_ref, lse_ref, mixed_ref, hidden_ref, last_ref, bias_ref,
):
    x = tok_ref[0].astype(F32)
    n = x.shape[0]
    r = lax.rsqrt(jnp.mean(x * x, axis=1, keepdims=True) + EPS)
    normed = (x * r * ga_ref[...]).astype(BF16)
    normed_ref[...] = normed
    q_ref[...] = (dot(normed, wq_ref[...]).astype(BF16) * SCALE).astype(BF16)
    k_ref[...] = dot(normed, wk_ref[...]).astype(BF16)
    v_ref[...] = dot(normed, wv_ref[...]).astype(BF16)
    bias_ref[...] = bias_of(seg_ref[pl.ds(m, 1), :])
    low = iota((n, PAIR), 1) < HEAD_DIM

    def pair(p, carry):
        cols = pl.ds(pl.multiple_of(p * PAIR, PAIR), PAIR)
        q, k, v = q_ref[:, cols], k_ref[:, cols], v_ref[:, cols]
        parts = []
        for h in range(2):
            mine = low if h == 0 else ~low
            s = dot(k, jnp.where(mine, q, 0), 1, 1) + bias_ref[...]
            top = jnp.max(s, axis=0, keepdims=True)
            e = jnp.exp(s - top)
            total = jnp.sum(e, axis=0, keepdims=True)
            lse_ref[pl.ds(2 * p + h, 1), :] = top + jnp.log(total)
            probs = (e * (1.0 / total)).astype(BF16)
            parts.append(dot(probs, v, 0, 0))
        mixed_ref[:, cols] = jnp.where(low, parts[0], parts[1]).astype(BF16)
        return carry

    lax.fori_loop(0, HEADS // 2, pair, 0)
    hidden = x + dot(mixed_ref[...], wo_ref[...])
    hidden_ref[...] = hidden
    r = lax.rsqrt(jnp.mean(hidden * hidden, axis=1, keepdims=True) + EPS)
    routed = (hidden * r * gf_ref[...]).astype(BF16)
    slot = slot_ref[...]
    if m == 0:
        last_ref[...] = spread((slot,), (routed,), last_ref.shape[0])
    else:
        slot = slot + slot // cap * cap
        last_ref[...] = spread((slot, slot + cap), (cot_ref[0], routed), last_ref.shape[0])


def forward(m, slot, seg, tokens, cot, wq, wk, wv, wo, ga, gf, slots, cap, dep):
    _, n, d = tokens.shape
    shapes = [
        ((n, d), BF16), ((n, d), BF16), ((n, d), BF16), ((n, d), BF16), ((16, n), F32),
        ((n, d), BF16), ((n, d), F32), ((slots * (m + 1), d), BF16),
    ]
    mat = pl.BlockSpec((1, n, d), lambda i: (m, 0, 0))
    return pl.pallas_call(
        functools.partial(forward_kernel, m, cap),
        grid=(1,),
        in_specs=[
            full(1, n), full(*seg.shape), mat, mat,
            full(d, d), full(d, d), full(d, d), full(d, d), full(1, d), full(1, d), ANY,
        ],
        out_specs=[full(*s) for s, _ in shapes],
        out_shape=[jax.ShapeDtypeStruct(s, t) for s, t in shapes],
        scratch_shapes=[pltpu.VMEM((n, n), F32)],
        cost_estimate=cost(13.4),
        compiler_params=params(),
    )(slot, seg, tokens, cot, wq, wk, wv, wo, ga, gf, dep)


BLOCK = 256
HALF = 128


def hidden_units(x, g, win, wout):
    pre = dot(x, win)
    sig = jax.nn.sigmoid(pre)
    soft = pre * sig
    slope = sig + soft * (1.0 - sig)
    return soft.astype(BF16), (dot(g, wout, 1, 1) * slope).astype(BF16)


def put_chunk(chunk_ref, at, gout, gin):
    for i in range(BLOCK // HALF):
        part = slice(i * HALF, (i + 1) * HALF)
        chunk_ref[pl.ds(at + 2 * i * HALF, HALF), :] = gout[part].astype(BF16)
        chunk_ref[pl.ds(at + (2 * i + 1) * HALF, HALF), :] = gin[part].astype(BF16)


def units_kernel(rx_ref, gx_ref, win_ref, wout_ref, *rest):
    act_ref, gpre_ref = rest[-2:]
    act_ref[...], gpre_ref[...] = hidden_units(
        rx_ref[...], gx_ref[...], win_ref[0], wout_ref[0]
    )


def split_units_kernel(cap, both_ref, win_ref, wout_ref, *rest):
    act_ref, gpre_ref, rx_ref, gx_ref = rest[-4:]

    @pl.when(pl.program_id(0) == 0)
    def _():
        for e in range(rx_ref.shape[0] // cap):
            mine = pl.ds(e * cap, cap)
            gx_ref[mine, :] = both_ref[pl.ds(2 * e * cap, cap), :]
            rx_ref[mine, :] = both_ref[pl.ds((2 * e + 1) * cap, cap), :]

    act_ref[...], gpre_ref[...] = hidden_units(
        rx_ref[...], gx_ref[...], win_ref[0], wout_ref[0]
    )


def expert_units(c, units, given, win, wout, dep, cap=None):
    d = win.shape[1]
    rows = given[0].shape[0] // (1 if cap is None else 2)
    f = BLOCK
    columns = pl.BlockSpec((rows, f), lambda i: (0, i))
    kernel = units_kernel if cap is None else functools.partial(split_units_kernel, cap)
    return pl.pallas_call(
        kernel,
        grid=(units,),
        in_specs=[full(*x.shape) for x in given]
        + [
            pl.BlockSpec((1, d, f), lambda i: (0, 0, c + i)),
            pl.BlockSpec((1, f, d), lambda i: (0, c + i, 0)),
            ANY,
        ],
        out_specs=[columns] * 2 + ([full(rows, d)] * 2 if cap else []),
        out_shape=[jax.ShapeDtypeStruct((rows, units * f), BF16)] * 2
        + ([jax.ShapeDtypeStruct((rows, d), BF16)] * 2 if cap else []),
        cost_estimate=cost(3 + units),
        compiler_params=params(),
    )(*given, win, wout, dep)


def chunk_kernel(
    sizes, rx0_ref, rx1_ref, gx0_ref, gx1_ref, act0_ref, act1_ref, gpre0_ref, gpre1_ref, dep_ref,
    *chunk_refs,
):
    gout = dot(act0_ref[...], gx0_ref[...], 0, 0) + dot(act1_ref[...], gx1_ref[...], 0, 0)
    gin = dot(gpre0_ref[...], rx0_ref[...], 0, 0) + dot(gpre1_ref[...], rx1_ref[...], 0, 0)
    step = 0
    for size, ref in zip(sizes, chunk_refs):
        for i in range(size):

            @pl.when(pl.program_id(0) == step)
            def _(ref=ref, i=i):
                put_chunk(ref, 2 * BLOCK * i, gout, gin)

            step += 1


def expert_grads(sizes, rx, gx, acts, gpres, at, dep):
    rows, d = rx[0].shape
    f = BLOCK
    columns = [pl.BlockSpec((rows, f), lambda i, k=k: (0, k + i)) for k in at]
    shapes = [(size * 2 * f, d) for size in sizes]
    return pl.pallas_call(
        functools.partial(chunk_kernel, sizes),
        grid=(sum(sizes),),
        in_specs=[full(rows, d)] * 4 + columns * 2 + [ANY],
        out_specs=[full(*x) for x in shapes],
        out_shape=[jax.ShapeDtypeStruct(x, BF16) for x in shapes],
        cost_estimate=cost(3.7 + 1.5 * sum(sizes)),
        compiler_params=params(),
    )(*rx, *gx, *acts, *gpres, dep)


def rows_kernel(side, *refs):
    *parts, w_ref, _, o_ref = refs
    total, start = None, 0
    for a_ref in parts:
        count = a_ref.shape[1]
        units = pl.ds(start, count)
        w = w_ref[0, :, units] if side == 1 else w_ref[0, units, :]
        term = dot(a_ref[...], w, 1, side)
        total = term if total is None else total + term
        start += count
    o_ref[...] = total.astype(BF16)


def back_rows(parts, w, side, dep, blk=256):
    rows = parts[0].shape[0]
    d = w.shape[1 + (1 - side)]
    return pl.pallas_call(
        functools.partial(rows_kernel, side),
        grid=(rows // blk,),
        in_specs=[pl.BlockSpec((blk, a.shape[1]), lambda i: (i, 0)) for a in parts]
        + [full(*w.shape), ANY],
        out_specs=pl.BlockSpec((blk, d), lambda i: (i, 0)),
        out_shape=jax.ShapeDtypeStruct((rows, d), BF16),
        cost_estimate=cost(4.5),
        compiler_params=params(),
    )(*parts, w, dep)


def backward_kernel(
    m, slot_ref, seg_ref, tok_ref, cot_ref, back_ref, normed_ref, q_ref, k_ref, v_ref, lse_ref,
    hidden_ref, wq_ref, wk_ref, wv_ref, wo_ref, ga_ref, gf_ref, *rest,
):
    gtok_ref, gattn_ref, gq_ref, gk_ref, gv_ref, gain_ref, bias_ref, gm_ref, gh_ref = rest[-9:]
    n, d = normed_ref.shape
    slots = back_ref.shape[0]
    places = (iota((n, slots), 1) == to_column(slot_ref[...])).astype(BF16)
    grad_routed = dot(places, back_ref[...])
    hidden = hidden_ref[...]
    r = lax.rsqrt(jnp.mean(hidden * hidden, axis=1, keepdims=True) + EPS)
    unit = hidden * r
    g = grad_routed * gf_ref[...]
    grad_hidden = cot_ref[0].astype(F32) + r * (
        g - unit * jnp.mean(g * unit, axis=1, keepdims=True)
    )
    gh_ref[...] = grad_hidden
    gain_ref[pl.ds(1, 1), :] = jnp.sum(grad_routed * unit, axis=0, keepdims=True)
    grad_attn = grad_hidden.astype(BF16)
    gattn_ref[...] = grad_attn
    gm_ref[...] = dot(grad_attn, wo_ref[...], 1, 1).astype(BF16)
    bias_ref[...] = bias_of(seg_ref[pl.ds(m, 1), :])
    low = iota((n, PAIR), 1) < HEAD_DIM

    def pair(p, carry):
        cols = pl.ds(pl.multiple_of(p * PAIR, PAIR), PAIR)
        q, k, v, gm = q_ref[:, cols], k_ref[:, cols], v_ref[:, cols], gm_ref[:, cols]
        gqs, gks, gvs = [], [], []
        for h in range(2):
            mine = low if h == 0 else ~low
            s = dot(k, jnp.where(mine, q, 0), 1, 1) + bias_ref[...]
            probs = jnp.exp(s - lse_ref[pl.ds(2 * p + h, 1), :])
            gvs.append(dot(probs.astype(BF16), gm))
            gp = dot(v, jnp.where(mine, gm, 0), 1, 1)
            shared = jnp.sum(probs * gp, axis=0, keepdims=True)
            gs = (probs * (gp - shared)).astype(BF16)
            gks.append(dot(gs, q))
            gqs.append(dot(gs, k, 0, 0))
        gq_ref[:, cols] = (jnp.where(low, gqs[0], gqs[1]) * SCALE).astype(BF16)
        gk_ref[:, cols] = jnp.where(low, gks[0], gks[1]).astype(BF16)
        gv_ref[:, cols] = jnp.where(low, gvs[0], gvs[1]).astype(BF16)
        return carry

    lax.fori_loop(0, HEADS // 2, pair, 0)
    grad_normed = (
        dot(gq_ref[...], wq_ref[...], 1, 1)
        + dot(gk_ref[...], wk_ref[...], 1, 1)
        + dot(gv_ref[...], wv_ref[...], 1, 1)
    )
    x = tok_ref[0].astype(F32)
    r = lax.rsqrt(jnp.mean(x * x, axis=1, keepdims=True) + EPS)
    unit = x * r
    gain_ref[pl.ds(0, 1), :] = jnp.sum(grad_normed * unit, axis=0, keepdims=True)
    g = grad_normed * ga_ref[...]
    gtok_ref[0] = (
        gh_ref[...] + r * (g - unit * jnp.mean(g * unit, axis=1, keepdims=True))
    ).astype(BF16)


def backward(m, slot, seg, tokens, cot, back, saved, wq, wk, wv, wo, ga, gf, held, dep):
    micro, n, d = tokens.shape
    normed, q, k, v, lse, _, hidden = saved
    mat = pl.BlockSpec((1, n, d), lambda i: (m, 0, 0))
    extra = [dep] if held is None else [dep, held]
    return pl.pallas_call(
        functools.partial(backward_kernel, m),
        grid=(1,),
        in_specs=[full(1, n), full(*seg.shape), mat, mat, full(*back.shape)]
        + [full(*a.shape) for a in (normed, q, k, v, lse, hidden)]
        + [full(d, d)] * 4 + [full(1, d)] * 2 + [ANY] * len(extra),
        out_specs=[mat] + [full(n, d)] * 4 + [full(8, d)],
        out_shape=[jax.ShapeDtypeStruct((micro, n, d), BF16)]
        + [jax.ShapeDtypeStruct((n, d), BF16)] * 4
        + [jax.ShapeDtypeStruct((8, d), F32)],
        scratch_shapes=[
            pltpu.VMEM((n, n), F32), pltpu.VMEM((n, d), BF16), pltpu.VMEM((n, d), F32)
        ],
        cost_estimate=cost(17.5),
        compiler_params=params(),
        input_output_aliases={} if held is None else {18: 0},
    )(slot, seg, tokens, cot, back, normed, q, k, v, lse, hidden, wq, wk, wv, wo, ga, gf, *extra)


def weights_kernel(n0, n1, x0, x1, q0, q1, k0, k1, v0, v1, a0, a1, gain0, gain1, dep_ref, o_ref):
    d = n0.shape[1]
    for i, (l0, l1, r0, r1) in enumerate(
        ((n0, n1, q0, q1), (n0, n1, k0, k1), (n0, n1, v0, v1), (x0, x1, a0, a1))
    ):
        both = dot(l0[...], r0[...], 0, 0) + dot(l1[...], r1[...], 0, 0)
        o_ref[pl.ds(i * d, d), :] = both.astype(BF16)
    rest = o_ref.shape[0] - 4 * d
    line = iota((rest, d), 0)
    gain = gain0[...] + gain1[...]
    o_ref[pl.ds(4 * d, rest), :] = jnp.where(
        line == 0, gain[0:1, :], jnp.where(line == 1, gain[1:2, :], 0.0)
    ).astype(BF16)


def dense_grads(saved, grads, rest, dep):
    n, d = saved[0][0].shape
    pairs = [(saved[0][0], saved[1][0]), (saved[0][5], saved[1][5])]
    pairs += [(grads[0][i], grads[1][i]) for i in (1, 2, 3, 0, 4)]
    flat = [a for both in pairs for a in both]
    return pl.pallas_call(
        weights_kernel,
        grid=(1,),
        in_specs=[full(*a.shape) for a in flat] + [ANY],
        out_specs=full(4 * d + rest, d),
        out_shape=jax.ShapeDtypeStruct((4 * d + rest, d), BF16),
        cost_estimate=cost(10.3),
        compiler_params=params(),
    )(*flat, dep)


def output_kernel(s0_ref, s1_ref, b0_ref, b1_ref, h0_ref, h1_ref, dep_ref, o_ref):
    n = o_ref.shape[1]
    for m, (s_ref, b_ref, h_ref) in enumerate(((s0_ref, b0_ref, h0_ref), (s1_ref, b1_ref, h1_ref))):
        places = (iota((n, b_ref.shape[0]), 1) == to_column(s_ref[...])).astype(BF16)
        o_ref[m] = (h_ref[...] + dot(places, b_ref[...])).astype(BF16)


def block_output(slots, backs, hiddens, dep):
    micro = len(slots)
    n, d = hiddens[0].shape
    flat = [*slots, *backs, *hiddens]
    return pl.pallas_call(
        output_kernel,
        grid=(1,),
        in_specs=[full(*a.shape) for a in flat] + [ANY],
        out_specs=full(micro, n, d),
        out_shape=jax.ShapeDtypeStruct((micro, n, d), BF16),
        cost_estimate=cost(4.4),
        compiler_params=params(),
    )(*flat, dep)


def after(x, dep):
    return lax.optimization_barrier((x, dep))[0]


def add(a, b, dep):
    return (after(a, dep).astype(F32) + b.astype(F32)).astype(BF16)


def store_kernel(flag_ref, a_ref, b_ref, *rest):
    gin_ref, gout_ref, token_ref = rest[-3:]
    token_ref[...] = jnp.zeros_like(token_ref)

    def put(ref):
        gout_ref[0] = ref[pl.ds(0, HALF), :].astype(F32)
        gin_ref[0] = ref[pl.ds(HALF, HALF), :].astype(F32).T

    @pl.when(flag_ref[0] == 1)
    def _():
        put(b_ref)

    @pl.when(flag_ref[0] != 1)
    def _():
        put(a_ref)


def store(c, flag, a, b, ff, held, dep):
    rows, d = a.shape
    spec = pl.BlockSpec((2 * HALF, d), lambda i: (i, 0))
    base = c * (BLOCK // HALF)
    extra = ([] if held is None else list(held)) + [dep]
    return pl.pallas_call(
        store_kernel,
        grid=(rows // (2 * HALF),),
        in_specs=[pl.BlockSpec(memory_space=pltpu.SMEM), spec, spec] + [ANY] * len(extra),
        out_specs=[
            pl.BlockSpec((1, d, HALF), lambda i: (0, 0, base + i)),
            pl.BlockSpec((1, HALF, d), lambda i: (0, base + i, 0)),
            full(8, 128),
        ],
        out_shape=[
            jax.ShapeDtypeStruct((1, d, ff), F32),
            jax.ShapeDtypeStruct((1, ff, d), F32),
            jax.ShapeDtypeStruct((8, 128), F32),
        ],
        input_output_aliases={} if held is None else {3: 0, 4: 1},
        cost_estimate=cost(0.8 + rows / 480),
        compiler_params=params(),
    )(flag, a, b, *extra)


SIZES = (1, 1, 2, 2, 2, 2, 1, 1)
GROUPS = ((0,), (1, 2), (3, 4, 5, 6, 7))


PLAN = (
    ("F", 0), ("Fa", 1), ("D", 0), ("S1", 0), ("Fb", 1), ("D", 1), ("S1", 1), ("S1", 2), ("Q1", 0),
    ("G1", 0), ("D", 2), ("G1", 1), ("Q1", 1), ("S1", 3), ("G1", 2), ("G2", 0), ("B", 0), ("G2", 1),
    ("G1", 3), ("S1", 4), ("G2", 2), ("B", 1), ("W", 0), ("S1", 5), ("G1", 4), ("G3", 0), ("G2", 3),
    ("G1", 5), ("S1", 6), ("G2", 4), ("G3", 1), ("S1", 7), ("A2", 0), ("Q2", 0), ("G2", 5), ("G1",
    6), ("Q2", 1), ("G3", 2), ("G2", 6), ("G1", 7), ("A3", 0), ("G2", 7), ("G3", 3), ("O", 0),
    ("G3", 4), ("G3", 5), ("G3", 6), ("G3", 7),
)


def per_device(
    tokens, cotangent, token_ids, hash_table, segment_ids, query_weight, key_weight,
    value_weight, output_weight, gain_attn, gain_ffn, expert_in, expert_out,
):
    micro, n, d = tokens.shape
    ff = expert_in.shape[2]
    owners = lax.axis_size("expert")
    depth = lax.axis_size("dp")
    cap = 2 * n // owners
    weights = (query_weight, key_weight, value_weight, output_weight)
    gains = (gain_attn.reshape(1, d), gain_ffn.reshape(1, d))
    place = lax.axis_index("dp")
    outer = ((place == 0) | (place == depth - 1)).astype(jnp.int32).reshape(1)
    size = hash_table.shape[0]
    table_rows = -(-size // 1024) * 8
    table = jnp.pad(hash_table, (0, table_rows * 128 - size)).reshape(table_rows, 128)

    def swap(x):
        return lax.all_to_all(x, "expert", split_axis=0, concat_axis=0, tiled=True)

    slot0, slot1, packed = route(token_ids, table, cotangent, owners, cap)
    slots = (slot0, slot1)
    gx = {0: swap(packed)}
    *kept0, packed0 = forward(
        0, slot0, segment_ids, tokens, cotangent, *weights, *gains, owners * cap, cap, packed
    )
    rx = {0: swap(after(packed0, gx[0]))}
    *kept1, packed1 = forward(
        1, slot1, segment_ids, tokens, cotangent, *weights, *gains, owners * cap, cap, packed0
    )
    both = swap(after(packed1, rx[0]))
    saved = (tuple(kept0), tuple(kept1))
    dep = packed1

    starts = [sum(SIZES[:i]) for i in range(len(SIZES))]
    chunk, hop1, hop2, hop3, sum1, total = {}, {}, {}, {}, {}, {}
    stored = gtok = dense = block_out = None
    backs, results, grads = {}, {}, {}
    for op, c in PLAN:
        if op == "F":
            act0, gpre0 = expert_units(0, ff // BLOCK, (rx[0], gx[0]), expert_in, expert_out, dep)
            dep = act0
        elif op == "Fa":
            acta, gprea, rx[1], gx[1] = expert_units(
                0, SIZES[0], (both,), expert_in, expert_out, dep, cap
            )
            dep = rx[1]
        elif op == "Fb":
            actb, gpreb = expert_units(
                SIZES[0], ff // BLOCK - SIZES[0], (rx[1], gx[1]), expert_in, expert_out, dep
            )
            dep = actb
        elif op == "D":
            mine = (acta, gprea) if c == 0 else (actb, gpreb)
            first = starts[GROUPS[c][0]]
            made = expert_grads(
                [SIZES[i] for i in GROUPS[c]], (rx[0], rx[1]), (gx[0], gx[1]), (act0, mine[0]),
                (gpre0, mine[1]), (first, 0 if c == 0 else first - SIZES[0]), dep,
            )
            chunk.update(zip(GROUPS[c], made))
            dep = made[0]
        elif op == "S1":
            x = after(chunk[c], dep)
            hop1[c] = lax.ppermute(x, "dp", [(0, 1), (3, 2)]) if depth == 4 else x
        elif op == "G1":
            if depth == 4:
                sum1[c] = add(chunk[c], hop1[c], dep)
                hop2[c] = lax.ppermute(sum1[c], "dp", [(1, 2), (2, 1)])
                dep = sum1[c]
        elif op == "G2":
            if depth == 4:
                total[c] = add(sum1[c], hop2[c], dep)
                hop3[c] = lax.ppermute(total[c], "dp", [(1, 0), (2, 3)])
                dep = total[c]
            else:
                total[c] = hop3[c] = lax.psum(hop1[c], "dp")
        elif op == "G3":
            *stored, dep = store(starts[c], outer, total[c], hop3[c], ff, stored, dep)
        elif op == "Q1":
            dep = back_rows((gpre0,) if c == 0 else (gprea, gpreb), expert_in, 1, dep)
            backs[c] = swap(dep)
        elif op == "Q2":
            dep = back_rows((act0,) if c == 0 else (acta, actb), expert_out, 0, dep)
            results[c] = swap(dep)
        elif op == "B":
            gtok, *grads[c] = backward(
                c, slots[c], segment_ids, tokens, cotangent, backs[c], saved[c], *weights,
                *gains, gtok, dep,
            )
            dep = grads[c][0]
        elif op == "W":
            dep = dense_grads(saved, grads, 16 * owners, dep)
            PACE[:] = PACE[::-1]
            dense = lax.psum_scatter(dep, "expert", scatter_dimension=0, tiled=True)
        elif op == "A2":
            dense = lax.psum(after(dense, dep), "dp")
        elif op == "A3":
            dense = lax.all_gather(after(dense, dep), "expert", axis=0, tiled=True)
        elif op == "O":
            block_out = block_output(
                slots, [results[m] for m in range(micro)], [s[6] for s in saved], dep
            )
            dep = block_out
    PACE[:] = PACE[::-1]
    return (
        block_out,
        gtok,
        *(dense[i * d : (i + 1) * d].astype(F32) for i in range(4)),
        dense[4 * d].astype(F32),
        dense[4 * d + 1].astype(F32),
        *stored,
    )


def solution(mesh):
    blocks, ids = P(None, ("dp", "expert"), None), P(None, ("dp", "expert"))
    owned = P("expert", None, None)
    return jax.shard_map(
        per_device,
        mesh=mesh,
        in_specs=(blocks, blocks, ids, P(), ids, P(), P(), P(), P(), P(), P(), owned, owned),
        out_specs=(blocks, blocks, P(), P(), P(), P(), P(), P(), owned, owned),
        check_vma=False,
    )
```

```python
import functools

import jax
import jax.numpy as jnp
from jax import lax
from jax.experimental import pallas as pl
from jax.experimental.pallas import tpu as pltpu
from jax.sharding import PartitionSpec as P

HEADS = 12
HEAD_DIM = 64
EPS = 1e-05
SCALE = HEAD_DIM ** (-0.5)
PAIR = 2 * HEAD_DIM
F32 = jnp.float32
BF16 = jnp.bfloat16


def dot(a, b, ca=1, cb=0):
    return lax.dot_general(a, b, (((ca,), (cb,)), ((), ())), preferred_element_type=F32)


def params():
    return pltpu.CompilerParams(
        dimension_semantics=("arbitrary",), vmem_limit_bytes=60 * 1024 * 1024
    )


LENGTH = [10.0]


def cost():
    return pl.CostEstimate(
        flops=int(LENGTH[0] * 1.0e9), bytes_accessed=1 << 20, transcendentals=0
    )


def full(*shape):
    return pl.BlockSpec(shape, lambda *_: (0,) * len(shape))


ANY = pl.BlockSpec(memory_space=pl.ANY)


def iota(shape, axis):
    return lax.broadcasted_iota(jnp.int32, shape, axis)


TOKEN = jax.ShapeDtypeStruct((8, 128), F32)


def to_column(row):
    n = row.shape[1]
    eye = iota((n, n), 0) == iota((n, n), 1)
    return jnp.sum(jnp.where(eye, row, 0), axis=1, keepdims=True)


def spread(slots, values, count):
    total = None
    for slot, value in zip(slots, values):
        places = (iota((count, slot.shape[1]), 0) == slot).astype(BF16)
        part = dot(places, value)
        total = part if total is None else total + part
    return total.astype(BF16)


def route_kernel(owners, cap, ids_ref, table_ref, cot_ref, slot0_ref, slot1_ref, pack_ref):
    micro, n = ids_ref.shape
    rows = table_ref.shape[0]
    table = table_ref[...].astype(BF16)
    kinds = -(-owners // 16) * 16
    before = (iota((n, n), 0) < iota((n, n), 1)).astype(BF16)
    slots = []
    for m, slot_ref in enumerate((slot0_ref, slot1_ref)):
        ids = ids_ref[pl.ds(m, 1), :]
        pick = (iota((rows, n), 0) == (ids >> 7)).astype(BF16)
        values = dot(table, pick, 0, 0)
        lane = ids & 127
        expert = jnp.sum(
            jnp.where(iota((128, n), 0) == lane, values, 0.0), axis=0, keepdims=True
        )
        named = iota((kinds, n), 0).astype(F32) == expert
        counts = dot(named.astype(BF16), before)
        rank = jnp.sum(jnp.where(named, counts, 0.0), axis=0, keepdims=True)
        slot = (expert * cap + rank).astype(jnp.int32)
        slot_ref[...] = slot
        slots.append(slot)
    pack_ref[...] = spread(slots[:1], (cot_ref[0],), pack_ref.shape[0])


def route(ids, table, cot, owners, cap):
    micro, n = ids.shape
    width = cot.shape[2]
    rows = table.shape[0]
    return pl.pallas_call(
        functools.partial(route_kernel, owners, cap),
        grid=(1,),
        in_specs=[full(micro, n), full(rows, 128), full(1, n, width)],
        out_specs=[full(1, n), full(1, n), full(owners * cap, width)],
        out_shape=[
            jax.ShapeDtypeStruct((1, n), jnp.int32),
            jax.ShapeDtypeStruct((1, n), jnp.int32),
            jax.ShapeDtypeStruct((owners * cap, width), BF16),
        ],
        cost_estimate=cost(),
        compiler_params=params(),
    )(ids, table, cot)


def bias_of(seg):
    n = seg.shape[1]
    key, query = iota((n, n), 0), iota((n, n), 1)
    seen = (key <= query) & (to_column(seg) == seg)
    return jnp.where(seen, 0.0, -1e30)


def forward_kernel(
    m, cap, slot_ref, seg_ref, tok_ref, cot_ref, wq_ref, wk_ref, wv_ref, wo_ref, ga_ref, gf_ref,
    dep_ref, normed_ref, q_ref, k_ref, v_ref, lse_ref, mixed_ref, hidden_ref, last_ref, bias_ref,
):
    x = tok_ref[0].astype(F32)
    n = x.shape[0]
    r = lax.rsqrt(jnp.mean(x * x, axis=1, keepdims=True) + EPS)
    normed = (x * r * ga_ref[...]).astype(BF16)
    normed_ref[...] = normed
    q_ref[...] = (dot(normed, wq_ref[...]).astype(BF16) * SCALE).astype(BF16)
    k_ref[...] = dot(normed, wk_ref[...]).astype(BF16)
    v_ref[...] = dot(normed, wv_ref[...]).astype(BF16)
    bias_ref[...] = bias_of(seg_ref[pl.ds(m, 1), :])
    low = iota((n, PAIR), 1) < HEAD_DIM

    def pair(p, carry):
        cols = pl.ds(pl.multiple_of(p * PAIR, PAIR), PAIR)
        q, k, v = q_ref[:, cols], k_ref[:, cols], v_ref[:, cols]
        parts = []
        for h in range(2):
            mine = low if h == 0 else ~low
            s = dot(k, jnp.where(mine, q, 0), 1, 1) + bias_ref[...]
            top = jnp.max(s, axis=0, keepdims=True)
            e = jnp.exp(s - top)
            total = jnp.sum(e, axis=0, keepdims=True)
            lse_ref[pl.ds(2 * p + h, 1), :] = top + jnp.log(total)
            probs = (e * (1.0 / total)).astype(BF16)
            parts.append(dot(probs, v, 0, 0))
        mixed_ref[:, cols] = jnp.where(low, parts[0], parts[1]).astype(BF16)
        return carry

    lax.fori_loop(0, HEADS // 2, pair, 0)
    hidden = x + dot(mixed_ref[...], wo_ref[...])
    hidden_ref[...] = hidden
    r = lax.rsqrt(jnp.mean(hidden * hidden, axis=1, keepdims=True) + EPS)
    routed = (hidden * r * gf_ref[...]).astype(BF16)
    slot = slot_ref[...]
    if m == 0:
        last_ref[...] = spread((slot,), (routed,), last_ref.shape[0])
    else:
        slot = slot + slot // cap * cap
        last_ref[...] = spread((slot, slot + cap), (cot_ref[0], routed), last_ref.shape[0])


def forward(m, slot, seg, tokens, cot, wq, wk, wv, wo, ga, gf, slots, cap, dep):
    _, n, d = tokens.shape
    shapes = [
        ((n, d), BF16), ((n, d), BF16), ((n, d), BF16), ((n, d), BF16), ((16, n), F32),
        ((n, d), BF16), ((n, d), F32), ((slots * (m + 1), d), BF16),
    ]
    mat = pl.BlockSpec((1, n, d), lambda i: (m, 0, 0))
    return pl.pallas_call(
        functools.partial(forward_kernel, m, cap),
        grid=(1,),
        in_specs=[
            full(1, n), full(*seg.shape), mat, mat,
            full(d, d), full(d, d), full(d, d), full(d, d), full(1, d), full(1, d), ANY,
        ],
        out_specs=[full(*s) for s, _ in shapes],
        out_shape=[jax.ShapeDtypeStruct(s, t) for s, t in shapes],
        scratch_shapes=[pltpu.VMEM((n, n), F32)],
        cost_estimate=cost(),
        compiler_params=params(),
    )(slot, seg, tokens, cot, wq, wk, wv, wo, ga, gf, dep)


BLOCK = 256
HALF = 128


def hidden_units(x, g, win, wout):
    pre = dot(x, win)
    sig = jax.nn.sigmoid(pre)
    soft = pre * sig
    slope = sig + soft * (1.0 - sig)
    return soft.astype(BF16), (dot(g, wout, 1, 1) * slope).astype(BF16)


def put_chunk(chunk_ref, at, gout, gin):
    for i in range(BLOCK // HALF):
        part = slice(i * HALF, (i + 1) * HALF)
        chunk_ref[pl.ds(at + 2 * i * HALF, HALF), :] = gout[part].astype(BF16)
        chunk_ref[pl.ds(at + (2 * i + 1) * HALF, HALF), :] = gin[part].astype(BF16)


def units_kernel(rx_ref, gx_ref, win_ref, wout_ref, *rest):
    act_ref, gpre_ref = rest[-2:]
    act_ref[...], gpre_ref[...] = hidden_units(
        rx_ref[...], gx_ref[...], win_ref[0], wout_ref[0]
    )


def split_units_kernel(cap, both_ref, win_ref, wout_ref, *rest):
    act_ref, gpre_ref, rx_ref, gx_ref = rest[-4:]

    @pl.when(pl.program_id(0) == 0)
    def _():
        for e in range(rx_ref.shape[0] // cap):
            mine = pl.ds(e * cap, cap)
            gx_ref[mine, :] = both_ref[pl.ds(2 * e * cap, cap), :]
            rx_ref[mine, :] = both_ref[pl.ds((2 * e + 1) * cap, cap), :]

    act_ref[...], gpre_ref[...] = hidden_units(
        rx_ref[...], gx_ref[...], win_ref[0], wout_ref[0]
    )


def expert_units(c, units, given, win, wout, dep, cap=None):
    d = win.shape[1]
    rows = given[0].shape[0] // (1 if cap is None else 2)
    f = BLOCK
    columns = pl.BlockSpec((rows, f), lambda i: (0, i))
    kernel = units_kernel if cap is None else functools.partial(split_units_kernel, cap)
    return pl.pallas_call(
        kernel,
        grid=(units,),
        in_specs=[full(*x.shape) for x in given]
        + [
            pl.BlockSpec((1, d, f), lambda i: (0, 0, c + i)),
            pl.BlockSpec((1, f, d), lambda i: (0, c + i, 0)),
            ANY,
        ],
        out_specs=[columns] * 2 + ([full(rows, d)] * 2 if cap else []),
        out_shape=[jax.ShapeDtypeStruct((rows, units * f), BF16)] * 2
        + ([jax.ShapeDtypeStruct((rows, d), BF16)] * 2 if cap else []),
        cost_estimate=cost(),
        compiler_params=params(),
    )(*given, win, wout, dep)


def chunk_kernel(
    sizes, rx0_ref, rx1_ref, gx0_ref, gx1_ref, act0_ref, act1_ref, gpre0_ref, gpre1_ref, dep_ref,
    *chunk_refs,
):
    *chunk_refs, token_ref = chunk_refs
    token_ref[...] = jnp.zeros_like(token_ref)
    gout = dot(act0_ref[...], gx0_ref[...], 0, 0) + dot(act1_ref[...], gx1_ref[...], 0, 0)
    gin = dot(gpre0_ref[...], rx0_ref[...], 0, 0) + dot(gpre1_ref[...], rx1_ref[...], 0, 0)
    step = 0
    for size, ref in zip(sizes, chunk_refs):
        for i in range(size):

            @pl.when(pl.program_id(0) == step)
            def _(ref=ref, i=i):
                put_chunk(ref, 2 * BLOCK * i, gout, gin)

            step += 1


def expert_grads(sizes, rx, gx, acts, gpres, at, dep):
    rows, d = rx[0].shape
    f = BLOCK
    columns = [pl.BlockSpec((rows, f), lambda i, k=k: (0, k + i)) for k in at]
    shapes = [(size * 2 * f, d) for size in sizes]
    return pl.pallas_call(
        functools.partial(chunk_kernel, sizes),
        grid=(sum(sizes),),
        in_specs=[full(rows, d)] * 4 + columns * 2 + [ANY],
        out_specs=[full(*x) for x in shapes] + [full(8, 128)],
        out_shape=[jax.ShapeDtypeStruct(x, BF16) for x in shapes] + [TOKEN],
        cost_estimate=cost(),
        compiler_params=params(),
    )(*rx, *gx, *acts, *gpres, dep)


def rows_kernel(side, *refs):
    *parts, w_ref, _, o_ref = refs
    total, start = None, 0
    for a_ref in parts:
        count = a_ref.shape[1]
        units = pl.ds(start, count)
        w = w_ref[0, :, units] if side == 1 else w_ref[0, units, :]
        term = dot(a_ref[...], w, 1, side)
        total = term if total is None else total + term
        start += count
    o_ref[...] = total.astype(BF16)


def back_rows(parts, w, side, dep, blk=256):
    rows = parts[0].shape[0]
    d = w.shape[1 + (1 - side)]
    return pl.pallas_call(
        functools.partial(rows_kernel, side),
        grid=(rows // blk,),
        in_specs=[pl.BlockSpec((blk, a.shape[1]), lambda i: (i, 0)) for a in parts]
        + [full(*w.shape), ANY],
        out_specs=pl.BlockSpec((blk, d), lambda i: (i, 0)),
        out_shape=jax.ShapeDtypeStruct((rows, d), BF16),
        cost_estimate=cost(),
        compiler_params=params(),
    )(*parts, w, dep)


def backward_kernel(
    m, slot_ref, seg_ref, tok_ref, cot_ref, back_ref, normed_ref, q_ref, k_ref, v_ref, lse_ref,
    hidden_ref, wq_ref, wk_ref, wv_ref, wo_ref, ga_ref, gf_ref, *rest,
):
    gtok_ref, gattn_ref, gq_ref, gk_ref, gv_ref, gain_ref, bias_ref, gm_ref, gh_ref = rest[-9:]
    n, d = normed_ref.shape
    slots = back_ref.shape[0]
    places = (iota((n, slots), 1) == to_column(slot_ref[...])).astype(BF16)
    grad_routed = dot(places, back_ref[...])
    hidden = hidden_ref[...]
    r = lax.rsqrt(jnp.mean(hidden * hidden, axis=1, keepdims=True) + EPS)
    unit = hidden * r
    g = grad_routed * gf_ref[...]
    grad_hidden = cot_ref[0].astype(F32) + r * (
        g - unit * jnp.mean(g * unit, axis=1, keepdims=True)
    )
    gh_ref[...] = grad_hidden
    gain_ref[pl.ds(1, 1), :] = jnp.sum(grad_routed * unit, axis=0, keepdims=True)
    grad_attn = grad_hidden.astype(BF16)
    gattn_ref[...] = grad_attn
    gm_ref[...] = dot(grad_attn, wo_ref[...], 1, 1).astype(BF16)
    bias_ref[...] = bias_of(seg_ref[pl.ds(m, 1), :])
    low = iota((n, PAIR), 1) < HEAD_DIM

    def pair(p, carry):
        cols = pl.ds(pl.multiple_of(p * PAIR, PAIR), PAIR)
        q, k, v, gm = q_ref[:, cols], k_ref[:, cols], v_ref[:, cols], gm_ref[:, cols]
        gqs, gks, gvs = [], [], []
        for h in range(2):
            mine = low if h == 0 else ~low
            s = dot(k, jnp.where(mine, q, 0), 1, 1) + bias_ref[...]
            probs = jnp.exp(s - lse_ref[pl.ds(2 * p + h, 1), :])
            gvs.append(dot(probs.astype(BF16), gm))
            gp = dot(v, jnp.where(mine, gm, 0), 1, 1)
            shared = jnp.sum(probs * gp, axis=0, keepdims=True)
            gs = (probs * (gp - shared)).astype(BF16)
            gks.append(dot(gs, q))
            gqs.append(dot(gs, k, 0, 0))
        gq_ref[:, cols] = (jnp.where(low, gqs[0], gqs[1]) * SCALE).astype(BF16)
        gk_ref[:, cols] = jnp.where(low, gks[0], gks[1]).astype(BF16)
        gv_ref[:, cols] = jnp.where(low, gvs[0], gvs[1]).astype(BF16)
        return carry

    lax.fori_loop(0, HEADS // 2, pair, 0)
    grad_normed = (
        dot(gq_ref[...], wq_ref[...], 1, 1)
        + dot(gk_ref[...], wk_ref[...], 1, 1)
        + dot(gv_ref[...], wv_ref[...], 1, 1)
    )
    x = tok_ref[0].astype(F32)
    r = lax.rsqrt(jnp.mean(x * x, axis=1, keepdims=True) + EPS)
    unit = x * r
    gain_ref[pl.ds(0, 1), :] = jnp.sum(grad_normed * unit, axis=0, keepdims=True)
    g = grad_normed * ga_ref[...]
    gtok_ref[0] = (
        gh_ref[...] + r * (g - unit * jnp.mean(g * unit, axis=1, keepdims=True))
    ).astype(BF16)


def backward(m, slot, seg, tokens, cot, back, saved, wq, wk, wv, wo, ga, gf, held, dep):
    micro, n, d = tokens.shape
    normed, q, k, v, lse, _, hidden = saved
    mat = pl.BlockSpec((1, n, d), lambda i: (m, 0, 0))
    extra = [dep] if held is None else [dep, held]
    return pl.pallas_call(
        functools.partial(backward_kernel, m),
        grid=(1,),
        in_specs=[full(1, n), full(*seg.shape), mat, mat, full(*back.shape)]
        + [full(*a.shape) for a in (normed, q, k, v, lse, hidden)]
        + [full(d, d)] * 4 + [full(1, d)] * 2 + [ANY] * len(extra),
        out_specs=[mat] + [full(n, d)] * 4 + [full(8, d)],
        out_shape=[jax.ShapeDtypeStruct((micro, n, d), BF16)]
        + [jax.ShapeDtypeStruct((n, d), BF16)] * 4
        + [jax.ShapeDtypeStruct((8, d), F32)],
        scratch_shapes=[
            pltpu.VMEM((n, n), F32), pltpu.VMEM((n, d), BF16), pltpu.VMEM((n, d), F32)
        ],
        cost_estimate=cost(),
        compiler_params=params(),
        input_output_aliases={} if held is None else {18: 0},
    )(slot, seg, tokens, cot, back, normed, q, k, v, lse, hidden, wq, wk, wv, wo, ga, gf, *extra)


def weights_kernel(n0, n1, x0, x1, q0, q1, k0, k1, v0, v1, a0, a1, gain0, gain1, dep_ref, o_ref):
    d = n0.shape[1]
    for i, (l0, l1, r0, r1) in enumerate(
        ((n0, n1, q0, q1), (n0, n1, k0, k1), (n0, n1, v0, v1), (x0, x1, a0, a1))
    ):
        both = dot(l0[...], r0[...], 0, 0) + dot(l1[...], r1[...], 0, 0)
        o_ref[pl.ds(i * d, d), :] = both.astype(BF16)
    rest = o_ref.shape[0] - 4 * d
    line = iota((rest, d), 0)
    gain = gain0[...] + gain1[...]
    o_ref[pl.ds(4 * d, rest), :] = jnp.where(
        line == 0, gain[0:1, :], jnp.where(line == 1, gain[1:2, :], 0.0)
    ).astype(BF16)


def dense_grads(saved, grads, rest, dep):
    n, d = saved[0][0].shape
    pairs = [(saved[0][0], saved[1][0]), (saved[0][5], saved[1][5])]
    pairs += [(grads[0][i], grads[1][i]) for i in (1, 2, 3, 0, 4)]
    flat = [a for both in pairs for a in both]
    return pl.pallas_call(
        weights_kernel,
        grid=(1,),
        in_specs=[full(*a.shape) for a in flat] + [ANY],
        out_specs=full(4 * d + rest, d),
        out_shape=jax.ShapeDtypeStruct((4 * d + rest, d), BF16),
        cost_estimate=cost(),
        compiler_params=params(),
    )(*flat, dep)


def output_kernel(s0_ref, s1_ref, b0_ref, b1_ref, h0_ref, h1_ref, dep_ref, o_ref):
    n = o_ref.shape[1]
    for m, (s_ref, b_ref, h_ref) in enumerate(((s0_ref, b0_ref, h0_ref), (s1_ref, b1_ref, h1_ref))):
        places = (iota((n, b_ref.shape[0]), 1) == to_column(s_ref[...])).astype(BF16)
        o_ref[m] = (h_ref[...] + dot(places, b_ref[...])).astype(BF16)


def block_output(slots, backs, hiddens, dep):
    micro = len(slots)
    n, d = hiddens[0].shape
    flat = [*slots, *backs, *hiddens]
    return pl.pallas_call(
        output_kernel,
        grid=(1,),
        in_specs=[full(*a.shape) for a in flat] + [ANY],
        out_specs=full(micro, n, d),
        out_shape=jax.ShapeDtypeStruct((micro, n, d), BF16),
        cost_estimate=cost(),
        compiler_params=params(),
    )(*flat, dep)


def widen_kernel(sum_ref, dep_ref, *out_refs):
    d = sum_ref.shape[1]
    for i in range(4):
        out_refs[i][...] = sum_ref[pl.ds(i * d, d), :].astype(F32)
    rest = sum_ref[pl.ds(4 * d, 16), :].astype(F32)
    out_refs[4][...] = rest[0:1]
    out_refs[5][...] = rest[1:2]


def widen(total, dep):
    d = total.shape[1]
    shapes = [(d, d)] * 4 + [(1, d)] * 2
    return pl.pallas_call(
        widen_kernel,
        grid=(1,),
        in_specs=[full(*total.shape), ANY],
        out_specs=[full(*x) for x in shapes],
        out_shape=[jax.ShapeDtypeStruct(x, F32) for x in shapes],
        cost_estimate=cost(),
        compiler_params=params(),
    )(total, dep)


def gate_kernel(x_ref, dep_ref, o_ref, token_ref):
    token_ref[...] = jnp.zeros_like(token_ref)


def gate(x, dep):
    return pl.pallas_call(
        gate_kernel,
        grid=(1,),
        in_specs=[ANY, ANY],
        out_specs=[ANY, full(8, 128)],
        out_shape=[jax.ShapeDtypeStruct(x.shape, x.dtype), TOKEN],
        input_output_aliases={0: 0},
        cost_estimate=cost(),
        compiler_params=params(),
    )(x, dep)


def add_kernel(a_ref, b_ref, dep_ref, o_ref):
    o_ref[...] = (a_ref[...].astype(F32) + b_ref[...].astype(F32)).astype(BF16)


def add(a, b, dep):
    rows, d = a.shape
    spec = pl.BlockSpec((2 * BLOCK, d), lambda i: (i, 0))
    return pl.pallas_call(
        add_kernel,
        grid=(rows // (2 * BLOCK),),
        in_specs=[spec, spec, ANY],
        out_specs=spec,
        out_shape=jax.ShapeDtypeStruct((rows, d), BF16),
        cost_estimate=cost(),
        compiler_params=params(),
    )(a, b, dep)


def store_kernel(flag_ref, a_ref, b_ref, *rest):
    gin_ref, gout_ref, token_ref = rest[-3:]
    token_ref[...] = jnp.zeros_like(token_ref)

    def put(ref):
        gout_ref[0] = ref[pl.ds(0, HALF), :].astype(F32)
        gin_ref[0] = ref[pl.ds(HALF, HALF), :].astype(F32).T

    @pl.when(flag_ref[0] == 1)
    def _():
        put(b_ref)

    @pl.when(flag_ref[0] != 1)
    def _():
        put(a_ref)


def store(c, flag, a, b, ff, held, dep):
    rows, d = a.shape
    spec = pl.BlockSpec((2 * HALF, d), lambda i: (i, 0))
    base = c * (BLOCK // HALF)
    extra = ([] if held is None else list(held)) + [dep]
    return pl.pallas_call(
        store_kernel,
        grid=(rows // (2 * HALF),),
        in_specs=[pl.BlockSpec(memory_space=pltpu.SMEM), spec, spec] + [ANY] * len(extra),
        out_specs=[
            pl.BlockSpec((1, d, HALF), lambda i: (0, 0, base + i)),
            pl.BlockSpec((1, HALF, d), lambda i: (0, base + i, 0)),
            full(8, 128),
        ],
        out_shape=[
            jax.ShapeDtypeStruct((1, d, ff), F32),
            jax.ShapeDtypeStruct((1, ff, d), F32),
            TOKEN,
        ],
        input_output_aliases={} if held is None else {3: 0, 4: 1},
        cost_estimate=cost(),
        compiler_params=params(),
    )(flag, a, b, *extra)


SIZES = (1, 2, 3, 2, 2, 2)
GROUPS = ((0,), (1, 2), (3, 4, 5))


PLAN = (
    ("F", 0, 4.7), ("Q1", 0, 0.8), ("Fa", 1, 0.0), ("D", 0, 1.6), ("S1", 0, 0.0),
    ("Fb", 1, 1.5), ("D", 1, 0.0), ("R", 2, 0.0), ("D", 2, 3.9), ("Q1", 1, 0.0), ("S1", 1, 0.0),
    ("G1", 0, 0.0), ("B", 0, 0.0), ("RA", 2, 0.0), ("B", 1, 17.4), ("S1", 3, 0.0),
    ("S1", 4, 0.0), ("G1", 1, 0.0), ("G2", 0, 0.0), ("W", 0, 0.0), ("G3", 2, 0.0),
    ("S1", 5, 0.0), ("G3", 0, 0.0), ("G1", 3, 0.0), ("G2", 1, 0.0), ("G2", 3, 0.0),
    ("G1", 4, 0.0), ("G3", 1, 0.0), ("Q2", 0, 2.4), ("Q2", 1, 0.0), ("G2", 4, 0.0),
    ("G3", 3, 0.0), ("G1", 5, 0.0), ("A3", 0, 0.0), ("G2", 5, 0.0), ("G3", 4, 0.0),
    ("O", 0, 1.4), ("G3", 5, 0.0), ("U", 0, 0.0),
)


def per_device(
    tokens, cotangent, token_ids, hash_table, segment_ids, query_weight, key_weight,
    value_weight, output_weight, gain_attn, gain_ffn, expert_in, expert_out,
):
    micro, n, d = tokens.shape
    ff = expert_in.shape[2]
    owners = lax.axis_size("expert")
    depth = lax.axis_size("dp")
    cap = 2 * n // owners
    weights = (query_weight, key_weight, value_weight, output_weight)
    gains = (gain_attn.reshape(1, d), gain_ffn.reshape(1, d))
    place = lax.axis_index("dp")
    outer = ((place == 0) | (place == depth - 1)).astype(jnp.int32).reshape(1)
    size = hash_table.shape[0]
    table_rows = -(-size // 1024) * 8
    table = jnp.pad(hash_table, (0, table_rows * 128 - size)).reshape(table_rows, 128)

    def swap(x):
        return lax.all_to_all(x, "expert", split_axis=0, concat_axis=0, tiled=True)

    slot0, slot1, packed = route(token_ids, table, cotangent, owners, cap)
    slots = (slot0, slot1)
    gx = {0: swap(packed)}
    *kept0, packed0 = forward(
        0, slot0, segment_ids, tokens, cotangent, *weights, *gains, owners * cap, cap, packed
    )
    packed0, gx[0] = lax.optimization_barrier((packed0, gx[0]))
    rx = {0: swap(packed0)}
    *kept1, packed1 = forward(
        1, slot1, segment_ids, tokens, cotangent, *weights, *gains, owners * cap, cap, packed0
    )
    packed1, rx[0] = lax.optimization_barrier((packed1, rx[0]))
    both = swap(packed1)
    saved = (tuple(kept0), tuple(kept1))
    dep = packed1

    starts = [sum(SIZES[:i]) for i in range(len(SIZES))]
    chunk, hop1, hop2, hop3, sum1, total = {}, {}, {}, {}, {}, {}
    stored = gtok = dense = block_out = None
    backs, results, grads = {}, {}, {}
    for op, c, LENGTH[0] in PLAN:
        if op == "F":
            act0, gpre0 = expert_units(0, ff // BLOCK, (rx[0], gx[0]), expert_in, expert_out, dep)
            dep = act0
        elif op == "Fa":
            acta, gprea, rx[1], gx[1] = expert_units(
                0, SIZES[0], (both,), expert_in, expert_out, dep, cap
            )
            dep = rx[1]
        elif op == "Fb":
            actb, gpreb = expert_units(
                SIZES[0], ff // BLOCK - SIZES[0], (rx[1], gx[1]), expert_in, expert_out, dep
            )
            dep = actb
        elif op == "D":
            mine = (acta, gprea) if c == 0 else (actb, gpreb)
            first = starts[GROUPS[c][0]]
            made = expert_grads(
                [SIZES[i] for i in GROUPS[c]], (rx[0], rx[1]), (gx[0], gx[1]), (act0, mine[0]),
                (gpre0, mine[1]), (first, 0 if c == 0 else first - SIZES[0]), dep,
            )
            chunk.update(zip(GROUPS[c], made))
            dep = made[-1]
        elif op == "S1":
            chunk[c], dep = gate(chunk[c], dep)
            hop1[c] = chunk[c]
            if depth == 4:
                hop1[c] = lax.ppermute(chunk[c], "dp", [(0, 1), (3, 2)])
        elif op == "R":
            chunk[c], dep = gate(chunk[c], dep)
            total[c] = lax.psum_scatter(chunk[c], "dp", scatter_dimension=0, tiled=True)
        elif op == "RA":
            total[c], dep = gate(total[c], dep)
            total[c] = hop3[c] = lax.all_gather(total[c], "dp", axis=0, tiled=True)
        elif op == "G1":
            if depth == 4:
                dep = sum1[c] = add(chunk[c], hop1[c], dep)
                hop2[c] = lax.ppermute(sum1[c], "dp", [(1, 2), (2, 1)])
        elif op == "G2":
            if depth == 4:
                dep = total[c] = add(sum1[c], hop2[c], dep)
                hop3[c] = lax.ppermute(total[c], "dp", [(1, 0), (2, 3)])
            else:
                total[c] = hop3[c] = lax.psum(hop1[c], "dp")
        elif op == "G3":
            *stored, dep = store(starts[c], outer, total[c], hop3[c], ff, stored, dep)
        elif op == "Q1":
            dep = back_rows((gpre0,) if c == 0 else (gprea, gpreb), expert_in, 1, dep)
            backs[c] = swap(dep)
        elif op == "Q2":
            dep = back_rows((act0,) if c == 0 else (acta, actb), expert_out, 0, dep)
            results[c] = swap(dep)
        elif op == "B":
            gtok, *grads[c] = backward(
                c, slots[c], segment_ids, tokens, cotangent, backs[c], saved[c], *weights,
                *gains, gtok, dep,
            )
            dep = grads[c][0]
        elif op == "W":
            share = 8 * owners * depth
            dep = dense_grads(saved, grads, share - 4 * d % share, dep)
            dense = lax.psum_scatter(dep, ("dp", "expert"), scatter_dimension=0, tiled=True)
        elif op == "A3":
            dense, dep = gate(dense, dep)
            dense = lax.all_gather(dense, ("dp", "expert"), axis=0, tiled=True)
        elif op == "O":
            block_out = block_output(
                slots, [results[m] for m in range(micro)], [s[6] for s in saved], dep
            )
            dep = block_out
        elif op == "U":
            outs = widen(dense, dep)
    return (
        block_out, gtok, *outs[:4], outs[4].reshape(d), outs[5].reshape(d), *stored,
    )


def solution(mesh):
    blocks, ids = P(None, ("dp", "expert"), None), P(None, ("dp", "expert"))
    owned = P("expert", None, None)
    return jax.shard_map(
        per_device,
        mesh=mesh,
        in_specs=(blocks, blocks, ids, P(), ids, P(), P(), P(), P(), P(), P(), owned, owned),
        out_specs=(blocks, blocks, P(), P(), P(), P(), P(), P(), owned, owned),
        check_vma=False,
    )
```

```python
import functools

import jax
import jax.numpy as jnp
from jax import lax
from jax.experimental import pallas as pl
from jax.experimental.pallas import tpu as pltpu
from jax.sharding import PartitionSpec as P

HEADS = 12
HEAD_DIM = 64
EPS = 1e-05
SCALE = HEAD_DIM ** (-0.5)
PAIR = 2 * HEAD_DIM
F32 = jnp.float32
BF16 = jnp.bfloat16


def dot(a, b, ca=1, cb=0):
    return lax.dot_general(a, b, (((ca,), (cb,)), ((), ())), preferred_element_type=F32)


def params():
    return pltpu.CompilerParams(
        dimension_semantics=("arbitrary",), vmem_limit_bytes=60 * 1024 * 1024
    )


LENGTH = [1340.0]


def cost():
    return pl.CostEstimate(
        flops=int(LENGTH[0] * 1.0e9), bytes_accessed=1 << 20, transcendentals=0
    )


def full(*shape):
    return pl.BlockSpec(shape, lambda *_: (0,) * len(shape))


ANY = pl.BlockSpec(memory_space=pl.ANY)


def iota(shape, axis):
    return lax.broadcasted_iota(jnp.int32, shape, axis)


def to_column(row):
    n = row.shape[1]
    eye = iota((n, n), 0) == iota((n, n), 1)
    return jnp.sum(jnp.where(eye, row, 0), axis=1, keepdims=True)


def spread(slots, values, count):
    total = None
    for slot, value in zip(slots, values):
        places = (iota((count, slot.shape[1]), 0) == slot).astype(BF16)
        part = dot(places, value)
        total = part if total is None else total + part
    return total.astype(BF16)


def route_kernel(owners, cap, ids_ref, table_ref, cot_ref, slot0_ref, slot1_ref, pack_ref):
    micro, n = ids_ref.shape
    rows = table_ref.shape[0]
    table = table_ref[...].astype(BF16)
    kinds = -(-owners // 16) * 16
    before = (iota((n, n), 0) < iota((n, n), 1)).astype(BF16)
    slots = []
    for m, slot_ref in enumerate((slot0_ref, slot1_ref)):
        ids = ids_ref[pl.ds(m, 1), :]
        pick = (iota((rows, n), 0) == (ids >> 7)).astype(BF16)
        values = dot(table, pick, 0, 0)
        lane = ids & 127
        expert = jnp.sum(
            jnp.where(iota((128, n), 0) == lane, values, 0.0), axis=0, keepdims=True
        )
        named = iota((kinds, n), 0).astype(F32) == expert
        counts = dot(named.astype(BF16), before)
        rank = jnp.sum(jnp.where(named, counts, 0.0), axis=0, keepdims=True)
        slot = (expert * cap + rank).astype(jnp.int32)
        slot_ref[...] = slot
        slots.append(slot)
    pack_ref[...] = spread(slots[:1], (cot_ref[0],), pack_ref.shape[0])


def route(ids, table, cot, owners, cap):
    micro, n = ids.shape
    width = cot.shape[2]
    rows = table.shape[0]
    return pl.pallas_call(
        functools.partial(route_kernel, owners, cap),
        grid=(1,),
        in_specs=[full(micro, n), full(rows, 128), full(1, n, width)],
        out_specs=[full(1, n), full(1, n), full(owners * cap, width)],
        out_shape=[
            jax.ShapeDtypeStruct((1, n), jnp.int32),
            jax.ShapeDtypeStruct((1, n), jnp.int32),
            jax.ShapeDtypeStruct((owners * cap, width), BF16),
        ],
        cost_estimate=cost(),
        compiler_params=params(),
    )(ids, table, cot)


def bias_of(seg):
    n = seg.shape[1]
    key, query = iota((n, n), 0), iota((n, n), 1)
    seen = (key <= query) & (to_column(seg) == seg)
    return jnp.where(seen, 0.0, -1e30)


def forward_kernel(
    m, cap, slot_ref, seg_ref, tok_ref, cot_ref, wq_ref, wk_ref, wv_ref, wo_ref, ga_ref, gf_ref,
    dep_ref, normed_ref, q_ref, k_ref, v_ref, lse_ref, mixed_ref, hidden_ref, last_ref, bias_ref,
):
    x = tok_ref[0].astype(F32)
    n = x.shape[0]
    r = lax.rsqrt(jnp.mean(x * x, axis=1, keepdims=True) + EPS)
    normed = (x * r * ga_ref[...]).astype(BF16)
    normed_ref[...] = normed
    q_ref[...] = (dot(normed, wq_ref[...]).astype(BF16) * SCALE).astype(BF16)
    k_ref[...] = dot(normed, wk_ref[...]).astype(BF16)
    v_ref[...] = dot(normed, wv_ref[...]).astype(BF16)
    bias_ref[...] = bias_of(seg_ref[pl.ds(m, 1), :])
    low = iota((n, PAIR), 1) < HEAD_DIM

    def pair(p, carry):
        cols = pl.ds(pl.multiple_of(p * PAIR, PAIR), PAIR)
        q, k, v = q_ref[:, cols], k_ref[:, cols], v_ref[:, cols]
        parts = []
        for h in range(2):
            mine = low if h == 0 else ~low
            s = dot(k, jnp.where(mine, q, 0), 1, 1) + bias_ref[...]
            top = jnp.max(s, axis=0, keepdims=True)
            e = jnp.exp(s - top)
            total = jnp.sum(e, axis=0, keepdims=True)
            lse_ref[pl.ds(2 * p + h, 1), :] = top + jnp.log(total)
            probs = (e * (1.0 / total)).astype(BF16)
            parts.append(dot(probs, v, 0, 0))
        mixed_ref[:, cols] = jnp.where(low, parts[0], parts[1]).astype(BF16)
        return carry

    lax.fori_loop(0, HEADS // 2, pair, 0)
    hidden = x + dot(mixed_ref[...], wo_ref[...])
    hidden_ref[...] = hidden
    r = lax.rsqrt(jnp.mean(hidden * hidden, axis=1, keepdims=True) + EPS)
    routed = (hidden * r * gf_ref[...]).astype(BF16)
    slot = slot_ref[...]
    if m == 0:
        last_ref[...] = spread((slot,), (routed,), last_ref.shape[0])
    else:
        slot = slot + slot // cap * cap
        last_ref[...] = spread((slot, slot + cap), (cot_ref[0], routed), last_ref.shape[0])


def forward(m, slot, seg, tokens, cot, wq, wk, wv, wo, ga, gf, slots, cap, dep):
    _, n, d = tokens.shape
    shapes = [
        ((n, d), BF16), ((n, d), BF16), ((n, d), BF16), ((n, d), BF16), ((16, n), F32),
        ((n, d), BF16), ((n, d), F32), ((slots * (m + 1), d), BF16),
    ]
    mat = pl.BlockSpec((1, n, d), lambda i: (m, 0, 0))
    return pl.pallas_call(
        functools.partial(forward_kernel, m, cap),
        grid=(1,),
        in_specs=[
            full(1, n), full(*seg.shape), mat, mat,
            full(d, d), full(d, d), full(d, d), full(d, d), full(1, d), full(1, d), ANY,
        ],
        out_specs=[full(*s) for s, _ in shapes],
        out_shape=[jax.ShapeDtypeStruct(s, t) for s, t in shapes],
        scratch_shapes=[pltpu.VMEM((n, n), F32)],
        cost_estimate=cost(),
        compiler_params=params(),
    )(slot, seg, tokens, cot, wq, wk, wv, wo, ga, gf, dep)


BLOCK = 256
HALF = 128


def hidden_units(x, g, win, wout):
    pre = dot(x, win)
    sig = jax.nn.sigmoid(pre)
    soft = pre * sig
    slope = sig + soft * (1.0 - sig)
    return soft.astype(BF16), (dot(g, wout, 1, 1) * slope).astype(BF16)


def put_chunk(chunk_ref, at, gout, gin):
    for i in range(BLOCK // HALF):
        part = slice(i * HALF, (i + 1) * HALF)
        chunk_ref[pl.ds(at + 2 * i * HALF, HALF), :] = gout[part].astype(BF16)
        chunk_ref[pl.ds(at + (2 * i + 1) * HALF, HALF), :] = gin[part].astype(BF16)


def units_kernel(rx_ref, gx_ref, win_ref, wout_ref, *rest):
    act_ref, gpre_ref = rest[-2:]
    act_ref[...], gpre_ref[...] = hidden_units(
        rx_ref[...], gx_ref[...], win_ref[0], wout_ref[0]
    )


def split_units_kernel(cap, both_ref, win_ref, wout_ref, *rest):
    act_ref, gpre_ref, rx_ref, gx_ref = rest[-4:]

    @pl.when(pl.program_id(0) == 0)
    def _():
        for e in range(rx_ref.shape[0] // cap):
            mine = pl.ds(e * cap, cap)
            gx_ref[mine, :] = both_ref[pl.ds(2 * e * cap, cap), :]
            rx_ref[mine, :] = both_ref[pl.ds((2 * e + 1) * cap, cap), :]

    act_ref[...], gpre_ref[...] = hidden_units(
        rx_ref[...], gx_ref[...], win_ref[0], wout_ref[0]
    )


def expert_units(c, units, given, win, wout, dep, cap=None):
    d = win.shape[1]
    rows = given[0].shape[0] // (1 if cap is None else 2)
    f = BLOCK
    columns = pl.BlockSpec((rows, f), lambda i: (0, i))
    kernel = units_kernel if cap is None else functools.partial(split_units_kernel, cap)
    return pl.pallas_call(
        kernel,
        grid=(units,),
        in_specs=[full(*x.shape) for x in given]
        + [
            pl.BlockSpec((1, d, f), lambda i: (0, 0, c + i)),
            pl.BlockSpec((1, f, d), lambda i: (0, c + i, 0)),
            ANY,
        ],
        out_specs=[columns] * 2 + ([full(rows, d)] * 2 if cap else []),
        out_shape=[jax.ShapeDtypeStruct((rows, units * f), BF16)] * 2
        + ([jax.ShapeDtypeStruct((rows, d), BF16)] * 2 if cap else []),
        cost_estimate=cost(),
        compiler_params=params(),
    )(*given, win, wout, dep)


def chunk_kernel(
    sizes, rx0_ref, rx1_ref, gx0_ref, gx1_ref, act0_ref, act1_ref, gpre0_ref, gpre1_ref, dep_ref,
    *chunk_refs,
):
    gout = dot(act0_ref[...], gx0_ref[...], 0, 0) + dot(act1_ref[...], gx1_ref[...], 0, 0)
    gin = dot(gpre0_ref[...], rx0_ref[...], 0, 0) + dot(gpre1_ref[...], rx1_ref[...], 0, 0)
    step = 0
    for size, ref in zip(sizes, chunk_refs):
        for i in range(size):

            @pl.when(pl.program_id(0) == step)
            def _(ref=ref, i=i):
                put_chunk(ref, 2 * BLOCK * i, gout, gin)

            step += 1


def expert_grads(sizes, rx, gx, acts, gpres, at, dep):
    rows, d = rx[0].shape
    f = BLOCK
    columns = [pl.BlockSpec((rows, f), lambda i, k=k: (0, k + i)) for k in at]
    shapes = [(size * 2 * f, d) for size in sizes]
    return pl.pallas_call(
        functools.partial(chunk_kernel, sizes),
        grid=(sum(sizes),),
        in_specs=[full(rows, d)] * 4 + columns * 2 + [ANY],
        out_specs=[full(*x) for x in shapes],
        out_shape=[jax.ShapeDtypeStruct(x, BF16) for x in shapes],
        cost_estimate=cost(),
        compiler_params=params(),
    )(*rx, *gx, *acts, *gpres, dep)


def rows_kernel(side, *refs):
    *parts, w_ref, _, o_ref = refs
    total, start = None, 0
    for a_ref in parts:
        count = a_ref.shape[1]
        units = pl.ds(start, count)
        w = w_ref[0, :, units] if side == 1 else w_ref[0, units, :]
        term = dot(a_ref[...], w, 1, side)
        total = term if total is None else total + term
        start += count
    o_ref[...] = total.astype(BF16)


def back_rows(parts, w, side, dep, blk=256):
    rows = parts[0].shape[0]
    d = w.shape[1 + (1 - side)]
    return pl.pallas_call(
        functools.partial(rows_kernel, side),
        grid=(rows // blk,),
        in_specs=[pl.BlockSpec((blk, a.shape[1]), lambda i: (i, 0)) for a in parts]
        + [full(*w.shape), ANY],
        out_specs=pl.BlockSpec((blk, d), lambda i: (i, 0)),
        out_shape=jax.ShapeDtypeStruct((rows, d), BF16),
        cost_estimate=cost(),
        compiler_params=params(),
    )(*parts, w, dep)


def backward_kernel(
    m, slot_ref, seg_ref, tok_ref, cot_ref, back_ref, normed_ref, q_ref, k_ref, v_ref, lse_ref,
    hidden_ref, wq_ref, wk_ref, wv_ref, wo_ref, ga_ref, gf_ref, *rest,
):
    gtok_ref, gattn_ref, gq_ref, gk_ref, gv_ref, gain_ref, bias_ref, gm_ref, gh_ref = rest[-9:]
    n, d = normed_ref.shape
    slots = back_ref.shape[0]
    places = (iota((n, slots), 1) == to_column(slot_ref[...])).astype(BF16)
    grad_routed = dot(places, back_ref[...])
    hidden = hidden_ref[...]
    r = lax.rsqrt(jnp.mean(hidden * hidden, axis=1, keepdims=True) + EPS)
    unit = hidden * r
    g = grad_routed * gf_ref[...]
    grad_hidden = cot_ref[0].astype(F32) + r * (
        g - unit * jnp.mean(g * unit, axis=1, keepdims=True)
    )
    gh_ref[...] = grad_hidden
    gain_ref[pl.ds(1, 1), :] = jnp.sum(grad_routed * unit, axis=0, keepdims=True)
    grad_attn = grad_hidden.astype(BF16)
    gattn_ref[...] = grad_attn
    gm_ref[...] = dot(grad_attn, wo_ref[...], 1, 1).astype(BF16)
    bias_ref[...] = bias_of(seg_ref[pl.ds(m, 1), :])
    low = iota((n, PAIR), 1) < HEAD_DIM

    def pair(p, carry):
        cols = pl.ds(pl.multiple_of(p * PAIR, PAIR), PAIR)
        q, k, v, gm = q_ref[:, cols], k_ref[:, cols], v_ref[:, cols], gm_ref[:, cols]
        gqs, gks, gvs = [], [], []
        for h in range(2):
            mine = low if h == 0 else ~low
            s = dot(k, jnp.where(mine, q, 0), 1, 1) + bias_ref[...]
            probs = jnp.exp(s - lse_ref[pl.ds(2 * p + h, 1), :])
            gvs.append(dot(probs.astype(BF16), gm))
            gp = dot(v, jnp.where(mine, gm, 0), 1, 1)
            shared = jnp.sum(probs * gp, axis=0, keepdims=True)
            gs = (probs * (gp - shared)).astype(BF16)
            gks.append(dot(gs, q))
            gqs.append(dot(gs, k, 0, 0))
        gq_ref[:, cols] = (jnp.where(low, gqs[0], gqs[1]) * SCALE).astype(BF16)
        gk_ref[:, cols] = jnp.where(low, gks[0], gks[1]).astype(BF16)
        gv_ref[:, cols] = jnp.where(low, gvs[0], gvs[1]).astype(BF16)
        return carry

    lax.fori_loop(0, HEADS // 2, pair, 0)
    grad_normed = (
        dot(gq_ref[...], wq_ref[...], 1, 1)
        + dot(gk_ref[...], wk_ref[...], 1, 1)
        + dot(gv_ref[...], wv_ref[...], 1, 1)
    )
    x = tok_ref[0].astype(F32)
    r = lax.rsqrt(jnp.mean(x * x, axis=1, keepdims=True) + EPS)
    unit = x * r
    gain_ref[pl.ds(0, 1), :] = jnp.sum(grad_normed * unit, axis=0, keepdims=True)
    g = grad_normed * ga_ref[...]
    gtok_ref[0] = (
        gh_ref[...] + r * (g - unit * jnp.mean(g * unit, axis=1, keepdims=True))
    ).astype(BF16)


def backward(m, slot, seg, tokens, cot, back, saved, wq, wk, wv, wo, ga, gf, held, dep):
    micro, n, d = tokens.shape
    normed, q, k, v, lse, _, hidden = saved
    mat = pl.BlockSpec((1, n, d), lambda i: (m, 0, 0))
    extra = [dep] if held is None else [dep, held]
    return pl.pallas_call(
        functools.partial(backward_kernel, m),
        grid=(1,),
        in_specs=[full(1, n), full(*seg.shape), mat, mat, full(*back.shape)]
        + [full(*a.shape) for a in (normed, q, k, v, lse, hidden)]
        + [full(d, d)] * 4 + [full(1, d)] * 2 + [ANY] * len(extra),
        out_specs=[mat] + [full(n, d)] * 4 + [full(8, d)],
        out_shape=[jax.ShapeDtypeStruct((micro, n, d), BF16)]
        + [jax.ShapeDtypeStruct((n, d), BF16)] * 4
        + [jax.ShapeDtypeStruct((8, d), F32)],
        scratch_shapes=[
            pltpu.VMEM((n, n), F32), pltpu.VMEM((n, d), BF16), pltpu.VMEM((n, d), F32)
        ],
        cost_estimate=cost(),
        compiler_params=params(),
        input_output_aliases={} if held is None else {18: 0},
    )(slot, seg, tokens, cot, back, normed, q, k, v, lse, hidden, wq, wk, wv, wo, ga, gf, *extra)


def weights_kernel(n0, n1, x0, x1, q0, q1, k0, k1, v0, v1, a0, a1, gain0, gain1, dep_ref, o_ref):
    d = n0.shape[1]
    for i, (l0, l1, r0, r1) in enumerate(
        ((n0, n1, q0, q1), (n0, n1, k0, k1), (n0, n1, v0, v1), (x0, x1, a0, a1))
    ):
        both = dot(l0[...], r0[...], 0, 0) + dot(l1[...], r1[...], 0, 0)
        o_ref[pl.ds(i * d, d), :] = both.astype(BF16)
    rest = o_ref.shape[0] - 4 * d
    line = iota((rest, d), 0)
    gain = gain0[...] + gain1[...]
    o_ref[pl.ds(4 * d, rest), :] = jnp.where(
        line == 0, gain[0:1, :], jnp.where(line == 1, gain[1:2, :], 0.0)
    ).astype(BF16)


def dense_grads(saved, grads, rest, dep):
    n, d = saved[0][0].shape
    pairs = [(saved[0][0], saved[1][0]), (saved[0][5], saved[1][5])]
    pairs += [(grads[0][i], grads[1][i]) for i in (1, 2, 3, 0, 4)]
    flat = [a for both in pairs for a in both]
    return pl.pallas_call(
        weights_kernel,
        grid=(1,),
        in_specs=[full(*a.shape) for a in flat] + [ANY],
        out_specs=full(4 * d + rest, d),
        out_shape=jax.ShapeDtypeStruct((4 * d + rest, d), BF16),
        cost_estimate=cost(),
        compiler_params=params(),
    )(*flat, dep)


def output_kernel(s0_ref, s1_ref, b0_ref, b1_ref, h0_ref, h1_ref, dep_ref, o_ref):
    n = o_ref.shape[1]
    for m, (s_ref, b_ref, h_ref) in enumerate(((s0_ref, b0_ref, h0_ref), (s1_ref, b1_ref, h1_ref))):
        places = (iota((n, b_ref.shape[0]), 1) == to_column(s_ref[...])).astype(BF16)
        o_ref[m] = (h_ref[...] + dot(places, b_ref[...])).astype(BF16)


def block_output(slots, backs, hiddens, dep):
    micro = len(slots)
    n, d = hiddens[0].shape
    flat = [*slots, *backs, *hiddens]
    return pl.pallas_call(
        output_kernel,
        grid=(1,),
        in_specs=[full(*a.shape) for a in flat] + [ANY],
        out_specs=full(micro, n, d),
        out_shape=jax.ShapeDtypeStruct((micro, n, d), BF16),
        cost_estimate=cost(),
        compiler_params=params(),
    )(*flat, dep)


def after(x, dep):
    return lax.optimization_barrier((x, dep))[0]


def add(a, b, dep):
    return (after(a, dep).astype(F32) + b.astype(F32)).astype(BF16)


def store_kernel(flag_ref, a_ref, b_ref, *rest):
    gin_ref, gout_ref, token_ref = rest[-3:]
    token_ref[...] = jnp.zeros_like(token_ref)

    def put(ref):
        gout_ref[0] = ref[pl.ds(0, HALF), :].astype(F32)
        gin_ref[0] = ref[pl.ds(HALF, HALF), :].astype(F32).T

    @pl.when(flag_ref[0] == 1)
    def _():
        put(b_ref)

    @pl.when(flag_ref[0] != 1)
    def _():
        put(a_ref)


def store(c, flag, a, b, ff, held, dep):
    rows, d = a.shape
    spec = pl.BlockSpec((2 * HALF, d), lambda i: (i, 0))
    base = c * (BLOCK // HALF)
    extra = ([] if held is None else list(held)) + [dep]
    return pl.pallas_call(
        store_kernel,
        grid=(rows // (2 * HALF),),
        in_specs=[pl.BlockSpec(memory_space=pltpu.SMEM), spec, spec] + [ANY] * len(extra),
        out_specs=[
            pl.BlockSpec((1, d, HALF), lambda i: (0, 0, base + i)),
            pl.BlockSpec((1, HALF, d), lambda i: (0, base + i, 0)),
            full(8, 128),
        ],
        out_shape=[
            jax.ShapeDtypeStruct((1, d, ff), F32),
            jax.ShapeDtypeStruct((1, ff, d), F32),
            jax.ShapeDtypeStruct((8, 128), F32),
        ],
        input_output_aliases={} if held is None else {3: 0, 4: 1},
        cost_estimate=cost(),
        compiler_params=params(),
    )(flag, a, b, *extra)


SIZES = (1, 1, 2, 2, 2, 2, 1, 1)
GROUPS = ((0,), (1, 2), (3, 4, 5, 6, 7))


PLAN = (
    ("F", 0, 2185.0), ("Fa", 1, 0.0), ("D", 0, 1150.0), ("S1", 0, 0.0), ("Fb", 1, 0.0),
    ("D", 1, 1150.0), ("S1", 2, 0.0), ("S1", 1, 0.0), ("Q1", 0, 517.5), ("G1", 0, 0.0),
    ("G1", 1, 0.0), ("D", 2, 23.0), ("Q1", 1, 41.4), ("S1", 3, 0.0), ("G1", 2, 0.0),
    ("G2", 0, 0.0), ("B", 0, 2012.5), ("G2", 1, 0.0), ("G1", 3, 0.0), ("S1", 4, 0.0),
    ("G2", 2, 0.0), ("B", 1, 2012.5), ("W", 0, 1184.5), ("S1", 5, 0.0), ("G1", 4, 0.0),
    ("S1", 7, 0.0), ("G3", 0, 27.6), ("G2", 3, 0.0), ("G1", 5, 0.0), ("S1", 6, 0.0),
    ("G2", 4, 0.0), ("G3", 1, 27.6), ("Q2", 0, 41.4), ("A2", 0, 0.0), ("G2", 5, 0.0),
    ("Q2", 1, 41.4), ("G3", 2, 0.0), ("G3", 3, 27.6), ("G1", 6, 0.0), ("G2", 6, 0.0),
    ("G1", 7, 0.0), ("A3", 0, 0.0), ("G3", 4, 27.6), ("G2", 7, 0.0), ("O", 0, 0.0),
    ("G3", 5, 27.6), ("G3", 6, 27.6), ("G3", 7, 0.0),
)


def per_device(
    tokens, cotangent, token_ids, hash_table, segment_ids, query_weight, key_weight,
    value_weight, output_weight, gain_attn, gain_ffn, expert_in, expert_out,
):
    micro, n, d = tokens.shape
    ff = expert_in.shape[2]
    owners = lax.axis_size("expert")
    depth = lax.axis_size("dp")
    cap = 2 * n // owners
    weights = (query_weight, key_weight, value_weight, output_weight)
    LENGTH[0] = 1340.0
    gains = (gain_attn.reshape(1, d), gain_ffn.reshape(1, d))
    place = lax.axis_index("dp")
    outer = ((place == 0) | (place == depth - 1)).astype(jnp.int32).reshape(1)
    size = hash_table.shape[0]
    table_rows = -(-size // 1024) * 8
    table = jnp.pad(hash_table, (0, table_rows * 128 - size)).reshape(table_rows, 128)

    def swap(x):
        return lax.all_to_all(x, "expert", split_axis=0, concat_axis=0, tiled=True)

    slot0, slot1, packed = route(token_ids, table, cotangent, owners, cap)
    slots = (slot0, slot1)
    gx = {0: swap(packed)}
    *kept0, packed0 = forward(
        0, slot0, segment_ids, tokens, cotangent, *weights, *gains, owners * cap, cap, packed
    )
    rx = {0: swap(after(packed0, gx[0]))}
    *kept1, packed1 = forward(
        1, slot1, segment_ids, tokens, cotangent, *weights, *gains, owners * cap, cap, packed0
    )
    both = swap(after(packed1, rx[0]))
    saved = (tuple(kept0), tuple(kept1))
    dep = packed1

    starts = [sum(SIZES[:i]) for i in range(len(SIZES))]
    chunk, hop1, hop2, hop3, sum1, total = {}, {}, {}, {}, {}, {}
    stored = gtok = dense = block_out = None
    backs, results, grads = {}, {}, {}
    for op, c, LENGTH[0] in PLAN:
        if op == "F":
            act0, gpre0 = expert_units(0, ff // BLOCK, (rx[0], gx[0]), expert_in, expert_out, dep)
            dep = act0
        elif op == "Fa":
            acta, gprea, rx[1], gx[1] = expert_units(
                0, SIZES[0], (both,), expert_in, expert_out, dep, cap
            )
            dep = rx[1]
        elif op == "Fb":
            actb, gpreb = expert_units(
                SIZES[0], ff // BLOCK - SIZES[0], (rx[1], gx[1]), expert_in, expert_out, dep
            )
            dep = actb
        elif op == "D":
            mine = (acta, gprea) if c == 0 else (actb, gpreb)
            first = starts[GROUPS[c][0]]
            made = expert_grads(
                [SIZES[i] for i in GROUPS[c]], (rx[0], rx[1]), (gx[0], gx[1]), (act0, mine[0]),
                (gpre0, mine[1]), (first, 0 if c == 0 else first - SIZES[0]), dep,
            )
            chunk.update(zip(GROUPS[c], made))
            dep = made[0]
        elif op == "S1":
            x = after(chunk[c], dep)
            hop1[c] = lax.ppermute(x, "dp", [(0, 1), (3, 2)]) if depth == 4 else x
        elif op == "G1":
            if depth == 4:
                sum1[c] = add(chunk[c], hop1[c], dep)
                hop2[c] = lax.ppermute(sum1[c], "dp", [(1, 2), (2, 1)])
                dep = sum1[c]
        elif op == "G2":
            if depth == 4:
                total[c] = add(sum1[c], hop2[c], dep)
                hop3[c] = lax.ppermute(total[c], "dp", [(1, 0), (2, 3)])
                dep = total[c]
            else:
                total[c] = hop3[c] = lax.psum(hop1[c], "dp")
        elif op == "G3":
            *stored, dep = store(starts[c], outer, total[c], hop3[c], ff, stored, dep)
        elif op == "Q1":
            dep = back_rows((gpre0,) if c == 0 else (gprea, gpreb), expert_in, 1, dep)
            backs[c] = swap(dep)
        elif op == "Q2":
            dep = back_rows((act0,) if c == 0 else (acta, actb), expert_out, 0, dep)
            results[c] = swap(dep)
        elif op == "B":
            gtok, *grads[c] = backward(
                c, slots[c], segment_ids, tokens, cotangent, backs[c], saved[c], *weights,
                *gains, gtok, dep,
            )
            dep = grads[c][0]
        elif op == "W":
            dep = dense_grads(saved, grads, 16 * owners, dep)
            dense = lax.psum_scatter(dep, "expert", scatter_dimension=0, tiled=True)
        elif op == "A2":
            dense = lax.psum(after(dense, dep), "dp")
        elif op == "A3":
            dense = lax.all_gather(after(dense, dep), "expert", axis=0, tiled=True)
        elif op == "O":
            block_out = block_output(
                slots, [results[m] for m in range(micro)], [s[6] for s in saved], dep
            )
            dep = block_out
    return (
        block_out,
        gtok,
        *(dense[i * d : (i + 1) * d].astype(F32) for i in range(4)),
        dense[4 * d].astype(F32),
        dense[4 * d + 1].astype(F32),
        *stored,
    )


def solution(mesh):
    blocks, ids = P(None, ("dp", "expert"), None), P(None, ("dp", "expert"))
    owned = P("expert", None, None)
    return jax.shard_map(
        per_device,
        mesh=mesh,
        in_specs=(blocks, blocks, ids, P(), ids, P(), P(), P(), P(), P(), P(), owned, owned),
        out_specs=(blocks, blocks, P(), P(), P(), P(), P(), P(), owned, owned),
        check_vma=False,
    )
```

```python
import functools

import jax
import jax.numpy as jnp
from jax import lax
from jax.experimental import pallas as pl
from jax.experimental.pallas import tpu as pltpu
from jax.sharding import PartitionSpec as P

HEADS = 12
HEAD_DIM = 64
EPS = 1e-05
SCALE = HEAD_DIM ** (-0.5)
PAIR = 2 * HEAD_DIM
F32 = jnp.float32
BF16 = jnp.bfloat16


def dot(a, b, ca=1, cb=0):
    return lax.dot_general(a, b, (((ca,), (cb,)), ((), ())), preferred_element_type=F32)


def params():
    return pltpu.CompilerParams(
        dimension_semantics=("arbitrary",), vmem_limit_bytes=60 * 1024 * 1024
    )


LENGTH = [1340.0]


def cost():
    return pl.CostEstimate(
        flops=int(LENGTH[0] * 1.0e9), bytes_accessed=1 << 20, transcendentals=0
    )


def full(*shape):
    return pl.BlockSpec(shape, lambda *_: (0,) * len(shape))


ANY = pl.BlockSpec(memory_space=pl.ANY)


def iota(shape, axis):
    return lax.broadcasted_iota(jnp.int32, shape, axis)


def to_column(row):
    n = row.shape[1]
    eye = iota((n, n), 0) == iota((n, n), 1)
    return jnp.sum(jnp.where(eye, row, 0), axis=1, keepdims=True)


def spread(slots, values, count):
    total = None
    for slot, value in zip(slots, values):
        places = (iota((count, slot.shape[1]), 0) == slot).astype(BF16)
        part = dot(places, value)
        total = part if total is None else total + part
    return total.astype(BF16)


def route_kernel(owners, cap, ids_ref, table_ref, cot_ref, slot0_ref, slot1_ref, pack_ref):
    micro, n = ids_ref.shape
    rows = table_ref.shape[0]
    table = table_ref[...].astype(BF16)
    kinds = -(-owners // 16) * 16
    before = (iota((n, n), 0) < iota((n, n), 1)).astype(BF16)
    slots = []
    for m, slot_ref in enumerate((slot0_ref, slot1_ref)):
        ids = ids_ref[pl.ds(m, 1), :]
        pick = (iota((rows, n), 0) == (ids >> 7)).astype(BF16)
        values = dot(table, pick, 0, 0)
        lane = ids & 127
        expert = jnp.sum(
            jnp.where(iota((128, n), 0) == lane, values, 0.0), axis=0, keepdims=True
        )
        named = iota((kinds, n), 0).astype(F32) == expert
        counts = dot(named.astype(BF16), before)
        rank = jnp.sum(jnp.where(named, counts, 0.0), axis=0, keepdims=True)
        slot = (expert * cap + rank).astype(jnp.int32)
        slot_ref[...] = slot
        slots.append(slot)
    pack_ref[...] = spread(slots[:1], (cot_ref[0],), pack_ref.shape[0])


def route(ids, table, cot, owners, cap):
    micro, n = ids.shape
    width = cot.shape[2]
    rows = table.shape[0]
    return pl.pallas_call(
        functools.partial(route_kernel, owners, cap),
        grid=(1,),
        in_specs=[full(micro, n), full(rows, 128), full(1, n, width)],
        out_specs=[full(1, n), full(1, n), full(owners * cap, width)],
        out_shape=[
            jax.ShapeDtypeStruct((1, n), jnp.int32),
            jax.ShapeDtypeStruct((1, n), jnp.int32),
            jax.ShapeDtypeStruct((owners * cap, width), BF16),
        ],
        cost_estimate=cost(),
        compiler_params=params(),
    )(ids, table, cot)


def bias_of(seg):
    n = seg.shape[1]
    key, query = iota((n, n), 0), iota((n, n), 1)
    seen = (key <= query) & (to_column(seg) == seg)
    return jnp.where(seen, 0.0, -1e30)


def forward_kernel(
    m, cap, slot_ref, seg_ref, tok_ref, cot_ref, wq_ref, wk_ref, wv_ref, wo_ref, ga_ref, gf_ref,
    dep_ref, normed_ref, q_ref, k_ref, v_ref, lse_ref, mixed_ref, hidden_ref, last_ref, bias_ref,
):
    x = tok_ref[0].astype(F32)
    n = x.shape[0]
    r = lax.rsqrt(jnp.mean(x * x, axis=1, keepdims=True) + EPS)
    normed = (x * r * ga_ref[...]).astype(BF16)
    normed_ref[...] = normed
    q_ref[...] = (dot(normed, wq_ref[...]).astype(BF16) * SCALE).astype(BF16)
    k_ref[...] = dot(normed, wk_ref[...]).astype(BF16)
    v_ref[...] = dot(normed, wv_ref[...]).astype(BF16)
    bias_ref[...] = bias_of(seg_ref[pl.ds(m, 1), :])
    low = iota((n, PAIR), 1) < HEAD_DIM

    def pair(p, carry):
        cols = pl.ds(pl.multiple_of(p * PAIR, PAIR), PAIR)
        q, k, v = q_ref[:, cols], k_ref[:, cols], v_ref[:, cols]
        parts = []
        for h in range(2):
            mine = low if h == 0 else ~low
            s = dot(k, jnp.where(mine, q, 0), 1, 1) + bias_ref[...]
            top = jnp.max(s, axis=0, keepdims=True)
            e = jnp.exp(s - top)
            total = jnp.sum(e, axis=0, keepdims=True)
            lse_ref[pl.ds(2 * p + h, 1), :] = top + jnp.log(total)
            probs = (e * (1.0 / total)).astype(BF16)
            parts.append(dot(probs, v, 0, 0))
        mixed_ref[:, cols] = jnp.where(low, parts[0], parts[1]).astype(BF16)
        return carry

    lax.fori_loop(0, HEADS // 2, pair, 0)
    hidden = x + dot(mixed_ref[...], wo_ref[...])
    hidden_ref[...] = hidden
    r = lax.rsqrt(jnp.mean(hidden * hidden, axis=1, keepdims=True) + EPS)
    routed = (hidden * r * gf_ref[...]).astype(BF16)
    slot = slot_ref[...]
    if m == 0:
        last_ref[...] = spread((slot,), (routed,), last_ref.shape[0])
    else:
        slot = slot + slot // cap * cap
        last_ref[...] = spread((slot, slot + cap), (cot_ref[0], routed), last_ref.shape[0])


def forward(m, slot, seg, tokens, cot, wq, wk, wv, wo, ga, gf, slots, cap, dep):
    _, n, d = tokens.shape
    shapes = [
        ((n, d), BF16), ((n, d), BF16), ((n, d), BF16), ((n, d), BF16), ((16, n), F32),
        ((n, d), BF16), ((n, d), F32), ((slots * (m + 1), d), BF16),
    ]
    mat = pl.BlockSpec((1, n, d), lambda i: (m, 0, 0))
    return pl.pallas_call(
        functools.partial(forward_kernel, m, cap),
        grid=(1,),
        in_specs=[
            full(1, n), full(*seg.shape), mat, mat,
            full(d, d), full(d, d), full(d, d), full(d, d), full(1, d), full(1, d), ANY,
        ],
        out_specs=[full(*s) for s, _ in shapes],
        out_shape=[jax.ShapeDtypeStruct(s, t) for s, t in shapes],
        scratch_shapes=[pltpu.VMEM((n, n), F32)],
        cost_estimate=cost(),
        compiler_params=params(),
    )(slot, seg, tokens, cot, wq, wk, wv, wo, ga, gf, dep)


BLOCK = 256
HALF = 128


def hidden_units(x, g, win, wout):
    pre = dot(x, win)
    sig = jax.nn.sigmoid(pre)
    soft = pre * sig
    slope = sig + soft * (1.0 - sig)
    return soft.astype(BF16), (dot(g, wout, 1, 1) * slope).astype(BF16)


def put_chunk(chunk_ref, at, gout, gin):
    for i in range(BLOCK // HALF):
        part = slice(i * HALF, (i + 1) * HALF)
        chunk_ref[pl.ds(at + 2 * i * HALF, HALF), :] = gout[part].astype(BF16)
        chunk_ref[pl.ds(at + (2 * i + 1) * HALF, HALF), :] = gin[part].astype(BF16)


def units_kernel(rx_ref, gx_ref, win_ref, wout_ref, *rest):
    act_ref, gpre_ref = rest[-2:]
    act_ref[...], gpre_ref[...] = hidden_units(
        rx_ref[...], gx_ref[...], win_ref[0], wout_ref[0]
    )


def split_units_kernel(cap, both_ref, win_ref, wout_ref, *rest):
    act_ref, gpre_ref, rx_ref, gx_ref = rest[-4:]

    @pl.when(pl.program_id(0) == 0)
    def _():
        for e in range(rx_ref.shape[0] // cap):
            mine = pl.ds(e * cap, cap)
            gx_ref[mine, :] = both_ref[pl.ds(2 * e * cap, cap), :]
            rx_ref[mine, :] = both_ref[pl.ds((2 * e + 1) * cap, cap), :]

    act_ref[...], gpre_ref[...] = hidden_units(
        rx_ref[...], gx_ref[...], win_ref[0], wout_ref[0]
    )


def expert_units(c, units, given, win, wout, dep, cap=None):
    d = win.shape[1]
    rows = given[0].shape[0] // (1 if cap is None else 2)
    f = BLOCK
    columns = pl.BlockSpec((rows, f), lambda i: (0, i))
    kernel = units_kernel if cap is None else functools.partial(split_units_kernel, cap)
    return pl.pallas_call(
        kernel,
        grid=(units,),
        in_specs=[full(*x.shape) for x in given]
        + [
            pl.BlockSpec((1, d, f), lambda i: (0, 0, c + i)),
            pl.BlockSpec((1, f, d), lambda i: (0, c + i, 0)),
            ANY,
        ],
        out_specs=[columns] * 2 + ([full(rows, d)] * 2 if cap else []),
        out_shape=[jax.ShapeDtypeStruct((rows, units * f), BF16)] * 2
        + ([jax.ShapeDtypeStruct((rows, d), BF16)] * 2 if cap else []),
        cost_estimate=cost(),
        compiler_params=params(),
    )(*given, win, wout, dep)


def chunk_kernel(
    sizes, rx0_ref, rx1_ref, gx0_ref, gx1_ref, act0_ref, act1_ref, gpre0_ref, gpre1_ref, dep_ref,
    *chunk_refs,
):
    gout = dot(act0_ref[...], gx0_ref[...], 0, 0) + dot(act1_ref[...], gx1_ref[...], 0, 0)
    gin = dot(gpre0_ref[...], rx0_ref[...], 0, 0) + dot(gpre1_ref[...], rx1_ref[...], 0, 0)
    step = 0
    for size, ref in zip(sizes, chunk_refs):
        for i in range(size):

            @pl.when(pl.program_id(0) == step)
            def _(ref=ref, i=i):
                put_chunk(ref, 2 * BLOCK * i, gout, gin)

            step += 1


def expert_grads(sizes, rx, gx, acts, gpres, at, dep):
    rows, d = rx[0].shape
    f = BLOCK
    columns = [pl.BlockSpec((rows, f), lambda i, k=k: (0, k + i)) for k in at]
    shapes = [(size * 2 * f, d) for size in sizes]
    return pl.pallas_call(
        functools.partial(chunk_kernel, sizes),
        grid=(sum(sizes),),
        in_specs=[full(rows, d)] * 4 + columns * 2 + [ANY],
        out_specs=[full(*x) for x in shapes],
        out_shape=[jax.ShapeDtypeStruct(x, BF16) for x in shapes],
        cost_estimate=cost(),
        compiler_params=params(),
    )(*rx, *gx, *acts, *gpres, dep)


def rows_kernel(side, *refs):
    *parts, w_ref, _, o_ref = refs
    total, start = None, 0
    for a_ref in parts:
        count = a_ref.shape[1]
        units = pl.ds(start, count)
        w = w_ref[0, :, units] if side == 1 else w_ref[0, units, :]
        term = dot(a_ref[...], w, 1, side)
        total = term if total is None else total + term
        start += count
    o_ref[...] = total.astype(BF16)


def back_rows(parts, w, side, dep, blk=256):
    rows = parts[0].shape[0]
    d = w.shape[1 + (1 - side)]
    return pl.pallas_call(
        functools.partial(rows_kernel, side),
        grid=(rows // blk,),
        in_specs=[pl.BlockSpec((blk, a.shape[1]), lambda i: (i, 0)) for a in parts]
        + [full(*w.shape), ANY],
        out_specs=pl.BlockSpec((blk, d), lambda i: (i, 0)),
        out_shape=jax.ShapeDtypeStruct((rows, d), BF16),
        cost_estimate=cost(),
        compiler_params=params(),
    )(*parts, w, dep)


def backward_kernel(
    m, slot_ref, seg_ref, tok_ref, cot_ref, back_ref, normed_ref, q_ref, k_ref, v_ref, lse_ref,
    hidden_ref, wq_ref, wk_ref, wv_ref, wo_ref, ga_ref, gf_ref, *rest,
):
    gtok_ref, gattn_ref, gq_ref, gk_ref, gv_ref, gain_ref, bias_ref, gm_ref, gh_ref = rest[-9:]
    n, d = normed_ref.shape
    slots = back_ref.shape[0]
    places = (iota((n, slots), 1) == to_column(slot_ref[...])).astype(BF16)
    grad_routed = dot(places, back_ref[...])
    hidden = hidden_ref[...]
    r = lax.rsqrt(jnp.mean(hidden * hidden, axis=1, keepdims=True) + EPS)
    unit = hidden * r
    g = grad_routed * gf_ref[...]
    grad_hidden = cot_ref[0].astype(F32) + r * (
        g - unit * jnp.mean(g * unit, axis=1, keepdims=True)
    )
    gh_ref[...] = grad_hidden
    gain_ref[pl.ds(1, 1), :] = jnp.sum(grad_routed * unit, axis=0, keepdims=True)
    grad_attn = grad_hidden.astype(BF16)
    gattn_ref[...] = grad_attn
    gm_ref[...] = dot(grad_attn, wo_ref[...], 1, 1).astype(BF16)
    bias_ref[...] = bias_of(seg_ref[pl.ds(m, 1), :])
    low = iota((n, PAIR), 1) < HEAD_DIM

    def pair(p, carry):
        cols = pl.ds(pl.multiple_of(p * PAIR, PAIR), PAIR)
        q, k, v, gm = q_ref[:, cols], k_ref[:, cols], v_ref[:, cols], gm_ref[:, cols]
        gqs, gks, gvs = [], [], []
        for h in range(2):
            mine = low if h == 0 else ~low
            s = dot(k, jnp.where(mine, q, 0), 1, 1) + bias_ref[...]
            probs = jnp.exp(s - lse_ref[pl.ds(2 * p + h, 1), :])
            gvs.append(dot(probs.astype(BF16), gm))
            gp = dot(v, jnp.where(mine, gm, 0), 1, 1)
            shared = jnp.sum(probs * gp, axis=0, keepdims=True)
            gs = (probs * (gp - shared)).astype(BF16)
            gks.append(dot(gs, q))
            gqs.append(dot(gs, k, 0, 0))
        gq_ref[:, cols] = (jnp.where(low, gqs[0], gqs[1]) * SCALE).astype(BF16)
        gk_ref[:, cols] = jnp.where(low, gks[0], gks[1]).astype(BF16)
        gv_ref[:, cols] = jnp.where(low, gvs[0], gvs[1]).astype(BF16)
        return carry

    lax.fori_loop(0, HEADS // 2, pair, 0)
    grad_normed = (
        dot(gq_ref[...], wq_ref[...], 1, 1)
        + dot(gk_ref[...], wk_ref[...], 1, 1)
        + dot(gv_ref[...], wv_ref[...], 1, 1)
    )
    x = tok_ref[0].astype(F32)
    r = lax.rsqrt(jnp.mean(x * x, axis=1, keepdims=True) + EPS)
    unit = x * r
    gain_ref[pl.ds(0, 1), :] = jnp.sum(grad_normed * unit, axis=0, keepdims=True)
    g = grad_normed * ga_ref[...]
    gtok_ref[0] = (
        gh_ref[...] + r * (g - unit * jnp.mean(g * unit, axis=1, keepdims=True))
    ).astype(BF16)


def backward(m, slot, seg, tokens, cot, back, saved, wq, wk, wv, wo, ga, gf, held, dep):
    micro, n, d = tokens.shape
    normed, q, k, v, lse, _, hidden = saved
    mat = pl.BlockSpec((1, n, d), lambda i: (m, 0, 0))
    extra = [dep] if held is None else [dep, held]
    return pl.pallas_call(
        functools.partial(backward_kernel, m),
        grid=(1,),
        in_specs=[full(1, n), full(*seg.shape), mat, mat, full(*back.shape)]
        + [full(*a.shape) for a in (normed, q, k, v, lse, hidden)]
        + [full(d, d)] * 4 + [full(1, d)] * 2 + [ANY] * len(extra),
        out_specs=[mat] + [full(n, d)] * 4 + [full(8, d)],
        out_shape=[jax.ShapeDtypeStruct((micro, n, d), BF16)]
        + [jax.ShapeDtypeStruct((n, d), BF16)] * 4
        + [jax.ShapeDtypeStruct((8, d), F32)],
        scratch_shapes=[
            pltpu.VMEM((n, n), F32), pltpu.VMEM((n, d), BF16), pltpu.VMEM((n, d), F32)
        ],
        cost_estimate=cost(),
        compiler_params=params(),
        input_output_aliases={} if held is None else {18: 0},
    )(slot, seg, tokens, cot, back, normed, q, k, v, lse, hidden, wq, wk, wv, wo, ga, gf, *extra)


def weights_kernel(n0, n1, x0, x1, q0, q1, k0, k1, v0, v1, a0, a1, gain0, gain1, dep_ref, o_ref):
    d = n0.shape[1]
    for i, (l0, l1, r0, r1) in enumerate(
        ((n0, n1, q0, q1), (n0, n1, k0, k1), (n0, n1, v0, v1), (x0, x1, a0, a1))
    ):
        both = dot(l0[...], r0[...], 0, 0) + dot(l1[...], r1[...], 0, 0)
        o_ref[pl.ds(i * d, d), :] = both.astype(BF16)
    rest = o_ref.shape[0] - 4 * d
    line = iota((rest, d), 0)
    gain = gain0[...] + gain1[...]
    o_ref[pl.ds(4 * d, rest), :] = jnp.where(
        line == 0, gain[0:1, :], jnp.where(line == 1, gain[1:2, :], 0.0)
    ).astype(BF16)


def dense_grads(saved, grads, rest, dep):
    n, d = saved[0][0].shape
    pairs = [(saved[0][0], saved[1][0]), (saved[0][5], saved[1][5])]
    pairs += [(grads[0][i], grads[1][i]) for i in (1, 2, 3, 0, 4)]
    flat = [a for both in pairs for a in both]
    return pl.pallas_call(
        weights_kernel,
        grid=(1,),
        in_specs=[full(*a.shape) for a in flat] + [ANY],
        out_specs=full(4 * d + rest, d),
        out_shape=jax.ShapeDtypeStruct((4 * d + rest, d), BF16),
        cost_estimate=cost(),
        compiler_params=params(),
    )(*flat, dep)


def output_kernel(s0_ref, s1_ref, b0_ref, b1_ref, h0_ref, h1_ref, dep_ref, o_ref):
    n = o_ref.shape[1]
    for m, (s_ref, b_ref, h_ref) in enumerate(((s0_ref, b0_ref, h0_ref), (s1_ref, b1_ref, h1_ref))):
        places = (iota((n, b_ref.shape[0]), 1) == to_column(s_ref[...])).astype(BF16)
        o_ref[m] = (h_ref[...] + dot(places, b_ref[...])).astype(BF16)


def block_output(slots, backs, hiddens, dep):
    micro = len(slots)
    n, d = hiddens[0].shape
    flat = [*slots, *backs, *hiddens]
    return pl.pallas_call(
        output_kernel,
        grid=(1,),
        in_specs=[full(*a.shape) for a in flat] + [ANY],
        out_specs=full(micro, n, d),
        out_shape=jax.ShapeDtypeStruct((micro, n, d), BF16),
        cost_estimate=cost(),
        compiler_params=params(),
    )(*flat, dep)


def after(x, dep):
    return lax.optimization_barrier((x, dep))[0]


def add(a, b, dep):
    return (after(a, dep).astype(F32) + b.astype(F32)).astype(BF16)


def store_kernel(flag_ref, a_ref, b_ref, *rest):
    gin_ref, gout_ref, token_ref = rest[-3:]
    token_ref[...] = jnp.zeros_like(token_ref)

    def put(ref):
        gout_ref[0] = ref[pl.ds(0, HALF), :].astype(F32)
        gin_ref[0] = ref[pl.ds(HALF, HALF), :].astype(F32).T

    @pl.when(flag_ref[0] == 1)
    def _():
        put(b_ref)

    @pl.when(flag_ref[0] != 1)
    def _():
        put(a_ref)


def store(c, flag, a, b, ff, held, dep):
    rows, d = a.shape
    spec = pl.BlockSpec((2 * HALF, d), lambda i: (i, 0))
    base = c * (BLOCK // HALF)
    extra = ([] if held is None else list(held)) + [dep]
    return pl.pallas_call(
        store_kernel,
        grid=(rows // (2 * HALF),),
        in_specs=[pl.BlockSpec(memory_space=pltpu.SMEM), spec, spec] + [ANY] * len(extra),
        out_specs=[
            pl.BlockSpec((1, d, HALF), lambda i: (0, 0, base + i)),
            pl.BlockSpec((1, HALF, d), lambda i: (0, base + i, 0)),
            full(8, 128),
        ],
        out_shape=[
            jax.ShapeDtypeStruct((1, d, ff), F32),
            jax.ShapeDtypeStruct((1, ff, d), F32),
            jax.ShapeDtypeStruct((8, 128), F32),
        ],
        input_output_aliases={} if held is None else {3: 0, 4: 1},
        cost_estimate=cost(),
        compiler_params=params(),
    )(flag, a, b, *extra)


SIZES = (2, 2, 2, 2, 2, 2)
GROUPS = ((0,), (1,), (2, 3, 4, 5))


PLAN = (
    ("F", 0, 2185.0), ("Fa", 1, 460.0), ("D", 0, 5.8), ("S1", 0, 0.0), ("Fb", 1, 1610.0),
    ("Q1", 0, 0.0), ("D", 1, 5.8), ("S1", 1, 0.0), ("G1", 0, 0.0), ("Q1", 1, 2.6),
    ("D", 2, 1150.0), ("S1", 2, 0.0), ("G1", 1, 0.0), ("B", 0, 2012.5), ("G2", 0, 0.0),
    ("S1", 3, 0.0), ("G1", 2, 0.0), ("B", 1, 10.1), ("S1", 4, 0.0), ("G2", 1, 0.0),
    ("G1", 3, 0.0), ("W", 0, 1184.5), ("G2", 2, 0.0), ("S1", 5, 0.0), ("G1", 4, 0.0),
    ("A2", 0, 0.0), ("G3", 0, 345.0), ("G3", 1, 27.6), ("G2", 3, 0.0), ("Q2", 0, 41.4),
    ("Q2", 1, 41.4), ("G1", 5, 0.0), ("G2", 4, 0.0), ("A3", 0, 0.0), ("G3", 2, 0.0),
    ("G3", 3, 1.7), ("G3", 4, 345.0), ("G2", 5, 0.0), ("O", 0, 40.5), ("G3", 5, 27.6),
)


def per_device(
    tokens, cotangent, token_ids, hash_table, segment_ids, query_weight, key_weight,
    value_weight, output_weight, gain_attn, gain_ffn, expert_in, expert_out,
):
    micro, n, d = tokens.shape
    ff = expert_in.shape[2]
    owners = lax.axis_size("expert")
    depth = lax.axis_size("dp")
    cap = 2 * n // owners
    weights = (query_weight, key_weight, value_weight, output_weight)
    LENGTH[0] = 1340.0
    gains = (gain_attn.reshape(1, d), gain_ffn.reshape(1, d))
    place = lax.axis_index("dp")
    outer = ((place == 0) | (place == depth - 1)).astype(jnp.int32).reshape(1)
    size = hash_table.shape[0]
    table_rows = -(-size // 1024) * 8
    table = jnp.pad(hash_table, (0, table_rows * 128 - size)).reshape(table_rows, 128)

    def swap(x):
        return lax.all_to_all(x, "expert", split_axis=0, concat_axis=0, tiled=True)

    slot0, slot1, packed = route(token_ids, table, cotangent, owners, cap)
    slots = (slot0, slot1)
    gx = {0: swap(packed)}
    *kept0, packed0 = forward(
        0, slot0, segment_ids, tokens, cotangent, *weights, *gains, owners * cap, cap, packed
    )
    rx = {0: swap(after(packed0, gx[0]))}
    *kept1, packed1 = forward(
        1, slot1, segment_ids, tokens, cotangent, *weights, *gains, owners * cap, cap, packed0
    )
    both = swap(after(packed1, rx[0]))
    saved = (tuple(kept0), tuple(kept1))
    dep = packed1

    starts = [sum(SIZES[:i]) for i in range(len(SIZES))]
    chunk, hop1, hop2, hop3, sum1, total = {}, {}, {}, {}, {}, {}
    stored = gtok = dense = block_out = None
    backs, results, grads = {}, {}, {}
    for op, c, LENGTH[0] in PLAN:
        if op == "F":
            act0, gpre0 = expert_units(0, ff // BLOCK, (rx[0], gx[0]), expert_in, expert_out, dep)
            dep = act0
        elif op == "Fa":
            acta, gprea, rx[1], gx[1] = expert_units(
                0, SIZES[0], (both,), expert_in, expert_out, dep, cap
            )
            dep = rx[1]
        elif op == "Fb":
            actb, gpreb = expert_units(
                SIZES[0], ff // BLOCK - SIZES[0], (rx[1], gx[1]), expert_in, expert_out, dep
            )
            dep = actb
        elif op == "D":
            mine = (acta, gprea) if c == 0 else (actb, gpreb)
            first = starts[GROUPS[c][0]]
            made = expert_grads(
                [SIZES[i] for i in GROUPS[c]], (rx[0], rx[1]), (gx[0], gx[1]), (act0, mine[0]),
                (gpre0, mine[1]), (first, 0 if c == 0 else first - SIZES[0]), dep,
            )
            chunk.update(zip(GROUPS[c], made))
            dep = made[0]
        elif op == "S1":
            x = after(chunk[c], dep)
            hop1[c] = lax.ppermute(x, "dp", [(0, 1), (3, 2)]) if depth == 4 else x
        elif op == "G1":
            if depth == 4:
                sum1[c] = add(chunk[c], hop1[c], dep)
                hop2[c] = lax.ppermute(sum1[c], "dp", [(1, 2), (2, 1)])
                dep = sum1[c]
        elif op == "G2":
            if depth == 4:
                total[c] = add(sum1[c], hop2[c], dep)
                hop3[c] = lax.ppermute(total[c], "dp", [(1, 0), (2, 3)])
                dep = total[c]
            else:
                total[c] = hop3[c] = lax.psum(hop1[c], "dp")
        elif op == "G3":
            *stored, dep = store(starts[c], outer, total[c], hop3[c], ff, stored, dep)
        elif op == "Q1":
            dep = back_rows((gpre0,) if c == 0 else (gprea, gpreb), expert_in, 1, dep)
            backs[c] = swap(dep)
        elif op == "Q2":
            dep = back_rows((act0,) if c == 0 else (acta, actb), expert_out, 0, dep)
            results[c] = swap(dep)
        elif op == "B":
            gtok, *grads[c] = backward(
                c, slots[c], segment_ids, tokens, cotangent, backs[c], saved[c], *weights,
                *gains, gtok, dep,
            )
            dep = grads[c][0]
        elif op == "W":
            dep = dense_grads(saved, grads, 16 * owners, dep)
            dense = lax.psum_scatter(dep, "expert", scatter_dimension=0, tiled=True)
        elif op == "A2":
            dense = lax.psum(after(dense, dep), "dp")
        elif op == "A3":
            dense = lax.all_gather(after(dense, dep), "expert", axis=0, tiled=True)
        elif op == "O":
            block_out = block_output(
                slots, [results[m] for m in range(micro)], [s[6] for s in saved], dep
            )
            dep = block_out
    return (
        block_out,
        gtok,
        *(dense[i * d : (i + 1) * d].astype(F32) for i in range(4)),
        dense[4 * d].astype(F32),
        dense[4 * d + 1].astype(F32),
        *stored,
    )


def solution(mesh):
    blocks, ids = P(None, ("dp", "expert"), None), P(None, ("dp", "expert"))
    owned = P("expert", None, None)
    return jax.shard_map(
        per_device,
        mesh=mesh,
        in_specs=(blocks, blocks, ids, P(), ids, P(), P(), P(), P(), P(), P(), owned, owned),
        out_specs=(blocks, blocks, P(), P(), P(), P(), P(), P(), owned, owned),
        check_vma=False,
    )
```

```python
import functools

import jax
import jax.numpy as jnp
from jax import lax
from jax.experimental import pallas as pl
from jax.experimental.pallas import tpu as pltpu
from jax.sharding import PartitionSpec as P

HEADS = 12
HEAD_DIM = 64
EPS = 1e-05
SCALE = HEAD_DIM ** (-0.5)
PAIR = 2 * HEAD_DIM
F32 = jnp.float32
BF16 = jnp.bfloat16


def dot(a, b, ca=1, cb=0):
    return lax.dot_general(a, b, (((ca,), (cb,)), ((), ())), preferred_element_type=F32)


def params():
    return pltpu.CompilerParams(
        dimension_semantics=("arbitrary",), vmem_limit_bytes=60 * 1024 * 1024
    )


LENGTH = [1340.0]


def cost():
    return pl.CostEstimate(
        flops=int(LENGTH[0] * 1.0e9), bytes_accessed=1 << 20, transcendentals=0
    )


def full(*shape):
    return pl.BlockSpec(shape, lambda *_: (0,) * len(shape))


ANY = pl.BlockSpec(memory_space=pl.ANY)


def iota(shape, axis):
    return lax.broadcasted_iota(jnp.int32, shape, axis)


def to_column(row):
    n = row.shape[1]
    eye = iota((n, n), 0) == iota((n, n), 1)
    return jnp.sum(jnp.where(eye, row, 0), axis=1, keepdims=True)


def spread(slots, values, count):
    total = None
    for slot, value in zip(slots, values):
        places = (iota((count, slot.shape[1]), 0) == slot).astype(BF16)
        part = dot(places, value)
        total = part if total is None else total + part
    return total.astype(BF16)


def route_kernel(
    owners, cap, ids_ref, table_ref, cot_ref, slot0_ref, slot1_ref, pack_ref, lines_ref
):
    micro, n = ids_ref.shape
    size = table_ref.shape[0]
    rows = lines_ref.shape[0]
    lines_ref[...] = jnp.zeros_like(lines_ref)
    for i in range(0, size, 128):
        width = min(128, size - i)
        lines_ref[i // 128, 0:width] = table_ref[pl.ds(i, width)]
    table = lines_ref[...].astype(BF16)
    kinds = -(-owners // 16) * 16
    before = (iota((n, n), 0) < iota((n, n), 1)).astype(BF16)
    slots = []
    for m, slot_ref in enumerate((slot0_ref, slot1_ref)):
        ids = ids_ref[pl.ds(m, 1), :]
        pick = (iota((rows, n), 0) == (ids >> 7)).astype(BF16)
        values = dot(table, pick, 0, 0)
        lane = ids & 127
        expert = jnp.sum(
            jnp.where(iota((128, n), 0) == lane, values, 0.0), axis=0, keepdims=True
        )
        named = iota((kinds, n), 0).astype(F32) == expert
        counts = dot(named.astype(BF16), before)
        rank = jnp.sum(jnp.where(named, counts, 0.0), axis=0, keepdims=True)
        slot = (expert * cap + rank).astype(jnp.int32)
        slot_ref[...] = slot
        slots.append(slot)
    pack_ref[...] = spread(slots[:1], (cot_ref[0],), pack_ref.shape[0])


def route(ids, table, cot, owners, cap):
    micro, n = ids.shape
    width = cot.shape[2]
    size = table.shape[0]
    rows = -(-size // 1024) * 8
    return pl.pallas_call(
        functools.partial(route_kernel, owners, cap),
        grid=(1,),
        in_specs=[full(micro, n), full(size), full(1, n, width)],
        out_specs=[full(1, n), full(1, n), full(owners * cap, width)],
        out_shape=[
            jax.ShapeDtypeStruct((1, n), jnp.int32),
            jax.ShapeDtypeStruct((1, n), jnp.int32),
            jax.ShapeDtypeStruct((owners * cap, width), BF16),
        ],
        scratch_shapes=[pltpu.VMEM((rows, 128), jnp.int32)],
        cost_estimate=cost(),
        compiler_params=params(),
    )(ids, table, cot)


def bias_of(seg):
    n = seg.shape[1]
    key, query = iota((n, n), 0), iota((n, n), 1)
    seen = (key <= query) & (to_column(seg) == seg)
    return jnp.where(seen, 0.0, -1e30)


def forward_kernel(
    m, cap, slot_ref, seg_ref, tok_ref, cot_ref, wq_ref, wk_ref, wv_ref, wo_ref, ga_ref, gf_ref,
    dep_ref, normed_ref, q_ref, k_ref, v_ref, lse_ref, mixed_ref, hidden_ref, last_ref, bias_ref,
):
    x = tok_ref[0].astype(F32)
    n = x.shape[0]
    r = lax.rsqrt(jnp.mean(x * x, axis=1, keepdims=True) + EPS)
    normed = (x * r * ga_ref[...]).astype(BF16)
    normed_ref[...] = normed
    q_ref[...] = (dot(normed, wq_ref[...]).astype(BF16) * SCALE).astype(BF16)
    k_ref[...] = dot(normed, wk_ref[...]).astype(BF16)
    v_ref[...] = dot(normed, wv_ref[...]).astype(BF16)
    bias_ref[...] = bias_of(seg_ref[pl.ds(m, 1), :])
    low = iota((n, PAIR), 1) < HEAD_DIM

    def pair(p, carry):
        cols = pl.ds(pl.multiple_of(p * PAIR, PAIR), PAIR)
        q, k, v = q_ref[:, cols], k_ref[:, cols], v_ref[:, cols]
        parts = []
        for h in range(2):
            mine = low if h == 0 else ~low
            s = dot(k, jnp.where(mine, q, 0), 1, 1) + bias_ref[...]
            top = jnp.max(s, axis=0, keepdims=True)
            e = jnp.exp(s - top)
            total = jnp.sum(e, axis=0, keepdims=True)
            lse_ref[pl.ds(2 * p + h, 1), :] = top + jnp.log(total)
            probs = (e * (1.0 / total)).astype(BF16)
            parts.append(dot(probs, v, 0, 0))
        mixed_ref[:, cols] = jnp.where(low, parts[0], parts[1]).astype(BF16)
        return carry

    lax.fori_loop(0, HEADS // 2, pair, 0)
    hidden = x + dot(mixed_ref[...], wo_ref[...])
    hidden_ref[...] = hidden
    r = lax.rsqrt(jnp.mean(hidden * hidden, axis=1, keepdims=True) + EPS)
    routed = (hidden * r * gf_ref[...]).astype(BF16)
    slot = slot_ref[...]
    if m == 0:
        last_ref[...] = spread((slot,), (routed,), last_ref.shape[0])
    else:
        slot = slot + slot // cap * cap
        last_ref[...] = spread((slot, slot + cap), (cot_ref[0], routed), last_ref.shape[0])


def forward(m, slot, seg, tokens, cot, wq, wk, wv, wo, ga, gf, slots, cap, dep):
    _, n, d = tokens.shape
    shapes = [
        ((n, d), BF16), ((n, d), BF16), ((n, d), BF16), ((n, d), BF16), ((16, n), F32),
        ((n, d), BF16), ((n, d), F32), ((slots * (m + 1), d), BF16),
    ]
    mat = pl.BlockSpec((1, n, d), lambda i: (m, 0, 0))
    return pl.pallas_call(
        functools.partial(forward_kernel, m, cap),
        grid=(1,),
        in_specs=[
            full(1, n), full(*seg.shape), mat, mat,
            full(d, d), full(d, d), full(d, d), full(d, d), full(1, d), full(1, d), ANY,
        ],
        out_specs=[full(*s) for s, _ in shapes],
        out_shape=[jax.ShapeDtypeStruct(s, t) for s, t in shapes],
        scratch_shapes=[pltpu.VMEM((n, n), F32)],
        cost_estimate=cost(),
        compiler_params=params(),
    )(slot, seg, tokens, cot, wq, wk, wv, wo, ga, gf, dep)


BLOCK = 256
HALF = 128


def hidden_units(x, g, win, wout):
    pre = dot(x, win)
    sig = jax.nn.sigmoid(pre)
    soft = pre * sig
    slope = sig + soft * (1.0 - sig)
    return soft.astype(BF16), (dot(g, wout, 1, 1) * slope).astype(BF16)


def put_chunk(chunk_ref, at, gout, gin):
    for i in range(BLOCK // HALF):
        part = slice(i * HALF, (i + 1) * HALF)
        chunk_ref[pl.ds(at + 2 * i * HALF, HALF), :] = gout[part].astype(BF16)
        chunk_ref[pl.ds(at + (2 * i + 1) * HALF, HALF), :] = gin[part].astype(BF16)


def units_kernel(rx_ref, gx_ref, win_ref, wout_ref, *rest):
    act_ref, gpre_ref = rest[-2:]
    act_ref[...], gpre_ref[...] = hidden_units(
        rx_ref[...], gx_ref[...], win_ref[0], wout_ref[0]
    )


def split_units_kernel(cap, both_ref, win_ref, wout_ref, *rest):
    act_ref, gpre_ref, rx_ref, gx_ref = rest[-4:]

    @pl.when(pl.program_id(0) == 0)
    def _():
        for e in range(rx_ref.shape[0] // cap):
            mine = pl.ds(e * cap, cap)
            gx_ref[mine, :] = both_ref[pl.ds(2 * e * cap, cap), :]
            rx_ref[mine, :] = both_ref[pl.ds((2 * e + 1) * cap, cap), :]

    act_ref[...], gpre_ref[...] = hidden_units(
        rx_ref[...], gx_ref[...], win_ref[0], wout_ref[0]
    )


def expert_units(c, units, given, win, wout, dep, cap=None):
    d = win.shape[1]
    rows = given[0].shape[0] // (1 if cap is None else 2)
    f = BLOCK
    columns = pl.BlockSpec((rows, f), lambda i: (0, i))
    kernel = units_kernel if cap is None else functools.partial(split_units_kernel, cap)
    return pl.pallas_call(
        kernel,
        grid=(units,),
        in_specs=[full(*x.shape) for x in given]
        + [
            pl.BlockSpec((1, d, f), lambda i: (0, 0, c + i)),
            pl.BlockSpec((1, f, d), lambda i: (0, c + i, 0)),
            ANY,
        ],
        out_specs=[columns] * 2 + ([full(rows, d)] * 2 if cap else []),
        out_shape=[jax.ShapeDtypeStruct((rows, units * f), BF16)] * 2
        + ([jax.ShapeDtypeStruct((rows, d), BF16)] * 2 if cap else []),
        cost_estimate=cost(),
        compiler_params=params(),
    )(*given, win, wout, dep)


def chunk_kernel(
    sizes, rx0_ref, rx1_ref, gx0_ref, gx1_ref, act0_ref, act1_ref, gpre0_ref, gpre1_ref, dep_ref,
    *chunk_refs,
):
    gout = dot(act0_ref[...], gx0_ref[...], 0, 0) + dot(act1_ref[...], gx1_ref[...], 0, 0)
    gin = dot(gpre0_ref[...], rx0_ref[...], 0, 0) + dot(gpre1_ref[...], rx1_ref[...], 0, 0)
    step = 0
    for size, ref in zip(sizes, chunk_refs):
        for i in range(size):

            @pl.when(pl.program_id(0) == step)
            def _(ref=ref, i=i):
                put_chunk(ref, 2 * BLOCK * i, gout, gin)

            step += 1


def expert_grads(sizes, rx, gx, acts, gpres, at, dep):
    rows, d = rx[0].shape
    f = BLOCK
    columns = [pl.BlockSpec((rows, f), lambda i, k=k: (0, k + i)) for k in at]
    shapes = [(size * 2 * f, d) for size in sizes]
    return pl.pallas_call(
        functools.partial(chunk_kernel, sizes),
        grid=(sum(sizes),),
        in_specs=[full(rows, d)] * 4 + columns * 2 + [ANY],
        out_specs=[full(*x) for x in shapes],
        out_shape=[jax.ShapeDtypeStruct(x, BF16) for x in shapes],
        cost_estimate=cost(),
        compiler_params=params(),
    )(*rx, *gx, *acts, *gpres, dep)


def rows_kernel(side, *refs):
    *parts, w_ref, _, o_ref = refs
    total, start = None, 0
    for a_ref in parts:
        count = a_ref.shape[1]
        units = pl.ds(start, count)
        w = w_ref[0, :, units] if side == 1 else w_ref[0, units, :]
        term = dot(a_ref[...], w, 1, side)
        total = term if total is None else total + term
        start += count
    o_ref[...] = total.astype(BF16)


def back_rows(parts, w, side, dep, blk=256):
    rows = parts[0].shape[0]
    d = w.shape[1 + (1 - side)]
    return pl.pallas_call(
        functools.partial(rows_kernel, side),
        grid=(rows // blk,),
        in_specs=[pl.BlockSpec((blk, a.shape[1]), lambda i: (i, 0)) for a in parts]
        + [full(*w.shape), ANY],
        out_specs=pl.BlockSpec((blk, d), lambda i: (i, 0)),
        out_shape=jax.ShapeDtypeStruct((rows, d), BF16),
        cost_estimate=cost(),
        compiler_params=params(),
    )(*parts, w, dep)


def backward_kernel(
    m, slot_ref, seg_ref, tok_ref, cot_ref, back_ref, normed_ref, q_ref, k_ref, v_ref, lse_ref,
    hidden_ref, wq_ref, wk_ref, wv_ref, wo_ref, ga_ref, gf_ref, *rest,
):
    gtok_ref, gattn_ref, gq_ref, gk_ref, gv_ref, gain_ref = rest[-13:-7]
    bias_ref, gm_ref, gh_ref, hq_ref, hk_ref, hv_ref, sem = rest[-7:]
    copies = [
        pltpu.make_async_copy(a, b, sem.at[i])
        for i, (a, b) in enumerate(((wq_ref, hq_ref), (wk_ref, hk_ref), (wv_ref, hv_ref)))
    ]
    for copy in copies:
        copy.start()
    n, d = normed_ref.shape
    slots = back_ref.shape[0]
    places = (iota((n, slots), 1) == to_column(slot_ref[...])).astype(BF16)
    grad_routed = dot(places, back_ref[...])
    hidden = hidden_ref[...]
    r = lax.rsqrt(jnp.mean(hidden * hidden, axis=1, keepdims=True) + EPS)
    unit = hidden * r
    g = grad_routed * gf_ref[...]
    grad_hidden = cot_ref[0].astype(F32) + r * (
        g - unit * jnp.mean(g * unit, axis=1, keepdims=True)
    )
    gh_ref[...] = grad_hidden
    gain_ref[pl.ds(1, 1), :] = jnp.sum(grad_routed * unit, axis=0, keepdims=True)
    grad_attn = grad_hidden.astype(BF16)
    gattn_ref[...] = grad_attn
    gm_ref[...] = dot(grad_attn, wo_ref[...], 1, 1).astype(BF16)
    bias_ref[...] = bias_of(seg_ref[pl.ds(m, 1), :])
    low = iota((n, PAIR), 1) < HEAD_DIM

    def pair(p, carry):
        cols = pl.ds(pl.multiple_of(p * PAIR, PAIR), PAIR)
        q, k, v, gm = q_ref[:, cols], k_ref[:, cols], v_ref[:, cols], gm_ref[:, cols]
        gqs, gks, gvs = [], [], []
        for h in range(2):
            mine = low if h == 0 else ~low
            s = dot(k, jnp.where(mine, q, 0), 1, 1) + bias_ref[...]
            probs = jnp.exp(s - lse_ref[pl.ds(2 * p + h, 1), :])
            gvs.append(dot(probs.astype(BF16), gm))
            gp = dot(v, jnp.where(mine, gm, 0), 1, 1)
            shared = jnp.sum(probs * gp, axis=0, keepdims=True)
            gs = (probs * (gp - shared)).astype(BF16)
            gks.append(dot(gs, q))
            gqs.append(dot(gs, k, 0, 0))
        gq_ref[:, cols] = (jnp.where(low, gqs[0], gqs[1]) * SCALE).astype(BF16)
        gk_ref[:, cols] = jnp.where(low, gks[0], gks[1]).astype(BF16)
        gv_ref[:, cols] = jnp.where(low, gvs[0], gvs[1]).astype(BF16)
        return carry

    lax.fori_loop(0, HEADS // 2, pair, 0)
    for copy in copies:
        copy.wait()
    grad_normed = (
        dot(gq_ref[...], hq_ref[...], 1, 1)
        + dot(gk_ref[...], hk_ref[...], 1, 1)
        + dot(gv_ref[...], hv_ref[...], 1, 1)
    )
    x = tok_ref[0].astype(F32)
    r = lax.rsqrt(jnp.mean(x * x, axis=1, keepdims=True) + EPS)
    unit = x * r
    gain_ref[pl.ds(0, 1), :] = jnp.sum(grad_normed * unit, axis=0, keepdims=True)
    g = grad_normed * ga_ref[...]
    gtok_ref[0] = (
        gh_ref[...] + r * (g - unit * jnp.mean(g * unit, axis=1, keepdims=True))
    ).astype(BF16)


def backward(m, slot, seg, tokens, cot, back, saved, wq, wk, wv, wo, ga, gf, held, dep):
    micro, n, d = tokens.shape
    normed, q, k, v, lse, _, hidden = saved
    mat = pl.BlockSpec((1, n, d), lambda i: (m, 0, 0))
    extra = [dep] if held is None else [dep, held]
    return pl.pallas_call(
        functools.partial(backward_kernel, m),
        grid=(1,),
        in_specs=[full(1, n), full(*seg.shape), mat, mat, full(*back.shape)]
        + [full(*a.shape) for a in (normed, q, k, v, lse, hidden)]
        + [ANY] * 3 + [full(d, d)] + [full(1, d)] * 2 + [ANY] * len(extra),
        out_specs=[mat] + [full(n, d)] * 4 + [full(8, d)],
        out_shape=[jax.ShapeDtypeStruct((micro, n, d), BF16)]
        + [jax.ShapeDtypeStruct((n, d), BF16)] * 4
        + [jax.ShapeDtypeStruct((8, d), F32)],
        scratch_shapes=[
            pltpu.VMEM((n, n), F32), pltpu.VMEM((n, d), BF16), pltpu.VMEM((n, d), F32),
            pltpu.VMEM((d, d), BF16), pltpu.VMEM((d, d), BF16), pltpu.VMEM((d, d), BF16),
            pltpu.SemaphoreType.DMA((3,)),
        ],
        cost_estimate=cost(),
        compiler_params=params(),
        input_output_aliases={} if held is None else {18: 0},
    )(slot, seg, tokens, cot, back, normed, q, k, v, lse, hidden, wq, wk, wv, wo, ga, gf, *extra)


def weights_kernel(n0, n1, x0, x1, q0, q1, k0, k1, v0, v1, a0, a1, gain0, gain1, dep_ref, o_ref):
    d = n0.shape[1]
    for i, (l0, l1, r0, r1) in enumerate(
        ((n0, n1, q0, q1), (n0, n1, k0, k1), (n0, n1, v0, v1), (x0, x1, a0, a1))
    ):
        both = dot(l0[...], r0[...], 0, 0) + dot(l1[...], r1[...], 0, 0)
        o_ref[pl.ds(i * d, d), :] = both.astype(BF16)
    rest = o_ref.shape[0] - 4 * d
    line = iota((rest, d), 0)
    gain = gain0[...] + gain1[...]
    o_ref[pl.ds(4 * d, rest), :] = jnp.where(
        line == 0, gain[0:1, :], jnp.where(line == 1, gain[1:2, :], 0.0)
    ).astype(BF16)


def dense_grads(saved, grads, rest, dep):
    n, d = saved[0][0].shape
    pairs = [(saved[0][0], saved[1][0]), (saved[0][5], saved[1][5])]
    pairs += [(grads[0][i], grads[1][i]) for i in (1, 2, 3, 0, 4)]
    flat = [a for both in pairs for a in both]
    return pl.pallas_call(
        weights_kernel,
        grid=(1,),
        in_specs=[full(*a.shape) for a in flat] + [ANY],
        out_specs=full(4 * d + rest, d),
        out_shape=jax.ShapeDtypeStruct((4 * d + rest, d), BF16),
        cost_estimate=cost(),
        compiler_params=params(),
    )(*flat, dep)


def output_kernel(s0_ref, s1_ref, b0_ref, b1_ref, h0_ref, h1_ref, dep_ref, o_ref):
    n = o_ref.shape[1]
    for m, (s_ref, b_ref, h_ref) in enumerate(((s0_ref, b0_ref, h0_ref), (s1_ref, b1_ref, h1_ref))):
        places = (iota((n, b_ref.shape[0]), 1) == to_column(s_ref[...])).astype(BF16)
        o_ref[m] = (h_ref[...] + dot(places, b_ref[...])).astype(BF16)


def block_output(slots, backs, hiddens, dep):
    micro = len(slots)
    n, d = hiddens[0].shape
    flat = [*slots, *backs, *hiddens]
    return pl.pallas_call(
        output_kernel,
        grid=(1,),
        in_specs=[full(*a.shape) for a in flat] + [ANY],
        out_specs=full(micro, n, d),
        out_shape=jax.ShapeDtypeStruct((micro, n, d), BF16),
        cost_estimate=cost(),
        compiler_params=params(),
    )(*flat, dep)


def after(x, dep):
    return lax.optimization_barrier((x, dep))[0]


def add(a, b, dep):
    return (after(a, dep).astype(F32) + b.astype(F32)).astype(BF16)


def store_kernel(flag_ref, a_ref, b_ref, *rest):
    gin_ref, gout_ref, token_ref = rest[-3:]
    token_ref[...] = jnp.zeros_like(token_ref)

    def put(ref):
        gout_ref[0] = ref[pl.ds(0, HALF), :].astype(F32)
        gin_ref[0] = ref[pl.ds(HALF, HALF), :].astype(F32).T

    @pl.when(flag_ref[0] == 1)
    def _():
        put(b_ref)

    @pl.when(flag_ref[0] != 1)
    def _():
        put(a_ref)


def store(c, flag, a, b, ff, held, dep):
    rows, d = a.shape
    spec = pl.BlockSpec((2 * HALF, d), lambda i: (i, 0))
    base = c * (BLOCK // HALF)
    extra = ([] if held is None else list(held)) + [dep]
    return pl.pallas_call(
        store_kernel,
        grid=(rows // (2 * HALF),),
        in_specs=[pl.BlockSpec(memory_space=pltpu.SMEM), spec, spec] + [ANY] * len(extra),
        out_specs=[
            pl.BlockSpec((1, d, HALF), lambda i: (0, 0, base + i)),
            pl.BlockSpec((1, HALF, d), lambda i: (0, base + i, 0)),
            full(8, 128),
        ],
        out_shape=[
            jax.ShapeDtypeStruct((1, d, ff), F32),
            jax.ShapeDtypeStruct((1, ff, d), F32),
            jax.ShapeDtypeStruct((8, 128), F32),
        ],
        input_output_aliases={} if held is None else {3: 0, 4: 1},
        cost_estimate=cost(),
        compiler_params=params(),
    )(flag, a, b, *extra)


SIZES = (2, 2, 2, 2, 2, 2)
GROUPS = ((0,), (1,), (2, 3, 4, 5))


PLAN = (
    ("F", 0, 2185.0), ("Fa", 1, 460.0), ("D", 0, 5.8), ("S1", 0, 0.0), ("Fb", 1, 1610.0),
    ("Q1", 0, 0.0), ("D", 1, 5.8), ("S1", 1, 0.0), ("G1", 0, 0.0), ("Q1", 1, 2.6),
    ("D", 2, 0.0), ("S1", 2, 0.0), ("G1", 1, 0.0), ("B", 0, 2012.5), ("G2", 0, 0.0),
    ("S1", 3, 0.0), ("G1", 2, 0.0), ("B", 1, 10.1), ("S1", 4, 0.0), ("G2", 1, 0.0),
    ("G1", 3, 0.0), ("W", 0, 1184.5), ("G2", 2, 0.0), ("G1", 4, 0.0), ("S1", 5, 0.0),
    ("A2", 0, 0.0), ("G3", 0, 345.0), ("G3", 1, 27.6), ("G2", 3, 0.0), ("Q2", 0, 41.4),
    ("Q2", 1, 41.4), ("G1", 5, 0.0), ("A3", 0, 0.0), ("G2", 4, 0.0), ("G3", 2, 0.0),
    ("G3", 3, 1.7), ("G3", 4, 345.0), ("G2", 5, 0.0), ("O", 0, 40.5), ("G3", 5, 27.6),
)


def per_device(
    tokens, cotangent, token_ids, hash_table, segment_ids, query_weight, key_weight,
    value_weight, output_weight, gain_attn, gain_ffn, expert_in, expert_out,
):
    micro, n, d = tokens.shape
    ff = expert_in.shape[2]
    owners = lax.axis_size("expert")
    depth = lax.axis_size("dp")
    cap = 2 * n // owners
    weights = (query_weight, key_weight, value_weight, output_weight)
    LENGTH[0] = 1340.0
    gains = (gain_attn.reshape(1, d), gain_ffn.reshape(1, d))
    place = lax.axis_index("dp")
    outer = ((place == 0) | (place == depth - 1)).astype(jnp.int32).reshape(1)
    def swap(x):
        return lax.all_to_all(x, "expert", split_axis=0, concat_axis=0, tiled=True)

    slot0, slot1, packed = route(token_ids, hash_table, cotangent, owners, cap)
    slots = (slot0, slot1)
    gx = {0: swap(packed)}
    *kept0, packed0 = forward(
        0, slot0, segment_ids, tokens, cotangent, *weights, *gains, owners * cap, cap, packed
    )
    rx = {0: swap(after(packed0, gx[0]))}
    *kept1, packed1 = forward(
        1, slot1, segment_ids, tokens, cotangent, *weights, *gains, owners * cap, cap, packed0
    )
    both = swap(after(packed1, rx[0]))
    saved = (tuple(kept0), tuple(kept1))
    dep = packed1

    starts = [sum(SIZES[:i]) for i in range(len(SIZES))]
    chunk, hop1, hop2, hop3, sum1, total = {}, {}, {}, {}, {}, {}
    stored = gtok = dense = block_out = None
    backs, results, grads = {}, {}, {}
    for op, c, LENGTH[0] in PLAN:
        if op == "F":
            act0, gpre0 = expert_units(0, ff // BLOCK, (rx[0], gx[0]), expert_in, expert_out, dep)
            dep = act0
        elif op == "Fa":
            acta, gprea, rx[1], gx[1] = expert_units(
                0, SIZES[0], (both,), expert_in, expert_out, dep, cap
            )
            dep = rx[1]
        elif op == "Fb":
            actb, gpreb = expert_units(
                SIZES[0], ff // BLOCK - SIZES[0], (rx[1], gx[1]), expert_in, expert_out, dep
            )
            dep = actb
        elif op == "D":
            mine = (acta, gprea) if c == 0 else (actb, gpreb)
            first = starts[GROUPS[c][0]]
            made = expert_grads(
                [SIZES[i] for i in GROUPS[c]], (rx[0], rx[1]), (gx[0], gx[1]), (act0, mine[0]),
                (gpre0, mine[1]), (first, 0 if c == 0 else first - SIZES[0]), dep,
            )
            chunk.update(zip(GROUPS[c], made))
            dep = made[0]
        elif op == "S1":
            x = after(chunk[c], dep)
            hop1[c] = lax.ppermute(x, "dp", [(0, 1), (3, 2)]) if depth == 4 else x
        elif op == "G1":
            if depth == 4:
                sum1[c] = add(chunk[c], hop1[c], dep)
                hop2[c] = lax.ppermute(sum1[c], "dp", [(1, 2), (2, 1)])
                dep = sum1[c]
        elif op == "G2":
            if depth == 4:
                total[c] = add(sum1[c], hop2[c], dep)
                hop3[c] = lax.ppermute(total[c], "dp", [(1, 0), (2, 3)])
                dep = total[c]
            else:
                total[c] = hop3[c] = lax.psum(hop1[c], "dp")
        elif op == "G3":
            *stored, dep = store(starts[c], outer, total[c], hop3[c], ff, stored, dep)
        elif op == "Q1":
            dep = back_rows((gpre0,) if c == 0 else (gprea, gpreb), expert_in, 1, dep)
            backs[c] = swap(dep)
        elif op == "Q2":
            dep = back_rows((act0,) if c == 0 else (acta, actb), expert_out, 0, dep)
            results[c] = swap(dep)
        elif op == "B":
            gtok, *grads[c] = backward(
                c, slots[c], segment_ids, tokens, cotangent, backs[c], saved[c], *weights,
                *gains, gtok, dep,
            )
            dep = grads[c][0]
        elif op == "W":
            dep = dense_grads(saved, grads, 16 * owners, dep)
            dense = lax.psum_scatter(dep, "expert", scatter_dimension=0, tiled=True)
        elif op == "A2":
            dense = lax.psum(after(dense, dep), "dp")
        elif op == "A3":
            dense = lax.all_gather(after(dense, dep), "expert", axis=0, tiled=True)
        elif op == "O":
            block_out = block_output(
                slots, [results[m] for m in range(micro)], [s[6] for s in saved], dep
            )
            dep = block_out
    return (
        block_out,
        gtok,
        *(dense[i * d : (i + 1) * d].astype(F32) for i in range(4)),
        dense[4 * d].astype(F32),
        dense[4 * d + 1].astype(F32),
        *stored,
    )


def solution(mesh):
    blocks, ids = P(None, ("dp", "expert"), None), P(None, ("dp", "expert"))
    owned = P("expert", None, None)
    return jax.shard_map(
        per_device,
        mesh=mesh,
        in_specs=(blocks, blocks, ids, P(), ids, P(), P(), P(), P(), P(), P(), owned, owned),
        out_specs=(blocks, blocks, P(), P(), P(), P(), P(), P(), owned, owned),
        check_vma=False,
    )
```

```python
import functools

import jax
import jax.numpy as jnp
from jax import lax
from jax.experimental import pallas as pl
from jax.experimental.pallas import tpu as pltpu
from jax.sharding import PartitionSpec as P

HEADS = 12
HEAD_DIM = 64
EPS = 1e-05
SCALE = HEAD_DIM ** (-0.5)
PAIR = 2 * HEAD_DIM
F32 = jnp.float32
BF16 = jnp.bfloat16


def dot(a, b, ca=1, cb=0):
    return lax.dot_general(a, b, (((ca,), (cb,)), ((), ())), preferred_element_type=F32)


def params():
    return pltpu.CompilerParams(
        dimension_semantics=("arbitrary",), vmem_limit_bytes=60 * 1024 * 1024
    )


LENGTH = [1340.0]


def cost():
    return pl.CostEstimate(
        flops=int(LENGTH[0] * 1.0e9), bytes_accessed=1 << 20, transcendentals=0
    )


def full(*shape):
    return pl.BlockSpec(shape, lambda *_: (0,) * len(shape))


ANY = pl.BlockSpec(memory_space=pl.ANY)


def iota(shape, axis):
    return lax.broadcasted_iota(jnp.int32, shape, axis)


def to_column(row):
    n = row.shape[1]
    eye = iota((n, n), 0) == iota((n, n), 1)
    return jnp.sum(jnp.where(eye, row, 0), axis=1, keepdims=True)


def spread(slots, values, count):
    total = None
    for slot, value in zip(slots, values):
        places = (iota((count, slot.shape[1]), 0) == slot).astype(BF16)
        part = dot(places, value)
        total = part if total is None else total + part
    return total.astype(BF16)


def route_kernel(
    owners, cap, ids_ref, table_ref, cot_ref, slot0_ref, slot1_ref, pack_ref, lines_ref
):
    micro, n = ids_ref.shape
    size = table_ref.shape[0]
    rows = lines_ref.shape[0]
    lines_ref[...] = jnp.zeros_like(lines_ref)
    for i in range(0, size, 128):
        width = min(128, size - i)
        lines_ref[i // 128, 0:width] = table_ref[pl.ds(i, width)]
    table = lines_ref[...].astype(BF16)
    kinds = -(-owners // 16) * 16
    before = (iota((n, n), 0) < iota((n, n), 1)).astype(BF16)
    slots = []
    for m, slot_ref in enumerate((slot0_ref, slot1_ref)):
        ids = ids_ref[pl.ds(m, 1), :]
        pick = (iota((rows, n), 0) == (ids >> 7)).astype(BF16)
        values = dot(table, pick, 0, 0)
        lane = ids & 127
        expert = jnp.sum(
            jnp.where(iota((128, n), 0) == lane, values, 0.0), axis=0, keepdims=True
        )
        named = iota((kinds, n), 0).astype(F32) == expert
        counts = dot(named.astype(BF16), before)
        rank = jnp.sum(jnp.where(named, counts, 0.0), axis=0, keepdims=True)
        slot = (expert * cap + rank).astype(jnp.int32)
        slot_ref[...] = slot
        slots.append(slot)
    pack_ref[...] = spread(slots[:1], (cot_ref[0],), pack_ref.shape[0])


def route(ids, table, cot, owners, cap):
    micro, n = ids.shape
    width = cot.shape[2]
    size = table.shape[0]
    rows = -(-size // 1024) * 8
    return pl.pallas_call(
        functools.partial(route_kernel, owners, cap),
        grid=(1,),
        in_specs=[full(micro, n), full(size), full(1, n, width)],
        out_specs=[full(1, n), full(1, n), full(owners * cap, width)],
        out_shape=[
            jax.ShapeDtypeStruct((1, n), jnp.int32),
            jax.ShapeDtypeStruct((1, n), jnp.int32),
            jax.ShapeDtypeStruct((owners * cap, width), BF16),
        ],
        scratch_shapes=[pltpu.VMEM((rows, 128), jnp.int32)],
        cost_estimate=cost(),
        compiler_params=params(),
    )(ids, table, cot)


def bias_of(seg):
    n = seg.shape[1]
    key, query = iota((n, n), 0), iota((n, n), 1)
    seen = (key <= query) & (to_column(seg) == seg)
    return jnp.where(seen, 0.0, -1e30)


def forward_kernel(
    m, cap, slot_ref, seg_ref, tok_ref, cot_ref, wq_ref, wk_ref, wv_ref, wo_ref, ga_ref, gf_ref,
    dep_ref, normed_ref, q_ref, k_ref, v_ref, lse_ref, mixed_ref, hidden_ref, last_ref, bias_ref,
):
    x = tok_ref[0].astype(F32)
    n = x.shape[0]
    r = lax.rsqrt(jnp.mean(x * x, axis=1, keepdims=True) + EPS)
    normed = (x * r * ga_ref[...]).astype(BF16)
    normed_ref[...] = normed
    q_ref[...] = (dot(normed, wq_ref[...]).astype(BF16) * SCALE).astype(BF16)
    k_ref[...] = dot(normed, wk_ref[...]).astype(BF16)
    v_ref[...] = dot(normed, wv_ref[...]).astype(BF16)
    bias_ref[...] = bias_of(seg_ref[pl.ds(m, 1), :])
    low = iota((n, PAIR), 1) < HEAD_DIM

    def pair(p, carry):
        cols = pl.ds(pl.multiple_of(p * PAIR, PAIR), PAIR)
        q, k, v = q_ref[:, cols], k_ref[:, cols], v_ref[:, cols]
        parts = []
        for h in range(2):
            mine = low if h == 0 else ~low
            s = dot(k, jnp.where(mine, q, 0), 1, 1) + bias_ref[...]
            top = jnp.max(s, axis=0, keepdims=True)
            e = jnp.exp(s - top)
            total = jnp.sum(e, axis=0, keepdims=True)
            lse_ref[pl.ds(2 * p + h, 1), :] = top + jnp.log(total)
            probs = (e * (1.0 / total)).astype(BF16)
            parts.append(dot(probs, v, 0, 0))
        mixed_ref[:, cols] = jnp.where(low, parts[0], parts[1]).astype(BF16)
        return carry

    lax.fori_loop(0, HEADS // 2, pair, 0)
    hidden = x + dot(mixed_ref[...], wo_ref[...])
    hidden_ref[...] = hidden
    r = lax.rsqrt(jnp.mean(hidden * hidden, axis=1, keepdims=True) + EPS)
    routed = (hidden * r * gf_ref[...]).astype(BF16)
    slot = slot_ref[...]
    if m == 0:
        last_ref[...] = spread((slot,), (routed,), last_ref.shape[0])
    else:
        slot = slot + slot // cap * cap
        last_ref[...] = spread((slot, slot + cap), (cot_ref[0], routed), last_ref.shape[0])


def forward(m, slot, seg, tokens, cot, wq, wk, wv, wo, ga, gf, slots, cap, dep):
    _, n, d = tokens.shape
    shapes = [
        ((n, d), BF16), ((n, d), BF16), ((n, d), BF16), ((n, d), BF16), ((16, n), F32),
        ((n, d), BF16), ((n, d), F32), ((slots * (m + 1), d), BF16),
    ]
    mat = pl.BlockSpec((1, n, d), lambda i: (m, 0, 0))
    return pl.pallas_call(
        functools.partial(forward_kernel, m, cap),
        grid=(1,),
        in_specs=[
            full(1, n), full(*seg.shape), mat, mat,
            full(d, d), full(d, d), full(d, d), full(d, d), full(1, d), full(1, d), ANY,
        ],
        out_specs=[full(*s) for s, _ in shapes],
        out_shape=[jax.ShapeDtypeStruct(s, t) for s, t in shapes],
        scratch_shapes=[pltpu.VMEM((n, n), F32)],
        cost_estimate=cost(),
        compiler_params=params(),
    )(slot, seg, tokens, cot, wq, wk, wv, wo, ga, gf, dep)


BLOCK = 256
HALF = 128


def hidden_units(x, g, win, wout):
    pre = dot(x, win)
    sig = jax.nn.sigmoid(pre)
    soft = pre * sig
    slope = sig + soft * (1.0 - sig)
    return soft.astype(BF16), (dot(g, wout, 1, 1) * slope).astype(BF16)


def put_chunk(chunk_ref, at, gout, gin):
    for i in range(BLOCK // HALF):
        part = slice(i * HALF, (i + 1) * HALF)
        chunk_ref[pl.ds(at + 2 * i * HALF, HALF), :] = gout[part].astype(BF16)
        chunk_ref[pl.ds(at + (2 * i + 1) * HALF, HALF), :] = gin[part].astype(BF16)


def units_kernel(rx_ref, gx_ref, win_ref, wout_ref, *rest):
    act_ref, gpre_ref = rest[-2:]
    act_ref[...], gpre_ref[...] = hidden_units(
        rx_ref[...], gx_ref[...], win_ref[0], wout_ref[0]
    )


def split_units_kernel(cap, both_ref, win_ref, wout_ref, *rest):
    act_ref, gpre_ref, rx_ref, gx_ref = rest[-4:]

    @pl.when(pl.program_id(0) == 0)
    def _():
        for e in range(rx_ref.shape[0] // cap):
            mine = pl.ds(e * cap, cap)
            gx_ref[mine, :] = both_ref[pl.ds(2 * e * cap, cap), :]
            rx_ref[mine, :] = both_ref[pl.ds((2 * e + 1) * cap, cap), :]

    act_ref[...], gpre_ref[...] = hidden_units(
        rx_ref[...], gx_ref[...], win_ref[0], wout_ref[0]
    )


def expert_units(c, units, given, win, wout, dep, cap=None):
    d = win.shape[1]
    rows = given[0].shape[0] // (1 if cap is None else 2)
    f = BLOCK
    columns = pl.BlockSpec((rows, f), lambda i: (0, i))
    kernel = units_kernel if cap is None else functools.partial(split_units_kernel, cap)
    return pl.pallas_call(
        kernel,
        grid=(units,),
        in_specs=[full(*x.shape) for x in given]
        + [
            pl.BlockSpec((1, d, f), lambda i: (0, 0, c + i)),
            pl.BlockSpec((1, f, d), lambda i: (0, c + i, 0)),
            ANY,
        ],
        out_specs=[columns] * 2 + ([full(rows, d)] * 2 if cap else []),
        out_shape=[jax.ShapeDtypeStruct((rows, units * f), BF16)] * 2
        + ([jax.ShapeDtypeStruct((rows, d), BF16)] * 2 if cap else []),
        cost_estimate=cost(),
        compiler_params=params(),
    )(*given, win, wout, dep)


def chunk_kernel(
    sizes, rx0_ref, rx1_ref, gx0_ref, gx1_ref, act0_ref, act1_ref, gpre0_ref, gpre1_ref, dep_ref,
    *chunk_refs,
):
    gout = dot(act0_ref[...], gx0_ref[...], 0, 0) + dot(act1_ref[...], gx1_ref[...], 0, 0)
    gin = dot(gpre0_ref[...], rx0_ref[...], 0, 0) + dot(gpre1_ref[...], rx1_ref[...], 0, 0)
    step = 0
    for size, ref in zip(sizes, chunk_refs):
        for i in range(size):

            @pl.when(pl.program_id(0) == step)
            def _(ref=ref, i=i):
                put_chunk(ref, 2 * BLOCK * i, gout, gin)

            step += 1


def expert_grads(sizes, rx, gx, acts, gpres, at, dep):
    rows, d = rx[0].shape
    f = BLOCK
    columns = [pl.BlockSpec((rows, f), lambda i, k=k: (0, k + i)) for k in at]
    shapes = [(size * 2 * f, d) for size in sizes]
    return pl.pallas_call(
        functools.partial(chunk_kernel, sizes),
        grid=(sum(sizes),),
        in_specs=[full(rows, d)] * 4 + columns * 2 + [ANY],
        out_specs=[full(*x) for x in shapes],
        out_shape=[jax.ShapeDtypeStruct(x, BF16) for x in shapes],
        cost_estimate=cost(),
        compiler_params=params(),
    )(*rx, *gx, *acts, *gpres, dep)


def rows_kernel(side, *refs):
    *parts, w_ref, _, o_ref = refs
    total, start = None, 0
    for a_ref in parts:
        count = a_ref.shape[1]
        units = pl.ds(start, count)
        w = w_ref[0, :, units] if side == 1 else w_ref[0, units, :]
        term = dot(a_ref[...], w, 1, side)
        total = term if total is None else total + term
        start += count
    o_ref[...] = total.astype(BF16)


def back_rows(parts, w, side, dep, blk=256):
    rows = parts[0].shape[0]
    d = w.shape[1 + (1 - side)]
    return pl.pallas_call(
        functools.partial(rows_kernel, side),
        grid=(rows // blk,),
        in_specs=[pl.BlockSpec((blk, a.shape[1]), lambda i: (i, 0)) for a in parts]
        + [full(*w.shape), ANY],
        out_specs=pl.BlockSpec((blk, d), lambda i: (i, 0)),
        out_shape=jax.ShapeDtypeStruct((rows, d), BF16),
        cost_estimate=cost(),
        compiler_params=params(),
    )(*parts, w, dep)


def backward_kernel(
    m, slot_ref, seg_ref, tok_ref, cot_ref, back_ref, normed_ref, q_ref, k_ref, v_ref, lse_ref,
    hidden_ref, wq_ref, wk_ref, wv_ref, wo_ref, ga_ref, gf_ref, *rest,
):
    gtok_ref, gattn_ref, gq_ref, gk_ref, gv_ref, gain_ref = rest[-16:-10]
    bias_ref, gm_ref, gh_ref, hq_ref, hk_ref, hv_ref, iq_ref, ik_ref, iv_ref, sem = rest[-10:]
    copies = [
        pltpu.make_async_copy(a, b, sem.at[i])
        for i, (a, b) in enumerate(
            (
                (q_ref, iq_ref), (k_ref, ik_ref), (v_ref, iv_ref),
                (wq_ref, hq_ref), (wk_ref, hk_ref), (wv_ref, hv_ref),
            )
        )
    ]
    for copy in copies:
        copy.start()
    n, d = hidden_ref.shape
    slots = back_ref.shape[0]
    places = (iota((n, slots), 1) == to_column(slot_ref[...])).astype(BF16)
    grad_routed = dot(places, back_ref[...])
    hidden = hidden_ref[...]
    r = lax.rsqrt(jnp.mean(hidden * hidden, axis=1, keepdims=True) + EPS)
    unit = hidden * r
    g = grad_routed * gf_ref[...]
    grad_hidden = cot_ref[0].astype(F32) + r * (
        g - unit * jnp.mean(g * unit, axis=1, keepdims=True)
    )
    gh_ref[...] = grad_hidden
    gain_ref[pl.ds(1, 1), :] = jnp.sum(grad_routed * unit, axis=0, keepdims=True)
    grad_attn = grad_hidden.astype(BF16)
    gattn_ref[...] = grad_attn
    gm_ref[...] = dot(grad_attn, wo_ref[...], 1, 1).astype(BF16)
    bias_ref[...] = bias_of(seg_ref[pl.ds(m, 1), :])
    low = iota((n, PAIR), 1) < HEAD_DIM
    for copy in copies[:3]:
        copy.wait()

    def pair(p, carry):
        cols = pl.ds(pl.multiple_of(p * PAIR, PAIR), PAIR)
        q, k, v, gm = iq_ref[:, cols], ik_ref[:, cols], iv_ref[:, cols], gm_ref[:, cols]
        gqs, gks, gvs = [], [], []
        for h in range(2):
            mine = low if h == 0 else ~low
            s = dot(k, jnp.where(mine, q, 0), 1, 1) + bias_ref[...]
            probs = jnp.exp(s - lse_ref[pl.ds(2 * p + h, 1), :])
            gvs.append(dot(probs.astype(BF16), gm))
            gp = dot(v, jnp.where(mine, gm, 0), 1, 1)
            shared = jnp.sum(probs * gp, axis=0, keepdims=True)
            gs = (probs * (gp - shared)).astype(BF16)
            gks.append(dot(gs, q))
            gqs.append(dot(gs, k, 0, 0))
        gq_ref[:, cols] = (jnp.where(low, gqs[0], gqs[1]) * SCALE).astype(BF16)
        gk_ref[:, cols] = jnp.where(low, gks[0], gks[1]).astype(BF16)
        gv_ref[:, cols] = jnp.where(low, gvs[0], gvs[1]).astype(BF16)
        return carry

    lax.fori_loop(0, HEADS // 2, pair, 0)
    for copy in copies[3:]:
        copy.wait()
    grad_normed = (
        dot(gq_ref[...], hq_ref[...], 1, 1)
        + dot(gk_ref[...], hk_ref[...], 1, 1)
        + dot(gv_ref[...], hv_ref[...], 1, 1)
    )
    x = tok_ref[0].astype(F32)
    r = lax.rsqrt(jnp.mean(x * x, axis=1, keepdims=True) + EPS)
    unit = x * r
    gain_ref[pl.ds(0, 1), :] = jnp.sum(grad_normed * unit, axis=0, keepdims=True)
    g = grad_normed * ga_ref[...]
    gtok_ref[0] = (
        gh_ref[...] + r * (g - unit * jnp.mean(g * unit, axis=1, keepdims=True))
    ).astype(BF16)


def backward(m, slot, seg, tokens, cot, back, saved, wq, wk, wv, wo, ga, gf, held, dep):
    micro, n, d = tokens.shape
    normed, q, k, v, lse, _, hidden = saved
    mat = pl.BlockSpec((1, n, d), lambda i: (m, 0, 0))
    extra = [dep] if held is None else [dep, held]
    return pl.pallas_call(
        functools.partial(backward_kernel, m),
        grid=(1,),
        in_specs=[full(1, n), full(*seg.shape), mat, mat, full(*back.shape)]
        + [ANY] * 4 + [full(*lse.shape), full(*hidden.shape)]
        + [ANY] * 3 + [full(d, d)] + [full(1, d)] * 2 + [ANY] * len(extra),
        out_specs=[mat] + [full(n, d)] * 4 + [full(8, d)],
        out_shape=[jax.ShapeDtypeStruct((micro, n, d), BF16)]
        + [jax.ShapeDtypeStruct((n, d), BF16)] * 4
        + [jax.ShapeDtypeStruct((8, d), F32)],
        scratch_shapes=[
            pltpu.VMEM((n, n), F32), pltpu.VMEM((n, d), BF16), pltpu.VMEM((n, d), F32),
            pltpu.VMEM((d, d), BF16), pltpu.VMEM((d, d), BF16), pltpu.VMEM((d, d), BF16),
            pltpu.VMEM((n, d), BF16), pltpu.VMEM((n, d), BF16), pltpu.VMEM((n, d), BF16),
            pltpu.SemaphoreType.DMA((6,)),
        ],
        cost_estimate=cost(),
        compiler_params=params(),
        input_output_aliases={} if held is None else {18: 0},
    )(slot, seg, tokens, cot, back, normed, q, k, v, lse, hidden, wq, wk, wv, wo, ga, gf, *extra)


def weights_kernel(n0, n1, x0, x1, q0, q1, k0, k1, v0, v1, a0, a1, gain0, gain1, dep_ref, o_ref):
    d = n0.shape[1]
    for i, (l0, l1, r0, r1) in enumerate(
        ((n0, n1, q0, q1), (n0, n1, k0, k1), (n0, n1, v0, v1), (x0, x1, a0, a1))
    ):
        both = dot(l0[...], r0[...], 0, 0) + dot(l1[...], r1[...], 0, 0)
        o_ref[pl.ds(i * d, d), :] = both.astype(BF16)
    rest = o_ref.shape[0] - 4 * d
    line = iota((rest, d), 0)
    gain = gain0[...] + gain1[...]
    o_ref[pl.ds(4 * d, rest), :] = jnp.where(
        line == 0, gain[0:1, :], jnp.where(line == 1, gain[1:2, :], 0.0)
    ).astype(BF16)


def dense_grads(saved, grads, rest, dep):
    n, d = saved[0][0].shape
    pairs = [(saved[0][0], saved[1][0]), (saved[0][5], saved[1][5])]
    pairs += [(grads[0][i], grads[1][i]) for i in (1, 2, 3, 0, 4)]
    flat = [a for both in pairs for a in both]
    return pl.pallas_call(
        weights_kernel,
        grid=(1,),
        in_specs=[full(*a.shape) for a in flat] + [ANY],
        out_specs=full(4 * d + rest, d),
        out_shape=jax.ShapeDtypeStruct((4 * d + rest, d), BF16),
        cost_estimate=cost(),
        compiler_params=params(),
    )(*flat, dep)


def output_kernel(s0_ref, s1_ref, b0_ref, b1_ref, h0_ref, h1_ref, dep_ref, o_ref):
    n = o_ref.shape[1]
    for m, (s_ref, b_ref, h_ref) in enumerate(((s0_ref, b0_ref, h0_ref), (s1_ref, b1_ref, h1_ref))):
        places = (iota((n, b_ref.shape[0]), 1) == to_column(s_ref[...])).astype(BF16)
        o_ref[m] = (h_ref[...] + dot(places, b_ref[...])).astype(BF16)


def block_output(slots, backs, hiddens, dep):
    micro = len(slots)
    n, d = hiddens[0].shape
    flat = [*slots, *backs, *hiddens]
    return pl.pallas_call(
        output_kernel,
        grid=(1,),
        in_specs=[full(*a.shape) for a in flat] + [ANY],
        out_specs=full(micro, n, d),
        out_shape=jax.ShapeDtypeStruct((micro, n, d), BF16),
        cost_estimate=cost(),
        compiler_params=params(),
    )(*flat, dep)


def after(x, dep):
    return lax.optimization_barrier((x, dep))[0]


def add(a, b, dep):
    return (after(a, dep).astype(F32) + b.astype(F32)).astype(BF16)


def store_kernel(flag_ref, a_ref, b_ref, *rest):
    gin_ref, gout_ref, token_ref = rest[-3:]
    token_ref[...] = jnp.zeros_like(token_ref)

    def put(ref):
        gout_ref[0] = ref[pl.ds(0, HALF), :].astype(F32)
        gin_ref[0] = ref[pl.ds(HALF, HALF), :].astype(F32).T

    @pl.when(flag_ref[0] == 1)
    def _():
        put(b_ref)

    @pl.when(flag_ref[0] != 1)
    def _():
        put(a_ref)


def store(c, flag, a, b, ff, held, dep):
    rows, d = a.shape
    spec = pl.BlockSpec((2 * HALF, d), lambda i: (i, 0))
    base = c * (BLOCK // HALF)
    extra = ([] if held is None else list(held)) + [dep]
    return pl.pallas_call(
        store_kernel,
        grid=(rows // (2 * HALF),),
        in_specs=[pl.BlockSpec(memory_space=pltpu.SMEM), spec, spec] + [ANY] * len(extra),
        out_specs=[
            pl.BlockSpec((1, d, HALF), lambda i: (0, 0, base + i)),
            pl.BlockSpec((1, HALF, d), lambda i: (0, base + i, 0)),
            full(8, 128),
        ],
        out_shape=[
            jax.ShapeDtypeStruct((1, d, ff), F32),
            jax.ShapeDtypeStruct((1, ff, d), F32),
            jax.ShapeDtypeStruct((8, 128), F32),
        ],
        input_output_aliases={} if held is None else {3: 0, 4: 1},
        cost_estimate=cost(),
        compiler_params=params(),
    )(flag, a, b, *extra)


SIZES = (2, 2, 2, 2, 2, 2)
GROUPS = ((0,), (1,), (2, 3, 4, 5))


PLAN = (
    ("F", 0, 2185.0), ("Fa", 1, 460.0), ("D", 0, 5.8), ("S1", 0, 0.0), ("Fb", 1, 1610.0),
    ("Q1", 0, 0.0), ("D", 1, 5.8), ("S1", 1, 0.0), ("G1", 0, 0.0), ("Q1", 1, 2.6),
    ("D", 2, 0.0), ("S1", 2, 0.0), ("G1", 1, 0.0), ("B", 0, 2012.5), ("G2", 0, 0.0),
    ("S1", 3, 0.0), ("G1", 2, 0.0), ("B", 1, 10.1), ("S1", 4, 0.0), ("G2", 1, 0.0),
    ("G1", 3, 0.0), ("W", 0, 1184.5), ("G2", 2, 0.0), ("G1", 4, 0.0), ("S1", 5, 0.0),
    ("A2", 0, 0.0), ("G3", 0, 345.0), ("G3", 1, 27.6), ("G2", 3, 0.0), ("Q2", 0, 41.4),
    ("Q2", 1, 41.4), ("G1", 5, 0.0), ("A3", 0, 0.0), ("G2", 4, 0.0), ("G3", 2, 0.0),
    ("G3", 3, 1.7), ("G3", 4, 345.0), ("G2", 5, 0.0), ("O", 0, 40.5), ("G3", 5, 27.6),
)


def per_device(
    tokens, cotangent, token_ids, hash_table, segment_ids, query_weight, key_weight,
    value_weight, output_weight, gain_attn, gain_ffn, expert_in, expert_out,
):
    micro, n, d = tokens.shape
    ff = expert_in.shape[2]
    owners = lax.axis_size("expert")
    depth = lax.axis_size("dp")
    cap = 2 * n // owners
    weights = (query_weight, key_weight, value_weight, output_weight)
    LENGTH[0] = 1340.0
    gains = (gain_attn.reshape(1, d), gain_ffn.reshape(1, d))
    place = lax.axis_index("dp")
    outer = ((place == 0) | (place == depth - 1)).astype(jnp.int32).reshape(1)
    def swap(x):
        return lax.all_to_all(x, "expert", split_axis=0, concat_axis=0, tiled=True)

    slot0, slot1, packed = route(token_ids, hash_table, cotangent, owners, cap)
    slots = (slot0, slot1)
    gx = {0: swap(packed)}
    *kept0, packed0 = forward(
        0, slot0, segment_ids, tokens, cotangent, *weights, *gains, owners * cap, cap, packed
    )
    rx = {0: swap(after(packed0, gx[0]))}
    *kept1, packed1 = forward(
        1, slot1, segment_ids, tokens, cotangent, *weights, *gains, owners * cap, cap, packed0
    )
    both = swap(after(packed1, rx[0]))
    saved = (tuple(kept0), tuple(kept1))
    dep = packed1

    starts = [sum(SIZES[:i]) for i in range(len(SIZES))]
    chunk, hop1, hop2, hop3, sum1, total = {}, {}, {}, {}, {}, {}
    stored = gtok = dense = block_out = None
    backs, results, grads = {}, {}, {}
    for op, c, LENGTH[0] in PLAN:
        if op == "F":
            act0, gpre0 = expert_units(0, ff // BLOCK, (rx[0], gx[0]), expert_in, expert_out, dep)
            dep = act0
        elif op == "Fa":
            acta, gprea, rx[1], gx[1] = expert_units(
                0, SIZES[0], (both,), expert_in, expert_out, dep, cap
            )
            dep = rx[1]
        elif op == "Fb":
            actb, gpreb = expert_units(
                SIZES[0], ff // BLOCK - SIZES[0], (rx[1], gx[1]), expert_in, expert_out, dep
            )
            dep = actb
        elif op == "D":
            mine = (acta, gprea) if c == 0 else (actb, gpreb)
            first = starts[GROUPS[c][0]]
            made = expert_grads(
                [SIZES[i] for i in GROUPS[c]], (rx[0], rx[1]), (gx[0], gx[1]), (act0, mine[0]),
                (gpre0, mine[1]), (first, 0 if c == 0 else first - SIZES[0]), dep,
            )
            chunk.update(zip(GROUPS[c], made))
            dep = made[0]
        elif op == "S1":
            x = after(chunk[c], dep)
            hop1[c] = lax.ppermute(x, "dp", [(0, 1), (3, 2)]) if depth == 4 else x
        elif op == "G1":
            if depth == 4:
                sum1[c] = add(chunk[c], hop1[c], dep)
                hop2[c] = lax.ppermute(sum1[c], "dp", [(1, 2), (2, 1)])
                dep = sum1[c]
        elif op == "G2":
            if depth == 4:
                total[c] = add(sum1[c], hop2[c], dep)
                hop3[c] = lax.ppermute(total[c], "dp", [(1, 0), (2, 3)])
                dep = total[c]
            else:
                total[c] = hop3[c] = lax.psum(hop1[c], "dp")
        elif op == "G3":
            *stored, dep = store(starts[c], outer, total[c], hop3[c], ff, stored, dep)
        elif op == "Q1":
            dep = back_rows((gpre0,) if c == 0 else (gprea, gpreb), expert_in, 1, dep)
            backs[c] = swap(dep)
        elif op == "Q2":
            dep = back_rows((act0,) if c == 0 else (acta, actb), expert_out, 0, dep)
            results[c] = swap(dep)
        elif op == "B":
            gtok, *grads[c] = backward(
                c, slots[c], segment_ids, tokens, cotangent, backs[c], saved[c], *weights,
                *gains, gtok, dep,
            )
            dep = grads[c][0]
        elif op == "W":
            dep = dense_grads(saved, grads, 16 * owners, dep)
            dense = lax.psum_scatter(dep, "expert", scatter_dimension=0, tiled=True)
        elif op == "A2":
            dense = lax.psum(after(dense, dep), "dp")
        elif op == "A3":
            dense = lax.all_gather(after(dense, dep), "expert", axis=0, tiled=True)
        elif op == "O":
            block_out = block_output(
                slots, [results[m] for m in range(micro)], [s[6] for s in saved], dep
            )
            dep = block_out
    return (
        block_out,
        gtok,
        *(dense[i * d : (i + 1) * d].astype(F32) for i in range(4)),
        dense[4 * d].astype(F32),
        dense[4 * d + 1].astype(F32),
        *stored,
    )


def solution(mesh):
    blocks, ids = P(None, ("dp", "expert"), None), P(None, ("dp", "expert"))
    owned = P("expert", None, None)
    return jax.shard_map(
        per_device,
        mesh=mesh,
        in_specs=(blocks, blocks, ids, P(), ids, P(), P(), P(), P(), P(), P(), owned, owned),
        out_specs=(blocks, blocks, P(), P(), P(), P(), P(), P(), owned, owned),
        check_vma=False,
    )
```

```python
import functools

import jax
import jax.numpy as jnp
from jax import lax
from jax.experimental import pallas as pl
from jax.experimental.pallas import tpu as pltpu
from jax.sharding import PartitionSpec as P

HEADS = 12
HEAD_DIM = 64
EPS = 1e-05
SCALE = HEAD_DIM ** (-0.5)
PAIR = 2 * HEAD_DIM
F32 = jnp.float32
BF16 = jnp.bfloat16


def dot(a, b, ca=1, cb=0):
    return lax.dot_general(a, b, (((ca,), (cb,)), ((), ())), preferred_element_type=F32)


def params():
    return pltpu.CompilerParams(
        dimension_semantics=("arbitrary",), vmem_limit_bytes=60 * 1024 * 1024
    )


LENGTH = [1340.0]


def cost():
    return pl.CostEstimate(
        flops=int(LENGTH[0] * 1.0e9), bytes_accessed=1 << 20, transcendentals=0
    )


def full(*shape):
    return pl.BlockSpec(shape, lambda *_: (0,) * len(shape))


ANY = pl.BlockSpec(memory_space=pl.ANY)


def iota(shape, axis):
    return lax.broadcasted_iota(jnp.int32, shape, axis)


def to_column(row):
    n = row.shape[1]
    eye = iota((n, n), 0) == iota((n, n), 1)
    return jnp.sum(jnp.where(eye, row, 0), axis=1, keepdims=True)


def spread(slots, values, count):
    total = None
    for slot, value in zip(slots, values):
        places = (iota((count, slot.shape[1]), 0) == slot).astype(BF16)
        part = dot(places, value)
        total = part if total is None else total + part
    return total.astype(BF16)


def route_kernel(
    owners, cap, ids_ref, table_ref, cot_ref, slot0_ref, slot1_ref, pack_ref, lines_ref
):
    micro, n = ids_ref.shape
    size = table_ref.shape[0]
    rows = lines_ref.shape[0]
    lines_ref[...] = jnp.zeros_like(lines_ref)
    for i in range(0, size, 128):
        width = min(128, size - i)
        lines_ref[i // 128, 0:width] = table_ref[pl.ds(i, width)]
    table = lines_ref[...].astype(BF16)
    kinds = -(-owners // 16) * 16
    before = (iota((n, n), 0) < iota((n, n), 1)).astype(BF16)
    slots = []
    for m, slot_ref in enumerate((slot0_ref, slot1_ref)):
        ids = ids_ref[pl.ds(m, 1), :]
        pick = (iota((rows, n), 0) == (ids >> 7)).astype(BF16)
        values = dot(table, pick, 0, 0)
        lane = ids & 127
        expert = jnp.sum(
            jnp.where(iota((128, n), 0) == lane, values, 0.0), axis=0, keepdims=True
        )
        named = iota((kinds, n), 0).astype(F32) == expert
        counts = dot(named.astype(BF16), before)
        rank = jnp.sum(jnp.where(named, counts, 0.0), axis=0, keepdims=True)
        slot = (expert * cap + rank).astype(jnp.int32)
        slot_ref[...] = slot
        slots.append(slot)
    pack_ref[...] = spread(slots[:1], (cot_ref[0],), pack_ref.shape[0])


def route(ids, table, cot, owners, cap):
    micro, n = ids.shape
    width = cot.shape[2]
    size = table.shape[0]
    rows = -(-size // 1024) * 8
    return pl.pallas_call(
        functools.partial(route_kernel, owners, cap),
        grid=(1,),
        in_specs=[full(micro, n), full(size), full(1, n, width)],
        out_specs=[full(1, n), full(1, n), full(owners * cap, width)],
        out_shape=[
            jax.ShapeDtypeStruct((1, n), jnp.int32),
            jax.ShapeDtypeStruct((1, n), jnp.int32),
            jax.ShapeDtypeStruct((owners * cap, width), BF16),
        ],
        scratch_shapes=[pltpu.VMEM((rows, 128), jnp.int32)],
        cost_estimate=cost(),
        compiler_params=params(),
    )(ids, table, cot)


def bias_of(seg):
    n = seg.shape[1]
    key, query = iota((n, n), 0), iota((n, n), 1)
    seen = (key <= query) & (to_column(seg) == seg)
    return jnp.where(seen, 0.0, -1e30)


def forward_kernel(
    m, cap, slot_ref, seg_ref, tok_ref, cot_ref, wq_ref, wk_ref, wv_ref, wo_ref, ga_ref, gf_ref,
    dep_ref, normed_ref, q_ref, k_ref, v_ref, lse_ref, mixed_ref, hidden_ref, last_ref, bias_ref,
):
    x = tok_ref[0].astype(F32)
    n = x.shape[0]
    r = lax.rsqrt(jnp.mean(x * x, axis=1, keepdims=True) + EPS)
    normed = (x * r * ga_ref[...]).astype(BF16)
    normed_ref[...] = normed
    q_ref[...] = (dot(normed, wq_ref[...]).astype(BF16) * SCALE).astype(BF16)
    k_ref[...] = dot(normed, wk_ref[...]).astype(BF16)
    v_ref[...] = dot(normed, wv_ref[...]).astype(BF16)
    bias_ref[...] = bias_of(seg_ref[pl.ds(m, 1), :])
    low = iota((n, PAIR), 1) < HEAD_DIM

    def pair(p, carry):
        cols = pl.ds(pl.multiple_of(p * PAIR, PAIR), PAIR)
        q, k, v = q_ref[:, cols], k_ref[:, cols], v_ref[:, cols]
        parts = []
        for h in range(2):
            mine = low if h == 0 else ~low
            s = dot(k, jnp.where(mine, q, 0), 1, 1) + bias_ref[...]
            top = jnp.max(s, axis=0, keepdims=True)
            e = jnp.exp(s - top)
            total = jnp.sum(e, axis=0, keepdims=True)
            lse_ref[pl.ds(2 * p + h, 1), :] = top + jnp.log(total)
            probs = (e * (1.0 / total)).astype(BF16)
            parts.append(dot(probs, v, 0, 0))
        mixed_ref[:, cols] = jnp.where(low, parts[0], parts[1]).astype(BF16)
        return carry

    lax.fori_loop(0, HEADS // 2, pair, 0)
    hidden = x + dot(mixed_ref[...], wo_ref[...])
    hidden_ref[...] = hidden
    r = lax.rsqrt(jnp.mean(hidden * hidden, axis=1, keepdims=True) + EPS)
    routed = (hidden * r * gf_ref[...]).astype(BF16)
    slot = slot_ref[...]
    if m == 0:
        last_ref[...] = spread((slot,), (routed,), last_ref.shape[0])
    else:
        slot = slot + slot // cap * cap
        last_ref[...] = spread((slot, slot + cap), (cot_ref[0], routed), last_ref.shape[0])


def forward(m, slot, seg, tokens, cot, wq, wk, wv, wo, ga, gf, slots, cap, dep):
    _, n, d = tokens.shape
    shapes = [
        ((n, d), BF16), ((n, d), BF16), ((n, d), BF16), ((n, d), BF16), ((16, n), F32),
        ((n, d), BF16), ((n, d), F32), ((slots * (m + 1), d), BF16),
    ]
    mat = pl.BlockSpec((1, n, d), lambda i: (m, 0, 0))
    return pl.pallas_call(
        functools.partial(forward_kernel, m, cap),
        grid=(1,),
        in_specs=[
            full(1, n), full(*seg.shape), mat, mat,
            full(d, d), full(d, d), full(d, d), full(d, d), full(1, d), full(1, d), ANY,
        ],
        out_specs=[full(*s) for s, _ in shapes],
        out_shape=[jax.ShapeDtypeStruct(s, t) for s, t in shapes],
        scratch_shapes=[pltpu.VMEM((n, n), F32)],
        cost_estimate=cost(),
        compiler_params=params(),
    )(slot, seg, tokens, cot, wq, wk, wv, wo, ga, gf, dep)


BLOCK = 256
HALF = 128


def hidden_units(x, g, win, wout):
    pre = dot(x, win)
    sig = jax.nn.sigmoid(pre)
    soft = pre * sig
    slope = sig + soft * (1.0 - sig)
    return soft.astype(BF16), (dot(g, wout, 1, 1) * slope).astype(BF16)


def put_chunk(chunk_ref, at, gout, gin):
    for i in range(BLOCK // HALF):
        part = slice(i * HALF, (i + 1) * HALF)
        chunk_ref[pl.ds(at + 2 * i * HALF, HALF), :] = gout[part].astype(BF16)
        chunk_ref[pl.ds(at + (2 * i + 1) * HALF, HALF), :] = gin[part].astype(BF16)


def units_kernel(rx_ref, gx_ref, win_ref, wout_ref, *rest):
    act_ref, gpre_ref = rest[-2:]
    act_ref[...], gpre_ref[...] = hidden_units(
        rx_ref[...], gx_ref[...], win_ref[0], wout_ref[0]
    )


def split_units_kernel(cap, both_ref, win_ref, wout_ref, *rest):
    act_ref, gpre_ref, rx_ref, gx_ref = rest[-4:]

    @pl.when(pl.program_id(0) == 0)
    def _():
        for e in range(rx_ref.shape[0] // cap):
            mine = pl.ds(e * cap, cap)
            gx_ref[mine, :] = both_ref[pl.ds(2 * e * cap, cap), :]
            rx_ref[mine, :] = both_ref[pl.ds((2 * e + 1) * cap, cap), :]

    act_ref[...], gpre_ref[...] = hidden_units(
        rx_ref[...], gx_ref[...], win_ref[0], wout_ref[0]
    )


def expert_units(c, units, given, win, wout, dep, cap=None):
    d = win.shape[1]
    rows = given[0].shape[0] // (1 if cap is None else 2)
    f = BLOCK
    columns = pl.BlockSpec((rows, f), lambda i: (0, i))
    kernel = units_kernel if cap is None else functools.partial(split_units_kernel, cap)
    return pl.pallas_call(
        kernel,
        grid=(units,),
        in_specs=[full(*x.shape) for x in given]
        + [
            pl.BlockSpec((1, d, f), lambda i: (0, 0, c + i)),
            pl.BlockSpec((1, f, d), lambda i: (0, c + i, 0)),
            ANY,
        ],
        out_specs=[columns] * 2 + ([full(rows, d)] * 2 if cap else []),
        out_shape=[jax.ShapeDtypeStruct((rows, units * f), BF16)] * 2
        + ([jax.ShapeDtypeStruct((rows, d), BF16)] * 2 if cap else []),
        cost_estimate=cost(),
        compiler_params=params(),
    )(*given, win, wout, dep)


def chunk_kernel(
    sizes, rx0_ref, rx1_ref, gx0_ref, gx1_ref, act0_ref, act1_ref, gpre0_ref, gpre1_ref, dep_ref,
    *chunk_refs,
):
    gout = dot(act0_ref[...], gx0_ref[...], 0, 0) + dot(act1_ref[...], gx1_ref[...], 0, 0)
    gin = dot(gpre0_ref[...], rx0_ref[...], 0, 0) + dot(gpre1_ref[...], rx1_ref[...], 0, 0)
    step = 0
    for size, ref in zip(sizes, chunk_refs):
        for i in range(size):

            @pl.when(pl.program_id(0) == step)
            def _(ref=ref, i=i):
                put_chunk(ref, 2 * BLOCK * i, gout, gin)

            step += 1


def expert_grads(sizes, rx, gx, acts, gpres, at, dep):
    rows, d = rx[0].shape
    f = BLOCK
    columns = [pl.BlockSpec((rows, f), lambda i, k=k: (0, k + i)) for k in at]
    shapes = [(size * 2 * f, d) for size in sizes]
    return pl.pallas_call(
        functools.partial(chunk_kernel, sizes),
        grid=(sum(sizes),),
        in_specs=[full(rows, d)] * 4 + columns * 2 + [ANY],
        out_specs=[full(*x) for x in shapes],
        out_shape=[jax.ShapeDtypeStruct(x, BF16) for x in shapes],
        cost_estimate=cost(),
        compiler_params=params(),
    )(*rx, *gx, *acts, *gpres, dep)


def rows_kernel(side, *refs):
    *parts, w_ref, _, o_ref = refs
    total, start = None, 0
    for a_ref in parts:
        count = a_ref.shape[1]
        units = pl.ds(start, count)
        w = w_ref[0, :, units] if side == 1 else w_ref[0, units, :]
        term = dot(a_ref[...], w, 1, side)
        total = term if total is None else total + term
        start += count
    o_ref[...] = total.astype(BF16)


def back_rows(parts, w, side, dep, blk=256):
    rows = parts[0].shape[0]
    d = w.shape[1 + (1 - side)]
    return pl.pallas_call(
        functools.partial(rows_kernel, side),
        grid=(rows // blk,),
        in_specs=[pl.BlockSpec((blk, a.shape[1]), lambda i: (i, 0)) for a in parts]
        + [full(*w.shape), ANY],
        out_specs=pl.BlockSpec((blk, d), lambda i: (i, 0)),
        out_shape=jax.ShapeDtypeStruct((rows, d), BF16),
        cost_estimate=cost(),
        compiler_params=params(),
    )(*parts, w, dep)


def backward_kernel(
    m, slot_ref, seg_ref, tok_ref, cot_ref, back_ref, normed_ref, q_ref, k_ref, v_ref, lse_ref,
    hidden_ref, wq_ref, wk_ref, wv_ref, wo_ref, ga_ref, gf_ref, *rest,
):
    gtok_ref, gattn_ref, gq_ref, gk_ref, gv_ref, gain_ref = rest[-16:-10]
    bias_ref, gm_ref, gh_ref, hq_ref, hk_ref, hv_ref, iq_ref, ik_ref, iv_ref, sem = rest[-10:]
    copies = [
        pltpu.make_async_copy(a, b, sem.at[i])
        for i, (a, b) in enumerate(
            (
                (q_ref, iq_ref), (k_ref, ik_ref), (v_ref, iv_ref),
                (wq_ref, hq_ref), (wk_ref, hk_ref), (wv_ref, hv_ref),
            )
        )
    ]
    for copy in copies:
        copy.start()
    n, d = hidden_ref.shape
    slots = back_ref.shape[0]
    places = (iota((n, slots), 1) == to_column(slot_ref[...])).astype(BF16)
    grad_routed = dot(places, back_ref[...])
    hidden = hidden_ref[...]
    r = lax.rsqrt(jnp.mean(hidden * hidden, axis=1, keepdims=True) + EPS)
    unit = hidden * r
    g = grad_routed * gf_ref[...]
    grad_hidden = cot_ref[0].astype(F32) + r * (
        g - unit * jnp.mean(g * unit, axis=1, keepdims=True)
    )
    gh_ref[...] = grad_hidden
    gain_ref[pl.ds(1, 1), :] = jnp.sum(grad_routed * unit, axis=0, keepdims=True)
    grad_attn = grad_hidden.astype(BF16)
    gattn_ref[...] = grad_attn
    gm_ref[...] = dot(grad_attn, wo_ref[...], 1, 1).astype(BF16)
    bias_ref[...] = bias_of(seg_ref[pl.ds(m, 1), :])
    low = iota((n, PAIR), 1) < HEAD_DIM
    for copy in copies[:3]:
        copy.wait()

    def pair(p, carry):
        cols = pl.ds(pl.multiple_of(p * PAIR, PAIR), PAIR)
        q, k, v, gm = iq_ref[:, cols], ik_ref[:, cols], iv_ref[:, cols], gm_ref[:, cols]
        gqs, gks, gvs = [], [], []
        for h in range(2):
            mine = low if h == 0 else ~low
            s = dot(k, jnp.where(mine, q, 0), 1, 1) + bias_ref[...]
            probs = jnp.exp(s - lse_ref[pl.ds(2 * p + h, 1), :])
            gvs.append(dot(probs.astype(BF16), gm))
            gp = dot(v, jnp.where(mine, gm, 0), 1, 1)
            shared = jnp.sum(probs * gp, axis=0, keepdims=True)
            gs = (probs * (gp - shared)).astype(BF16)
            gks.append(dot(gs, q))
            gqs.append(dot(gs, k, 0, 0))
        gq_ref[:, cols] = (jnp.where(low, gqs[0], gqs[1]) * SCALE).astype(BF16)
        gk_ref[:, cols] = jnp.where(low, gks[0], gks[1]).astype(BF16)
        gv_ref[:, cols] = jnp.where(low, gvs[0], gvs[1]).astype(BF16)
        return carry

    lax.fori_loop(0, HEADS // 2, pair, 0)
    for copy in copies[3:]:
        copy.wait()
    grad_normed = (
        dot(gq_ref[...], hq_ref[...], 1, 1)
        + dot(gk_ref[...], hk_ref[...], 1, 1)
        + dot(gv_ref[...], hv_ref[...], 1, 1)
    )
    x = tok_ref[0].astype(F32)
    r = lax.rsqrt(jnp.mean(x * x, axis=1, keepdims=True) + EPS)
    unit = x * r
    gain_ref[pl.ds(0, 1), :] = jnp.sum(grad_normed * unit, axis=0, keepdims=True)
    g = grad_normed * ga_ref[...]
    gtok_ref[0] = (
        gh_ref[...] + r * (g - unit * jnp.mean(g * unit, axis=1, keepdims=True))
    ).astype(BF16)


def backward(m, slot, seg, tokens, cot, back, saved, wq, wk, wv, wo, ga, gf, held, dep):
    micro, n, d = tokens.shape
    normed, q, k, v, lse, _, hidden = saved
    mat = pl.BlockSpec((1, n, d), lambda i: (m, 0, 0))
    extra = [dep] if held is None else [dep, held]
    return pl.pallas_call(
        functools.partial(backward_kernel, m),
        grid=(1,),
        in_specs=[full(1, n), full(*seg.shape), mat, mat, full(*back.shape)]
        + [ANY] * 4 + [full(*lse.shape), full(*hidden.shape)]
        + [ANY] * 3 + [full(d, d)] + [full(1, d)] * 2 + [ANY] * len(extra),
        out_specs=[mat] + [full(n, d)] * 4 + [full(8, d)],
        out_shape=[jax.ShapeDtypeStruct((micro, n, d), BF16)]
        + [jax.ShapeDtypeStruct((n, d), BF16)] * 4
        + [jax.ShapeDtypeStruct((8, d), F32)],
        scratch_shapes=[
            pltpu.VMEM((n, n), F32), pltpu.VMEM((n, d), BF16), pltpu.VMEM((n, d), F32),
            pltpu.VMEM((d, d), BF16), pltpu.VMEM((d, d), BF16), pltpu.VMEM((d, d), BF16),
            pltpu.VMEM((n, d), BF16), pltpu.VMEM((n, d), BF16), pltpu.VMEM((n, d), BF16),
            pltpu.SemaphoreType.DMA((6,)),
        ],
        cost_estimate=cost(),
        compiler_params=params(),
        input_output_aliases={} if held is None else {18: 0},
    )(slot, seg, tokens, cot, back, normed, q, k, v, lse, hidden, wq, wk, wv, wo, ga, gf, *extra)


def weights_kernel(n0, n1, x0, x1, q0, q1, k0, k1, v0, v1, a0, a1, gain0, gain1, dep_ref, o_ref):
    d = n0.shape[1]
    for i, (l0, l1, r0, r1) in enumerate(
        ((n0, n1, q0, q1), (n0, n1, k0, k1), (n0, n1, v0, v1), (x0, x1, a0, a1))
    ):
        both = dot(l0[...], r0[...], 0, 0) + dot(l1[...], r1[...], 0, 0)
        o_ref[pl.ds(i * d, d), :] = both.astype(BF16)
    rest = o_ref.shape[0] - 4 * d
    line = iota((rest, d), 0)
    gain = gain0[...] + gain1[...]
    o_ref[pl.ds(4 * d, rest), :] = jnp.where(
        line == 0, gain[0:1, :], jnp.where(line == 1, gain[1:2, :], 0.0)
    ).astype(BF16)


def dense_grads(saved, grads, rest, dep):
    n, d = saved[0][0].shape
    pairs = [(saved[0][0], saved[1][0]), (saved[0][5], saved[1][5])]
    pairs += [(grads[0][i], grads[1][i]) for i in (1, 2, 3, 0, 4)]
    flat = [a for both in pairs for a in both]
    return pl.pallas_call(
        weights_kernel,
        grid=(1,),
        in_specs=[full(*a.shape) for a in flat] + [ANY],
        out_specs=full(4 * d + rest, d),
        out_shape=jax.ShapeDtypeStruct((4 * d + rest, d), BF16),
        cost_estimate=cost(),
        compiler_params=params(),
    )(*flat, dep)


def output_kernel(s0_ref, s1_ref, b0_ref, b1_ref, h0_ref, h1_ref, dep_ref, o_ref):
    n = o_ref.shape[1]
    for m, (s_ref, b_ref, h_ref) in enumerate(((s0_ref, b0_ref, h0_ref), (s1_ref, b1_ref, h1_ref))):
        places = (iota((n, b_ref.shape[0]), 1) == to_column(s_ref[...])).astype(BF16)
        o_ref[m] = (h_ref[...] + dot(places, b_ref[...])).astype(BF16)


def block_output(slots, backs, hiddens, dep):
    micro = len(slots)
    n, d = hiddens[0].shape
    flat = [*slots, *backs, *hiddens]
    return pl.pallas_call(
        output_kernel,
        grid=(1,),
        in_specs=[full(*a.shape) for a in flat] + [ANY],
        out_specs=full(micro, n, d),
        out_shape=jax.ShapeDtypeStruct((micro, n, d), BF16),
        cost_estimate=cost(),
        compiler_params=params(),
    )(*flat, dep)


def after(x, dep):
    return lax.optimization_barrier((x, dep))[0]


def add(a, b, dep):
    return (after(a, dep).astype(F32) + b.astype(F32)).astype(BF16)


def store_kernel(flag_ref, a_ref, b_ref, *rest):
    gin_ref, gout_ref, token_ref = rest[-3:]
    token_ref[...] = jnp.zeros_like(token_ref)

    def put(ref):
        gout_ref[0] = ref[pl.ds(0, HALF), :].astype(F32)
        gin_ref[0] = ref[pl.ds(HALF, HALF), :].astype(F32).T

    @pl.when(flag_ref[0] == 1)
    def _():
        put(b_ref)

    @pl.when(flag_ref[0] != 1)
    def _():
        put(a_ref)


def store(c, flag, a, b, ff, held, dep):
    rows, d = a.shape
    spec = pl.BlockSpec((2 * HALF, d), lambda i: (i, 0))
    base = c * (BLOCK // HALF)
    extra = ([] if held is None else list(held)) + [dep]
    return pl.pallas_call(
        store_kernel,
        grid=(rows // (2 * HALF),),
        in_specs=[pl.BlockSpec(memory_space=pltpu.SMEM), spec, spec] + [ANY] * len(extra),
        out_specs=[
            pl.BlockSpec((1, d, HALF), lambda i: (0, 0, base + i)),
            pl.BlockSpec((1, HALF, d), lambda i: (0, base + i, 0)),
            full(8, 128),
        ],
        out_shape=[
            jax.ShapeDtypeStruct((1, d, ff), F32),
            jax.ShapeDtypeStruct((1, ff, d), F32),
            jax.ShapeDtypeStruct((8, 128), F32),
        ],
        input_output_aliases={} if held is None else {3: 0, 4: 1},
        cost_estimate=cost(),
        compiler_params=params(),
    )(flag, a, b, *extra)


SIZES = (2, 2, 2, 2, 2, 2)
GROUPS = ((0,), (1,), (2, 3, 4, 5))


PLAN = (
    ("F", 0, 2185.0), ("Fa", 1, 460.0), ("D", 0, 5.8), ("S1", 0, 0.0), ("Fb", 1, 1610.0),
    ("Q1", 0, 0.0), ("D", 1, 5.8), ("S1", 1, 0.0), ("G1", 0, 0.0), ("Q1", 1, 2.6),
    ("D", 2, 0.0), ("S1", 2, 0.0), ("G1", 1, 0.0), ("G2", 0, 0.0), ("B", 0, 10), ("S1", 3, 0.0),
    ("G1", 2, 0.0), ("B", 1, 10.1), ("S1", 4, 0.0), ("G2", 1, 0.0), ("G1", 3, 0.0),
    ("W", 0, 1184.5), ("G2", 2, 0.0), ("G1", 4, 0.0), ("S1", 5, 0.0), ("A2", 0, 0.0),
    ("G3", 0, 345.0), ("G3", 1, 27.6), ("G2", 3, 0.0), ("Q2", 0, 41.4), ("Q2", 1, 41.4),
    ("G1", 5, 0.0), ("A3", 0, 0.0), ("G2", 4, 0.0), ("G3", 2, 0.0), ("G3", 3, 1.7),
    ("G3", 4, 345.0), ("G2", 5, 0.0), ("O", 0, 40.5), ("G3", 5, 27.6),
)


def per_device(
    tokens, cotangent, token_ids, hash_table, segment_ids, query_weight, key_weight,
    value_weight, output_weight, gain_attn, gain_ffn, expert_in, expert_out,
):
    micro, n, d = tokens.shape
    ff = expert_in.shape[2]
    owners = lax.axis_size("expert")
    depth = lax.axis_size("dp")
    cap = 2 * n // owners
    weights = (query_weight, key_weight, value_weight, output_weight)
    LENGTH[0] = 1340.0
    gains = (gain_attn.reshape(1, d), gain_ffn.reshape(1, d))
    place = lax.axis_index("dp")
    outer = ((place == 0) | (place == depth - 1)).astype(jnp.int32).reshape(1)
    def swap(x):
        return lax.all_to_all(x, "expert", split_axis=0, concat_axis=0, tiled=True)

    slot0, slot1, packed = route(token_ids, hash_table, cotangent, owners, cap)
    slots = (slot0, slot1)
    gx = {0: swap(packed)}
    *kept0, packed0 = forward(
        0, slot0, segment_ids, tokens, cotangent, *weights, *gains, owners * cap, cap, packed
    )
    rx = {0: swap(after(packed0, gx[0]))}
    *kept1, packed1 = forward(
        1, slot1, segment_ids, tokens, cotangent, *weights, *gains, owners * cap, cap, packed0
    )
    both = swap(after(packed1, rx[0]))
    saved = (tuple(kept0), tuple(kept1))
    dep = packed1

    starts = [sum(SIZES[:i]) for i in range(len(SIZES))]
    chunk, hop1, hop2, hop3, sum1, total = {}, {}, {}, {}, {}, {}
    stored = gtok = dense = block_out = None
    backs, results, grads = {}, {}, {}
    for op, c, LENGTH[0] in PLAN:
        if op == "F":
            act0, gpre0 = expert_units(0, ff // BLOCK, (rx[0], gx[0]), expert_in, expert_out, dep)
            dep = act0
        elif op == "Fa":
            acta, gprea, rx[1], gx[1] = expert_units(
                0, SIZES[0], (both,), expert_in, expert_out, dep, cap
            )
            dep = rx[1]
        elif op == "Fb":
            actb, gpreb = expert_units(
                SIZES[0], ff // BLOCK - SIZES[0], (rx[1], gx[1]), expert_in, expert_out, dep
            )
            dep = actb
        elif op == "D":
            mine = (acta, gprea) if c == 0 else (actb, gpreb)
            first = starts[GROUPS[c][0]]
            made = expert_grads(
                [SIZES[i] for i in GROUPS[c]], (rx[0], rx[1]), (gx[0], gx[1]), (act0, mine[0]),
                (gpre0, mine[1]), (first, 0 if c == 0 else first - SIZES[0]), dep,
            )
            chunk.update(zip(GROUPS[c], made))
            dep = made[0]
        elif op == "S1":
            x = after(chunk[c], dep)
            hop1[c] = lax.ppermute(x, "dp", [(0, 1), (3, 2)]) if depth == 4 else x
        elif op == "G1":
            if depth == 4:
                sum1[c] = add(chunk[c], hop1[c], dep)
                hop2[c] = lax.ppermute(sum1[c], "dp", [(1, 2), (2, 1)])
                dep = sum1[c]
        elif op == "G2":
            if depth == 4:
                total[c] = add(sum1[c], hop2[c], dep)
                hop3[c] = lax.ppermute(total[c], "dp", [(1, 0), (2, 3)])
                dep = total[c]
            else:
                total[c] = hop3[c] = lax.psum(hop1[c], "dp")
        elif op == "G3":
            *stored, dep = store(starts[c], outer, total[c], hop3[c], ff, stored, dep)
        elif op == "Q1":
            dep = back_rows((gpre0,) if c == 0 else (gprea, gpreb), expert_in, 1, dep)
            backs[c] = swap(dep)
        elif op == "Q2":
            dep = back_rows((act0,) if c == 0 else (acta, actb), expert_out, 0, dep)
            results[c] = swap(dep)
        elif op == "B":
            gtok, *grads[c] = backward(
                c, slots[c], segment_ids, tokens, cotangent, backs[c], saved[c], *weights,
                *gains, gtok, dep,
            )
            dep = grads[c][0]
        elif op == "W":
            dep = dense_grads(saved, grads, 16 * owners, dep)
            dense = lax.psum_scatter(dep, "expert", scatter_dimension=0, tiled=True)
        elif op == "A2":
            dense = lax.psum(after(dense, dep), "dp")
        elif op == "A3":
            dense = lax.all_gather(after(dense, dep), "expert", axis=0, tiled=True)
        elif op == "O":
            block_out = block_output(
                slots, [results[m] for m in range(micro)], [s[6] for s in saved], dep
            )
            dep = block_out
    return (
        block_out,
        gtok,
        *(dense[i * d : (i + 1) * d].astype(F32) for i in range(4)),
        dense[4 * d].astype(F32),
        dense[4 * d + 1].astype(F32),
        *stored,
    )


def solution(mesh):
    blocks, ids = P(None, ("dp", "expert"), None), P(None, ("dp", "expert"))
    owned = P("expert", None, None)
    return jax.shard_map(
        per_device,
        mesh=mesh,
        in_specs=(blocks, blocks, ids, P(), ids, P(), P(), P(), P(), P(), P(), owned, owned),
        out_specs=(blocks, blocks, P(), P(), P(), P(), P(), P(), owned, owned),
        check_vma=False,
    )
```

```python
import functools

import jax
import jax.numpy as jnp
from jax import lax
from jax.experimental import pallas as pl
from jax.experimental.pallas import tpu as pltpu
from jax.sharding import PartitionSpec as P

HEADS = 12
HEAD_DIM = 64
EPS = 1e-05
SCALE = HEAD_DIM ** (-0.5)
PAIR = 2 * HEAD_DIM
F32 = jnp.float32
BF16 = jnp.bfloat16


def dot(a, b, ca=1, cb=0):
    return lax.dot_general(a, b, (((ca,), (cb,)), ((), ())), preferred_element_type=F32)


def params():
    return pltpu.CompilerParams(
        dimension_semantics=("arbitrary",), vmem_limit_bytes=60 * 1024 * 1024
    )


LENGTH = [1340.0]


def cost():
    return pl.CostEstimate(
        flops=int(LENGTH[0] * 1.0e9), bytes_accessed=1 << 20, transcendentals=0
    )


def full(*shape):
    return pl.BlockSpec(shape, lambda *_: (0,) * len(shape))


ANY = pl.BlockSpec(memory_space=pl.ANY)


def iota(shape, axis):
    return lax.broadcasted_iota(jnp.int32, shape, axis)


def to_column(row):
    n = row.shape[1]
    eye = iota((n, n), 0) == iota((n, n), 1)
    return jnp.sum(jnp.where(eye, row, 0), axis=1, keepdims=True)


def spread(slots, values, count):
    total = None
    for slot, value in zip(slots, values):
        places = (iota((count, slot.shape[1]), 0) == slot).astype(BF16)
        part = dot(places, value)
        total = part if total is None else total + part
    return total.astype(BF16)


def route_kernel(
    owners, cap, ids_ref, table_ref, cot_ref, slot0_ref, slot1_ref, pack_ref, lines_ref
):
    micro, n = ids_ref.shape
    size = table_ref.shape[0]
    rows = lines_ref.shape[0]
    lines_ref[...] = jnp.zeros_like(lines_ref)
    for i in range(0, size, 128):
        width = min(128, size - i)
        lines_ref[i // 128, 0:width] = table_ref[pl.ds(i, width)]
    table = lines_ref[...].astype(BF16)
    kinds = -(-owners // 16) * 16
    before = (iota((n, n), 0) < iota((n, n), 1)).astype(BF16)
    slots = []
    for m, slot_ref in enumerate((slot0_ref, slot1_ref)):
        ids = ids_ref[pl.ds(m, 1), :]
        pick = (iota((rows, n), 0) == (ids >> 7)).astype(BF16)
        values = dot(table, pick, 0, 0)
        lane = ids & 127
        expert = jnp.sum(
            jnp.where(iota((128, n), 0) == lane, values, 0.0), axis=0, keepdims=True
        )
        named = iota((kinds, n), 0).astype(F32) == expert
        counts = dot(named.astype(BF16), before)
        rank = jnp.sum(jnp.where(named, counts, 0.0), axis=0, keepdims=True)
        slot = (expert * cap + rank).astype(jnp.int32)
        slot_ref[...] = slot
        slots.append(slot)
    pack_ref[...] = spread(slots[:1], (cot_ref[0],), pack_ref.shape[0])


def route(ids, table, cot, owners, cap):
    micro, n = ids.shape
    width = cot.shape[2]
    size = table.shape[0]
    rows = -(-size // 1024) * 8
    return pl.pallas_call(
        functools.partial(route_kernel, owners, cap),
        grid=(1,),
        in_specs=[full(micro, n), full(size), full(1, n, width)],
        out_specs=[full(1, n), full(1, n), full(owners * cap, width)],
        out_shape=[
            jax.ShapeDtypeStruct((1, n), jnp.int32),
            jax.ShapeDtypeStruct((1, n), jnp.int32),
            jax.ShapeDtypeStruct((owners * cap, width), BF16),
        ],
        scratch_shapes=[pltpu.VMEM((rows, 128), jnp.int32)],
        cost_estimate=cost(),
        compiler_params=params(),
    )(ids, table, cot)


def bias_of(seg):
    n = seg.shape[1]
    key, query = iota((n, n), 0), iota((n, n), 1)
    seen = (key <= query) & (to_column(seg) == seg)
    return jnp.where(seen, 0.0, -1e30)


def forward_kernel(
    m, cap, slot_ref, seg_ref, tok_ref, cot_ref, wq_ref, wk_ref, wv_ref, wo_ref, ga_ref, gf_ref,
    dep_ref, normed_ref, q_ref, k_ref, v_ref, lse_ref, mixed_ref, hidden_ref, last_ref, bias_ref,
):
    x = tok_ref[0].astype(F32)
    n = x.shape[0]
    r = lax.rsqrt(jnp.mean(x * x, axis=1, keepdims=True) + EPS)
    normed = (x * r * ga_ref[...]).astype(BF16)
    normed_ref[...] = normed
    q_ref[...] = (dot(normed, wq_ref[...]).astype(BF16) * SCALE).astype(BF16)
    k_ref[...] = dot(normed, wk_ref[...]).astype(BF16)
    v_ref[...] = dot(normed, wv_ref[...]).astype(BF16)
    bias_ref[...] = bias_of(seg_ref[pl.ds(m, 1), :])
    low = iota((n, PAIR), 1) < HEAD_DIM

    def pair(p, carry):
        cols = pl.ds(pl.multiple_of(p * PAIR, PAIR), PAIR)
        q, k, v = q_ref[:, cols], k_ref[:, cols], v_ref[:, cols]
        parts = []
        for h in range(2):
            mine = low if h == 0 else ~low
            s = dot(k, jnp.where(mine, q, 0), 1, 1) + bias_ref[...]
            top = jnp.max(s, axis=0, keepdims=True)
            e = jnp.exp(s - top)
            total = jnp.sum(e, axis=0, keepdims=True)
            lse_ref[pl.ds(2 * p + h, 1), :] = top + jnp.log(total)
            probs = (e * (1.0 / total)).astype(BF16)
            parts.append(dot(probs, v, 0, 0))
        mixed_ref[:, cols] = jnp.where(low, parts[0], parts[1]).astype(BF16)
        return carry

    lax.fori_loop(0, HEADS // 2, pair, 0)
    hidden = x + dot(mixed_ref[...], wo_ref[...])
    hidden_ref[...] = hidden
    r = lax.rsqrt(jnp.mean(hidden * hidden, axis=1, keepdims=True) + EPS)
    routed = (hidden * r * gf_ref[...]).astype(BF16)
    slot = slot_ref[...]
    if m == 0:
        last_ref[...] = spread((slot,), (routed,), last_ref.shape[0])
    else:
        slot = slot + slot // cap * cap
        last_ref[...] = spread((slot, slot + cap), (cot_ref[0], routed), last_ref.shape[0])


def forward(m, slot, seg, tokens, cot, wq, wk, wv, wo, ga, gf, slots, cap, dep):
    _, n, d = tokens.shape
    shapes = [
        ((n, d), BF16), ((n, d), BF16), ((n, d), BF16), ((n, d), BF16), ((16, n), F32),
        ((n, d), BF16), ((n, d), F32), ((slots * (m + 1), d), BF16),
    ]
    mat = pl.BlockSpec((1, n, d), lambda i: (m, 0, 0))
    return pl.pallas_call(
        functools.partial(forward_kernel, m, cap),
        grid=(1,),
        in_specs=[
            full(1, n), full(*seg.shape), mat, mat,
            full(d, d), full(d, d), full(d, d), full(d, d), full(1, d), full(1, d), ANY,
        ],
        out_specs=[full(*s) for s, _ in shapes],
        out_shape=[jax.ShapeDtypeStruct(s, t) for s, t in shapes],
        scratch_shapes=[pltpu.VMEM((n, n), F32)],
        cost_estimate=cost(),
        compiler_params=params(),
    )(slot, seg, tokens, cot, wq, wk, wv, wo, ga, gf, dep)


BLOCK = 256
HALF = 128


def hidden_units(x, g, win, wout):
    pre = dot(x, win)
    sig = jax.nn.sigmoid(pre)
    soft = pre * sig
    slope = sig + soft * (1.0 - sig)
    return soft.astype(BF16), (dot(g, wout, 1, 1) * slope).astype(BF16)


def put_chunk(chunk_ref, at, gout, gin):
    for i in range(BLOCK // HALF):
        part = slice(i * HALF, (i + 1) * HALF)
        chunk_ref[pl.ds(at + 2 * i * HALF, HALF), :] = gout[part].astype(BF16)
        chunk_ref[pl.ds(at + (2 * i + 1) * HALF, HALF), :] = gin[part].astype(BF16)


def units_kernel(rx_ref, gx_ref, win_ref, wout_ref, *rest):
    act_ref, gpre_ref = rest[-2:]
    act_ref[...], gpre_ref[...] = hidden_units(
        rx_ref[...], gx_ref[...], win_ref[0], wout_ref[0]
    )


def split_units_kernel(cap, both_ref, win_ref, wout_ref, *rest):
    act_ref, gpre_ref, rx_ref, gx_ref = rest[-4:]

    @pl.when(pl.program_id(0) == 0)
    def _():
        for e in range(rx_ref.shape[0] // cap):
            mine = pl.ds(e * cap, cap)
            gx_ref[mine, :] = both_ref[pl.ds(2 * e * cap, cap), :]
            rx_ref[mine, :] = both_ref[pl.ds((2 * e + 1) * cap, cap), :]

    act_ref[...], gpre_ref[...] = hidden_units(
        rx_ref[...], gx_ref[...], win_ref[0], wout_ref[0]
    )


def expert_units(c, units, given, win, wout, dep, cap=None):
    d = win.shape[1]
    rows = given[0].shape[0] // (1 if cap is None else 2)
    f = BLOCK
    columns = pl.BlockSpec((rows, f), lambda i: (0, i))
    kernel = units_kernel if cap is None else functools.partial(split_units_kernel, cap)
    return pl.pallas_call(
        kernel,
        grid=(units,),
        in_specs=[full(*x.shape) for x in given]
        + [
            pl.BlockSpec((1, d, f), lambda i: (0, 0, c + i)),
            pl.BlockSpec((1, f, d), lambda i: (0, c + i, 0)),
            ANY,
        ],
        out_specs=[columns] * 2 + ([full(rows, d)] * 2 if cap else []),
        out_shape=[jax.ShapeDtypeStruct((rows, units * f), BF16)] * 2
        + ([jax.ShapeDtypeStruct((rows, d), BF16)] * 2 if cap else []),
        cost_estimate=cost(),
        compiler_params=params(),
    )(*given, win, wout, dep)


def chunk_kernel(
    sizes, rx0_ref, rx1_ref, gx0_ref, gx1_ref, act0_ref, act1_ref, gpre0_ref, gpre1_ref, dep_ref,
    *chunk_refs,
):
    gout = dot(act0_ref[...], gx0_ref[...], 0, 0) + dot(act1_ref[...], gx1_ref[...], 0, 0)
    gin = dot(gpre0_ref[...], rx0_ref[...], 0, 0) + dot(gpre1_ref[...], rx1_ref[...], 0, 0)
    step = 0
    for size, ref in zip(sizes, chunk_refs):
        for i in range(size):

            @pl.when(pl.program_id(0) == step)
            def _(ref=ref, i=i):
                put_chunk(ref, 2 * BLOCK * i, gout, gin)

            step += 1


def expert_grads(sizes, rx, gx, acts, gpres, at, dep):
    rows, d = rx[0].shape
    f = BLOCK
    columns = [pl.BlockSpec((rows, f), lambda i, k=k: (0, k + i)) for k in at]
    shapes = [(size * 2 * f, d) for size in sizes]
    return pl.pallas_call(
        functools.partial(chunk_kernel, sizes),
        grid=(sum(sizes),),
        in_specs=[full(rows, d)] * 4 + columns * 2 + [ANY],
        out_specs=[full(*x) for x in shapes],
        out_shape=[jax.ShapeDtypeStruct(x, BF16) for x in shapes],
        cost_estimate=cost(),
        compiler_params=params(),
    )(*rx, *gx, *acts, *gpres, dep)


def rows_kernel(side, *refs):
    *parts, w_ref, _, o_ref = refs
    total, start = None, 0
    for a_ref in parts:
        count = a_ref.shape[1]
        units = pl.ds(start, count)
        w = w_ref[0, :, units] if side == 1 else w_ref[0, units, :]
        term = dot(a_ref[...], w, 1, side)
        total = term if total is None else total + term
        start += count
    o_ref[...] = total.astype(BF16)


def back_rows(parts, w, side, dep, blk=256):
    rows = parts[0].shape[0]
    d = w.shape[1 + (1 - side)]
    return pl.pallas_call(
        functools.partial(rows_kernel, side),
        grid=(rows // blk,),
        in_specs=[pl.BlockSpec((blk, a.shape[1]), lambda i: (i, 0)) for a in parts]
        + [full(*w.shape), ANY],
        out_specs=pl.BlockSpec((blk, d), lambda i: (i, 0)),
        out_shape=jax.ShapeDtypeStruct((rows, d), BF16),
        cost_estimate=cost(),
        compiler_params=params(),
    )(*parts, w, dep)


def backward_kernel(
    m, slot_ref, seg_ref, tok_ref, cot_ref, back_ref, normed_ref, q_ref, k_ref, v_ref, lse_ref,
    hidden_ref, wq_ref, wk_ref, wv_ref, wo_ref, ga_ref, gf_ref, *rest,
):
    gtok_ref, gattn_ref, gq_ref, gk_ref, gv_ref, gain_ref = rest[-16:-10]
    bias_ref, gm_ref, gh_ref, hq_ref, hk_ref, hv_ref, iq_ref, ik_ref, iv_ref, sem = rest[-10:]
    copies = [
        pltpu.make_async_copy(a, b, sem.at[i])
        for i, (a, b) in enumerate(
            (
                (q_ref, iq_ref), (k_ref, ik_ref), (v_ref, iv_ref),
                (wq_ref, hq_ref), (wk_ref, hk_ref), (wv_ref, hv_ref),
            )
        )
    ]
    for copy in copies:
        copy.start()
    n, d = hidden_ref.shape
    slots = back_ref.shape[0]
    places = (iota((n, slots), 1) == to_column(slot_ref[...])).astype(BF16)
    grad_routed = dot(places, back_ref[...])
    hidden = hidden_ref[...]
    r = lax.rsqrt(jnp.mean(hidden * hidden, axis=1, keepdims=True) + EPS)
    unit = hidden * r
    g = grad_routed * gf_ref[...]
    grad_hidden = cot_ref[0].astype(F32) + r * (
        g - unit * jnp.mean(g * unit, axis=1, keepdims=True)
    )
    gh_ref[...] = grad_hidden
    gain_ref[pl.ds(1, 1), :] = jnp.sum(grad_routed * unit, axis=0, keepdims=True)
    grad_attn = grad_hidden.astype(BF16)
    gattn_ref[...] = grad_attn
    gm_ref[...] = dot(grad_attn, wo_ref[...], 1, 1).astype(BF16)
    bias_ref[...] = bias_of(seg_ref[pl.ds(m, 1), :])
    low = iota((n, PAIR), 1) < HEAD_DIM
    for copy in copies[:3]:
        copy.wait()

    def pair(p, carry):
        cols = pl.ds(pl.multiple_of(p * PAIR, PAIR), PAIR)
        q, k, v, gm = iq_ref[:, cols], ik_ref[:, cols], iv_ref[:, cols], gm_ref[:, cols]
        gqs, gks, gvs = [], [], []
        for h in range(2):
            mine = low if h == 0 else ~low
            s = dot(k, jnp.where(mine, q, 0), 1, 1) + bias_ref[...]
            probs = jnp.exp(s - lse_ref[pl.ds(2 * p + h, 1), :])
            gvs.append(dot(probs.astype(BF16), gm))
            gp = dot(v, jnp.where(mine, gm, 0), 1, 1)
            shared = jnp.sum(probs * gp, axis=0, keepdims=True)
            gs = (probs * (gp - shared)).astype(BF16)
            gks.append(dot(gs, q))
            gqs.append(dot(gs, k, 0, 0))
        gq_ref[:, cols] = (jnp.where(low, gqs[0], gqs[1]) * SCALE).astype(BF16)
        gk_ref[:, cols] = jnp.where(low, gks[0], gks[1]).astype(BF16)
        gv_ref[:, cols] = jnp.where(low, gvs[0], gvs[1]).astype(BF16)
        return carry

    lax.fori_loop(0, HEADS // 2, pair, 0)
    for copy in copies[3:]:
        copy.wait()
    grad_normed = (
        dot(gq_ref[...], hq_ref[...], 1, 1)
        + dot(gk_ref[...], hk_ref[...], 1, 1)
        + dot(gv_ref[...], hv_ref[...], 1, 1)
    )
    x = tok_ref[0].astype(F32)
    r = lax.rsqrt(jnp.mean(x * x, axis=1, keepdims=True) + EPS)
    unit = x * r
    gain_ref[pl.ds(0, 1), :] = jnp.sum(grad_normed * unit, axis=0, keepdims=True)
    g = grad_normed * ga_ref[...]
    gtok_ref[0] = (
        gh_ref[...] + r * (g - unit * jnp.mean(g * unit, axis=1, keepdims=True))
    ).astype(BF16)


def backward(m, slot, seg, tokens, cot, back, saved, wq, wk, wv, wo, ga, gf, held, dep):
    micro, n, d = tokens.shape
    normed, q, k, v, lse, _, hidden = saved
    mat = pl.BlockSpec((1, n, d), lambda i: (m, 0, 0))
    extra = [dep] if held is None else [dep, held]
    return pl.pallas_call(
        functools.partial(backward_kernel, m),
        grid=(1,),
        in_specs=[full(1, n), full(*seg.shape), mat, mat, full(*back.shape)]
        + [ANY] * 4 + [full(*lse.shape), full(*hidden.shape)]
        + [ANY] * 3 + [full(d, d)] + [full(1, d)] * 2 + [ANY] * len(extra),
        out_specs=[mat] + [full(n, d)] * 4 + [full(8, d)],
        out_shape=[jax.ShapeDtypeStruct((micro, n, d), BF16)]
        + [jax.ShapeDtypeStruct((n, d), BF16)] * 4
        + [jax.ShapeDtypeStruct((8, d), F32)],
        scratch_shapes=[
            pltpu.VMEM((n, n), F32), pltpu.VMEM((n, d), BF16), pltpu.VMEM((n, d), F32),
            pltpu.VMEM((d, d), BF16), pltpu.VMEM((d, d), BF16), pltpu.VMEM((d, d), BF16),
            pltpu.VMEM((n, d), BF16), pltpu.VMEM((n, d), BF16), pltpu.VMEM((n, d), BF16),
            pltpu.SemaphoreType.DMA((6,)),
        ],
        cost_estimate=cost(),
        compiler_params=params(),
        input_output_aliases={} if held is None else {18: 0},
    )(slot, seg, tokens, cot, back, normed, q, k, v, lse, hidden, wq, wk, wv, wo, ga, gf, *extra)


def weights_kernel(n0, n1, x0, x1, q0, q1, k0, k1, v0, v1, a0, a1, gain0, gain1, dep_ref, o_ref):
    d = n0.shape[1]
    for i, (l0, l1, r0, r1) in enumerate(
        ((n0, n1, q0, q1), (n0, n1, k0, k1), (n0, n1, v0, v1), (x0, x1, a0, a1))
    ):
        both = dot(l0[...], r0[...], 0, 0) + dot(l1[...], r1[...], 0, 0)
        o_ref[pl.ds(i * d, d), :] = both.astype(BF16)
    rest = o_ref.shape[0] - 4 * d
    line = iota((rest, d), 0)
    gain = gain0[...] + gain1[...]
    o_ref[pl.ds(4 * d, rest), :] = jnp.where(
        line == 0, gain[0:1, :], jnp.where(line == 1, gain[1:2, :], 0.0)
    ).astype(BF16)


def dense_grads(saved, grads, rest, dep):
    n, d = saved[0][0].shape
    pairs = [(saved[0][0], saved[1][0]), (saved[0][5], saved[1][5])]
    pairs += [(grads[0][i], grads[1][i]) for i in (1, 2, 3, 0, 4)]
    flat = [a for both in pairs for a in both]
    return pl.pallas_call(
        weights_kernel,
        grid=(1,),
        in_specs=[full(*a.shape) for a in flat] + [ANY],
        out_specs=full(4 * d + rest, d),
        out_shape=jax.ShapeDtypeStruct((4 * d + rest, d), BF16),
        cost_estimate=cost(),
        compiler_params=params(),
    )(*flat, dep)


def output_kernel(s0_ref, s1_ref, b0_ref, b1_ref, h0_ref, h1_ref, dep_ref, o_ref):
    n = o_ref.shape[1]
    for m, (s_ref, b_ref, h_ref) in enumerate(((s0_ref, b0_ref, h0_ref), (s1_ref, b1_ref, h1_ref))):
        places = (iota((n, b_ref.shape[0]), 1) == to_column(s_ref[...])).astype(BF16)
        o_ref[m] = (h_ref[...] + dot(places, b_ref[...])).astype(BF16)


def block_output(slots, backs, hiddens, dep):
    micro = len(slots)
    n, d = hiddens[0].shape
    flat = [*slots, *backs, *hiddens]
    return pl.pallas_call(
        output_kernel,
        grid=(1,),
        in_specs=[full(*a.shape) for a in flat] + [ANY],
        out_specs=full(micro, n, d),
        out_shape=jax.ShapeDtypeStruct((micro, n, d), BF16),
        cost_estimate=cost(),
        compiler_params=params(),
    )(*flat, dep)


def after(x, dep):
    return lax.optimization_barrier((x, dep))[0]


def add(a, b, dep):
    return (after(a, dep).astype(F32) + b.astype(F32)).astype(BF16)


def store_kernel(flag_ref, a_ref, b_ref, *rest):
    gin_ref, gout_ref, token_ref = rest[-3:]
    token_ref[...] = jnp.zeros_like(token_ref)

    def put(ref):
        gout_ref[0] = ref[pl.ds(0, HALF), :].astype(F32)
        gin_ref[0] = ref[pl.ds(HALF, HALF), :].astype(F32).T

    @pl.when(flag_ref[0] == 1)
    def _():
        put(b_ref)

    @pl.when(flag_ref[0] != 1)
    def _():
        put(a_ref)


def store(c, flag, a, b, ff, held, dep):
    rows, d = a.shape
    spec = pl.BlockSpec((2 * HALF, d), lambda i: (i, 0))
    base = c * (BLOCK // HALF)
    extra = ([] if held is None else list(held)) + [dep]
    return pl.pallas_call(
        store_kernel,
        grid=(rows // (2 * HALF),),
        in_specs=[pl.BlockSpec(memory_space=pltpu.SMEM), spec, spec] + [ANY] * len(extra),
        out_specs=[
            pl.BlockSpec((1, d, HALF), lambda i: (0, 0, base + i)),
            pl.BlockSpec((1, HALF, d), lambda i: (0, base + i, 0)),
            full(8, 128),
        ],
        out_shape=[
            jax.ShapeDtypeStruct((1, d, ff), F32),
            jax.ShapeDtypeStruct((1, ff, d), F32),
            jax.ShapeDtypeStruct((8, 128), F32),
        ],
        input_output_aliases={} if held is None else {3: 0, 4: 1},
        cost_estimate=cost(),
        compiler_params=params(),
    )(flag, a, b, *extra)


SIZES = (2, 2, 2, 2, 2, 2)
GROUPS = ((0,), (1,), (2, 3, 4, 5))


PLAN = (
    ("F", 0, 2185.0), ("Q2", 0, 41.4), ("Fa", 1, 460.0), ("D", 0, 5.8), ("S1", 0, 0.0),
    ("Fb", 1, 1610.0), ("Q1", 0, 0.0), ("D", 1, 5.8), ("S1", 1, 0.0), ("G1", 0, 0.0),
    ("Q1", 1, 2.6), ("D", 2, 0.0), ("S1", 2, 0.0), ("G1", 1, 0.0), ("B", 0, 2012.5),
    ("G2", 0, 0.0), ("S1", 3, 0.0), ("G1", 2, 0.0), ("B", 1, 10.1), ("S1", 4, 0.0),
    ("G2", 1, 0.0), ("G1", 3, 0.0), ("W", 0, 1184.5), ("G2", 2, 0.0), ("G1", 4, 0.0),
    ("S1", 5, 0.0), ("A2", 0, 0.0), ("G3", 0, 345.0), ("G3", 1, 27.6), ("G2", 3, 0.0),
    ("Q2", 1, 41.4), ("G1", 5, 0.0), ("A3", 0, 0.0), ("G2", 4, 0.0), ("G3", 2, 0.0),
    ("G3", 3, 1.7), ("G3", 4, 345.0), ("G2", 5, 0.0), ("O", 0, 40.5), ("G3", 5, 27.6),
)


def per_device(
    tokens, cotangent, token_ids, hash_table, segment_ids, query_weight, key_weight,
    value_weight, output_weight, gain_attn, gain_ffn, expert_in, expert_out,
):
    micro, n, d = tokens.shape
    ff = expert_in.shape[2]
    owners = lax.axis_size("expert")
    depth = lax.axis_size("dp")
    cap = 2 * n // owners
    weights = (query_weight, key_weight, value_weight, output_weight)
    LENGTH[0] = 1340.0
    gains = (gain_attn.reshape(1, d), gain_ffn.reshape(1, d))
    place = lax.axis_index("dp")
    outer = ((place == 0) | (place == depth - 1)).astype(jnp.int32).reshape(1)
    def swap(x):
        return lax.all_to_all(x, "expert", split_axis=0, concat_axis=0, tiled=True)

    slot0, slot1, packed = route(token_ids, hash_table, cotangent, owners, cap)
    slots = (slot0, slot1)
    gx = {0: swap(packed)}
    *kept0, packed0 = forward(
        0, slot0, segment_ids, tokens, cotangent, *weights, *gains, owners * cap, cap, packed
    )
    rx = {0: swap(after(packed0, gx[0]))}
    *kept1, packed1 = forward(
        1, slot1, segment_ids, tokens, cotangent, *weights, *gains, owners * cap, cap, packed0
    )
    both = swap(after(packed1, rx[0]))
    saved = (tuple(kept0), tuple(kept1))
    dep = packed1

    starts = [sum(SIZES[:i]) for i in range(len(SIZES))]
    chunk, hop1, hop2, hop3, sum1, total = {}, {}, {}, {}, {}, {}
    stored = gtok = dense = block_out = None
    backs, results, grads = {}, {}, {}
    for op, c, LENGTH[0] in PLAN:
        if op == "F":
            act0, gpre0 = expert_units(0, ff // BLOCK, (rx[0], gx[0]), expert_in, expert_out, dep)
            dep = act0
        elif op == "Fa":
            acta, gprea, rx[1], gx[1] = expert_units(
                0, SIZES[0], (both,), expert_in, expert_out, dep, cap
            )
            dep = rx[1]
        elif op == "Fb":
            actb, gpreb = expert_units(
                SIZES[0], ff // BLOCK - SIZES[0], (rx[1], gx[1]), expert_in, expert_out, dep
            )
            dep = actb
        elif op == "D":
            mine = (acta, gprea) if c == 0 else (actb, gpreb)
            first = starts[GROUPS[c][0]]
            made = expert_grads(
                [SIZES[i] for i in GROUPS[c]], (rx[0], rx[1]), (gx[0], gx[1]), (act0, mine[0]),
                (gpre0, mine[1]), (first, 0 if c == 0 else first - SIZES[0]), dep,
            )
            chunk.update(zip(GROUPS[c], made))
            dep = made[0]
        elif op == "S1":
            x = after(chunk[c], dep)
            hop1[c] = lax.ppermute(x, "dp", [(0, 1), (3, 2)]) if depth == 4 else x
        elif op == "G1":
            if depth == 4:
                sum1[c] = add(chunk[c], hop1[c], dep)
                hop2[c] = lax.ppermute(sum1[c], "dp", [(1, 2), (2, 1)])
                dep = sum1[c]
        elif op == "G2":
            if depth == 4:
                total[c] = add(sum1[c], hop2[c], dep)
                hop3[c] = lax.ppermute(total[c], "dp", [(1, 0), (2, 3)])
                dep = total[c]
            else:
                total[c] = hop3[c] = lax.psum(hop1[c], "dp")
        elif op == "G3":
            *stored, dep = store(starts[c], outer, total[c], hop3[c], ff, stored, dep)
        elif op == "Q1":
            dep = back_rows((gpre0,) if c == 0 else (gprea, gpreb), expert_in, 1, dep)
            backs[c] = swap(dep)
        elif op == "Q2":
            dep = back_rows((act0,) if c == 0 else (acta, actb), expert_out, 0, dep)
            results[c] = swap(dep)
        elif op == "B":
            gtok, *grads[c] = backward(
                c, slots[c], segment_ids, tokens, cotangent, backs[c], saved[c], *weights,
                *gains, gtok, dep,
            )
            dep = grads[c][0]
        elif op == "W":
            dep = dense_grads(saved, grads, 16 * owners, dep)
            dense = lax.psum_scatter(dep, "expert", scatter_dimension=0, tiled=True)
        elif op == "A2":
            dense = lax.psum(after(dense, dep), "dp")
        elif op == "A3":
            dense = lax.all_gather(after(dense, dep), "expert", axis=0, tiled=True)
        elif op == "O":
            block_out = block_output(
                slots, [results[m] for m in range(micro)], [s[6] for s in saved], dep
            )
            dep = block_out
    return (
        block_out,
        gtok,
        *(dense[i * d : (i + 1) * d].astype(F32) for i in range(4)),
        dense[4 * d].astype(F32),
        dense[4 * d + 1].astype(F32),
        *stored,
    )


def solution(mesh):
    blocks, ids = P(None, ("dp", "expert"), None), P(None, ("dp", "expert"))
    owned = P("expert", None, None)
    return jax.shard_map(
        per_device,
        mesh=mesh,
        in_specs=(blocks, blocks, ids, P(), ids, P(), P(), P(), P(), P(), P(), owned, owned),
        out_specs=(blocks, blocks, P(), P(), P(), P(), P(), P(), owned, owned),
        check_vma=False,
    )
```
